8 devices in a mesh: data: 1 (over z), expert: 8 (over y, x, core).
Axes of the slice: x: 2, y: 2, z: 1, core: 2. Of those that a mesh axis runs over, the one named last changes fastest.
Arguments:
- token_rows: bfloat16 [16384, 512], P(('data', 'expert'))
- expert_ids: int32 [16384, 2], P(('data', 'expert'))
- gate_weights: float32 [16384, 2], P(('data', 'expert'))
- w_in: bfloat16 [512, 512, 1024], P('expert')
- w_out: bfloat16 [512, 1024, 512], P('expert')
Outputs:
- output: bfloat16 [16384, 512], P(('data', 'expert'))
All inputs are finite; a program needn't handle non-finite values.
Results may differ from the reference program's by a relative error of at most 0.001.
Values are sent between devices in bfloat16 or wider.
A program may use at most 1 GiB of HBM per device.

```python
import math
import jax
import jax.numpy as jnp
from jax import lax

TOKENS_DEV = 2048
GROUP_DEVS = 8
MODEL_DIM = 512
HIDDEN_DIM = 1024
EXPERTS = 512
TOP_K = 2

TOKENS = TOKENS_DEV * GROUP_DEVS
MEAN_LOAD = TOKENS_DEV * TOP_K // EXPERTS
CAPACITY = TOKENS * TOP_K // EXPERTS
POP_SPREAD = MEAN_LOAD // 2
DEV_SPREAD = MEAN_LOAD // 4


def draw_routing(key):
    key_order, key_pop, key_dev, key_tok, key_col = jax.random.split(key, 5)
    expert_order = jax.random.permutation(key_order, EXPERTS)
    pop_bias = jax.random.randint(key_pop, (EXPERTS,), 0, POP_SPREAD + 1)
    pop_bias = pop_bias.at[0].set(POP_SPREAD).at[1].set(0)
    dev_bias = jax.random.randint(key_dev, (GROUP_DEVS, EXPERTS), 0, DEV_SPREAD + 1)
    dev_bias = dev_bias.at[:, 0].set(DEV_SPREAD).at[:, 1].set(0)
    pair_load = MEAN_LOAD + (pop_bias - jnp.roll(pop_bias, -1))[None, :] + dev_bias - jnp.roll(dev_bias, -1, axis=1)
    run_ends = jnp.cumsum(pair_load, axis=1)
    positions = jnp.arange(TOKENS_DEV * TOP_K, dtype=jnp.int32)

    def find_run(row_ends):
        return jnp.searchsorted(row_ends, positions, side="right")

    run_index = jax.vmap(find_run)(run_ends)
    labels = expert_order[run_index].reshape(GROUP_DEVS, TOP_K, TOKENS_DEV)
    choices = jnp.swapaxes(labels, 1, 2)

    def token_order(sub_key):
        return jax.random.permutation(sub_key, TOKENS_DEV)

    tok_perm = jax.vmap(token_order)(jax.random.split(key_tok, GROUP_DEVS))
    choices = jnp.take_along_axis(choices, tok_perm[:, :, None], axis=1)
    choices = jax.random.permutation(key_col, choices, axis=2, independent=True)
    return choices.reshape(TOKENS, TOP_K).astype(jnp.int32)


def draw_matrices(key, fan_in, fan_out):
    def one_matrix(sub_key):
        return (jax.random.normal(sub_key, (fan_in, fan_out), jnp.float32) / math.sqrt(fan_in)).astype(jnp.bfloat16)
    return lax.map(one_matrix, jax.random.split(key, EXPERTS))


def setup_inputs(seed: int = 0, part: int = 0) -> dict:
    root = jax.random.key(seed)
    part_key = jax.random.fold_in(root, part)
    key_route, key_rows, key_gate = jax.random.split(part_key, 3)
    key_up, key_down = jax.random.split(jax.random.fold_in(root, 1000003), 2)
    token_rows = jax.random.normal(key_rows, (TOKENS, MODEL_DIM), jnp.float32).astype(jnp.bfloat16)
    gate_weights = jax.random.uniform(key_gate, (TOKENS, TOP_K), jnp.float32, 0.5, 1.5) / math.sqrt(TOP_K)
    return {"token_rows": token_rows, "expert_ids": draw_routing(key_route), "gate_weights": gate_weights, "w_in": draw_matrices(key_up, MODEL_DIM, HIDDEN_DIM), "w_out": draw_matrices(key_down, HIDDEN_DIM, MODEL_DIM)}


def expert_ffn(operands):
    rows, up_weight, down_weight = operands
    hidden = jax.nn.gelu(jnp.dot(rows, up_weight, preferred_element_type=jnp.float32)).astype(jnp.bfloat16)
    return jnp.dot(hidden, down_weight, preferred_element_type=jnp.float32).astype(jnp.bfloat16)


def reference(token_rows, expert_ids, gate_weights, w_in, w_out):
    pairs = TOP_K * TOKENS
    flat_ids = expert_ids.T.reshape(pairs)
    sort_order = jnp.argsort(flat_ids, stable=True)
    position = jnp.zeros((pairs,), jnp.int32).at[sort_order].set(jnp.arange(pairs, dtype=jnp.int32))
    counts = jnp.bincount(flat_ids, length=EXPERTS)
    seg_start = jnp.cumsum(counts) - counts
    slot = position - seg_start[flat_ids]
    keep = slot < CAPACITY
    slot_safe = jnp.where(keep, slot, CAPACITY)
    buffer = jnp.zeros((EXPERTS, CAPACITY, MODEL_DIM), token_rows.dtype).at[flat_ids, slot_safe].set(jnp.tile(token_rows, (TOP_K, 1)), mode="drop")
    outputs = lax.map(expert_ffn, (buffer, w_in, w_out))
    weight = jnp.where(keep, gate_weights.T.reshape(pairs), 0.0).reshape(TOP_K, TOKENS)
    slot_read = jnp.minimum(slot, CAPACITY - 1).reshape(TOP_K, TOKENS)

    def add_choice(total, pieces):
        choice_weight, choice_ids, choice_slot = pieces
        return total + choice_weight[:, None] * outputs[choice_ids, choice_slot].astype(jnp.float32), None

    mixed, _ = lax.scan(add_choice, token_rows.astype(jnp.float32), (weight, flat_ids.reshape(TOP_K, TOKENS), slot_read))
    return mixed.astype(jnp.bfloat16)
```

```python
import functools

import jax
import jax.numpy as jnp
from jax import lax
from jax.experimental import pallas as pl
from jax.experimental.pallas import tpu as pltpu
from jax.sharding import PartitionSpec as P

GROUPS = 2
BUFS = 4
LANES = 128
MESH = pl.DeviceIdType.MESH


def route_local(expert_ids, experts):
    ids_t = expert_ids.T
    onehot = (ids_t[:, :, None] == jnp.arange(experts, dtype=jnp.int32)).astype(jnp.int32)
    running = jnp.cumsum(onehot, axis=1)
    counts = running[:, -1, :]
    rank_local = jnp.sum(onehot * running, axis=2) - 1
    return ids_t, counts, rank_local


def padded_step(groups, token_rows, expert_ids, gate_weights, w_in, w_out):
    tokens, top_k = expert_ids.shape
    local_experts, model_dim = w_in.shape[0], w_in.shape[1]
    experts = local_experts * groups
    mean_load = tokens * top_k // experts
    send_cap = 7 * mean_load // 4
    capacity = groups * mean_load
    rows_total = experts * send_cap
    ids_t, counts, rank_local = route_local(expert_ids, experts)
    inclusive = counts
    shift = 1
    while shift < groups:
        pairs_list = [(source, source + shift) for source in range(groups - shift)]
        inclusive = inclusive + lax.ppermute(inclusive, "expert", pairs_list)
        shift = shift * 2
    before = inclusive - counts
    totals = lax.psum(counts, "expert")
    prior = jnp.cumsum(totals, axis=0) - totals
    within = jnp.cumsum(counts, axis=0) - counts
    slot = jnp.take_along_axis(prior + before, ids_t, axis=1) + rank_local
    keep = slot < capacity
    target = ids_t * send_cap + jnp.take_along_axis(within, ids_t, axis=1) + rank_local
    token_ids = jnp.broadcast_to(jnp.arange(tokens, dtype=jnp.int32), (top_k, tokens))
    source_row = jnp.full((rows_total,), tokens, jnp.int32).at[jnp.where(keep, target, rows_total).reshape(-1)].set(token_ids.reshape(-1), mode="drop")
    padded = jnp.concatenate([token_rows, jnp.zeros((1, model_dim), token_rows.dtype)], axis=0)
    outbound = jnp.take(padded, source_row, axis=0).reshape(experts, send_cap, model_dim)
    inbound = lax.all_to_all(outbound, "expert", 0, 0, tiled=True).reshape(groups, local_experts, send_cap, model_dim)
    pre_act = jnp.einsum("gesd,edf->gesf", inbound, w_in, preferred_element_type=jnp.float32)
    hidden = jax.nn.gelu(pre_act).astype(jnp.bfloat16)
    expert_out = jnp.einsum("gesf,efd->gesd", hidden, w_out, preferred_element_type=jnp.float32).astype(jnp.bfloat16)
    returned = lax.all_to_all(expert_out.reshape(experts, send_cap, model_dim), "expert", 0, 0, tiled=True).reshape(rows_total, model_dim)
    picked = jnp.take(returned, target, axis=0)
    weight = jnp.where(keep, gate_weights.T, 0.0)
    mixed = jnp.sum(weight[:, :, None] * picked.astype(jnp.float32), axis=0)
    return (token_rows.astype(jnp.float32) + mixed).astype(jnp.bfloat16)


def block_rows(tokens, top_k, groups):
    mean = tokens * top_k // (groups * GROUPS)
    return (mean * 19 // 16 + 15) // 16 * 16


def dot_f32(a, b):
    return jnp.dot(a, b, preferred_element_type=jnp.float32)


def routing(groups, expert_ids, local_experts, capacity):
    tokens, top_k = expert_ids.shape
    experts = local_experts * groups
    group_experts = local_experts // GROUPS
    rows = block_rows(tokens, top_k, groups)
    positions = GROUPS * groups * rows
    me = lax.axis_index("expert")
    block = 256
    lane = jnp.arange(experts, dtype=jnp.int32)
    onehot = expert_ids.T[:, :, None] == lane
    onehot_b = onehot.astype(jnp.bfloat16).reshape(top_k, tokens // block, block, experts)
    tri = (jnp.arange(block)[:, None] > jnp.arange(block)[None, :]).astype(jnp.bfloat16)
    within = jnp.einsum("ab,jnbe->jnae", tri, onehot_b, preferred_element_type=jnp.float32)
    sums = jnp.sum(onehot_b.astype(jnp.float32), axis=2)
    base = jnp.cumsum(sums, axis=1) - sums
    counts = jnp.sum(sums, axis=1)
    everyone = lax.all_gather(counts, "expert")
    before = jnp.cumsum(everyone, axis=0) - everyone
    totals = jnp.sum(everyone, axis=0)
    prior = jnp.cumsum(totals, axis=0) - totals
    kept = jnp.clip(capacity - prior - before, 0.0, everyone)
    kept_all = jnp.sum(kept, axis=1)
    same = (lane[:, None] // group_experts == lane[None, :] // group_experts) & (lane[:, None] < lane[None, :])
    start = dot_f32(kept_all.astype(jnp.bfloat16), same.astype(jnp.bfloat16))
    overflow = jnp.max(start + kept_all) > rows
    block_of = (lane % local_experts // group_experts) * groups + lane // local_experts
    mine, mine_start = kept[me], start[me]
    first = (block_of * rows).astype(jnp.float32) + mine_start
    offset = jnp.stack([first, first + mine[0]])
    rank = within + base[:, :, None, :]
    value = jnp.where(rank < mine[:, None, None, :], rank + offset[:, None, None, :], float(positions))
    pos = jnp.sum(jnp.where(onehot.reshape(value.shape), value, 0.0), axis=3).reshape(top_k, tokens).astype(jnp.int32)
    high = (pos[:, :, None] // LANES == jnp.arange(positions // LANES, dtype=jnp.int32)).astype(jnp.bfloat16)
    low = pos[:, :, None] % LANES == jnp.arange(LANES, dtype=jnp.int32)
    token = jnp.arange(tokens, dtype=jnp.int32)[:, None]
    low_hi = jnp.where(low, (token // 8).astype(jnp.float32), 0.0).astype(jnp.bfloat16)
    low_lo = jnp.where(low, (token % 8).astype(jnp.float32), 0.0).astype(jnp.bfloat16)
    found = jnp.einsum("jth,jtl->hl", high, jnp.concatenate([low_hi, low_lo], axis=2), preferred_element_type=jnp.float32)
    pack = (found[:, :LANES] * 8.0 + found[:, LANES:]).astype(jnp.int32).reshape(-1)

    cum = jnp.cumsum(kept_all, axis=0) - kept_all
    local = lambda a: lax.dynamic_slice_in_dim(a, me * local_experts, local_experts, 1)
    k_l, s_l, c_l = local(kept_all), local(start), local(cum)
    q = jnp.arange(capacity, dtype=jnp.float32)[:, None]
    lhs = jnp.zeros((capacity, local_experts), jnp.float32)
    for s in range(groups):
        inside = (q >= c_l[s]) & (q < c_l[s] + k_l[s])
        lhs = lhs + jnp.where(inside, s * rows + s_l[s] - c_l[s] + q, 0.0)
    lhs = lhs.astype(jnp.int32).reshape(-1)

    in_group = (jnp.arange(local_experts, dtype=jnp.int32) % group_experts).astype(jnp.float32)
    v = in_group * capacity + c_l - s_l
    v = v.reshape(groups, GROUPS, group_experts)
    step = v - jnp.concatenate([jnp.zeros_like(v[:, :, :1]), v[:, :, :-1]], axis=2)
    p = jnp.arange(rows, dtype=jnp.float32)[:, None]
    reached = p >= s_l.reshape(groups, GROUPS, 1, group_experts)
    ret = p[:, 0] + jnp.sum(jnp.where(reached, step[:, :, None, :], 0.0), axis=3)
    ret = jnp.clip(ret, 0.0, group_experts * capacity - 1.0).astype(jnp.int32)
    ret = ret.transpose(1, 0, 2).reshape(-1)
    return overflow, pack, lhs, ret, pos.reshape(-1)


def exchange_kernel(
    groups, rows, capacity,
    pack_idx, lhs_idx, ret_idx, comb_idx, gates, x_ref, win_ref, wout_ref, out_ref,
    xr_rows, send, recv, rf_rows, stage0, stage1, of_rows, rsend, rrecv, retf_rows, wi, wo,
    wsem, ssem, rsem, rssem, rrsem,
):
    tokens, model_dim = x_ref.shape
    sub = model_dim // LANES
    local_experts = win_ref.shape[0]
    group_experts = local_experts // GROUPS
    me = lax.axis_index("expert")
    span = rows * sub
    stages = (stage0, stage1)
    xr, rf, of, retf = (r.reshape(r.shape[0] * sub, LANES) for r in (xr_rows, rf_rows, of_rows, retf_rows))

    def fetch(e, slot):
        a = pltpu.make_async_copy(win_ref.at[e], wi.at[slot], wsem.at[slot, 0])
        b = pltpu.make_async_copy(wout_ref.at[e], wo.at[slot], wsem.at[slot, 1])
        return a, b

    for e in range(BUFS):
        for c in fetch(e, e):
            c.start()
    barrier = pltpu.get_barrier_semaphore()
    for k in range(1, groups):
        pl.semaphore_signal(barrier, inc=1, device_id={"expert": lax.rem(me + k, groups)}, device_id_type=MESH)
    for k in range(sub):
        xr[pl.ds(k, tokens, stride=sub), :] = x_ref[:, k * LANES:(k + 1) * LANES].astype(jnp.float32)
    retf[pl.ds(GROUPS * groups * span, 8 * sub), :] = jnp.zeros((8 * sub, LANES), jnp.float32)
    pl.semaphore_wait(barrier, groups - 1)

    def gather_block(idx, first, table, dst):
        def body(c, carry):
            got = [table[idx[first + c * 16 + r]] for r in range(16)]
            dst[pl.ds(pl.multiple_of(c * 16 * sub, 16 * sub), 16 * sub), :] = jnp.concatenate(got, axis=0).astype(jnp.bfloat16)
            return carry
        lax.fori_loop(0, rows // 16, body, 0)

    def widen(src, dst, first):
        def body(c, carry):
            part = pl.multiple_of(c * 16 * sub, 16 * sub)
            dst[pl.ds(pl.multiple_of(first + part, 16), 16 * sub), :] = src[pl.ds(part, 16 * sub), :].astype(jnp.float32)
            return carry
        lax.fori_loop(0, rows // 16, body, 0)

    def copy_to(src, dst, g, k, s_sem, r_sem):
        peer = lax.rem(me + k, groups)
        return pltpu.make_async_remote_copy(
            src_ref=src.at[g, peer], dst_ref=dst.at[g, me], send_sem=s_sem.at[g, k], recv_sem=r_sem.at[g, k],
            device_id={"expert": peer}, device_id_type=MESH)

    def send_blocks(g, idx, table, src, dst, s_sem, r_sem):
        late = None
        for k in list(range(1, groups)) + [0]:
            peer = lax.rem(me + k, groups)
            gather_block(idx, (g * groups + peer) * rows, table, src.at[g, peer])
            if late is not None:
                late.start()
            late = copy_to(src, dst, g, k, s_sem, r_sem) if k else None

    def take_blocks(g, src, dst, own, first, s_sem, r_sem):
        for k in range(groups):
            peer = lax.rem(me - k + groups, groups)
            if k:
                pltpu.make_async_remote_copy(
                    src_ref=own.at[g, peer], dst_ref=src.at[g, peer], send_sem=s_sem.at[g, k], recv_sem=r_sem.at[g, k],
                    device_id={"expert": peer}, device_id_type=MESH).wait_recv()
                widen(src.at[g, peer], dst, first + peer * span)
            else:
                widen(own.at[g, peer], dst, first + peer * span)

    for g in range(GROUPS):
        send_blocks(g, pack_idx, xr_rows, send, recv, ssem, rsem)

    for g in range(GROUPS):
        take_blocks(g, recv, rf, send, 0, ssem, rsem)

        def gather_lhs(e, stage):
            for q in range(capacity):
                stage[pl.ds(q * sub, sub), :] = rf_rows[lhs_idx[q * local_experts + e]]

        def ffn(e, stage):
            slot = lax.rem(e, BUFS)
            for c in fetch(e, slot):
                c.wait()
            lhs = jnp.concatenate([stage[pl.ds(k, capacity, stride=sub), :] for k in range(sub)], axis=1).astype(jnp.bfloat16)
            hidden = jax.nn.gelu(dot_f32(lhs, wi[slot])).astype(jnp.bfloat16)
            out = dot_f32(hidden, wo[slot]).astype(jnp.bfloat16).astype(jnp.float32)
            at = (e - g * group_experts) * capacity * sub
            for k in range(sub):
                of[pl.ds(at + k, capacity, stride=sub), :] = out[:, k * LANES:(k + 1) * LANES]

        def body(i, carry):
            for half in range(2):
                e = g * group_experts + i * 2 + half
                gather_lhs(e, stages[half])
                ffn(e, stages[half])

                @pl.when(e + BUFS < local_experts)
                def _():
                    for c in fetch(e + BUFS, lax.rem(e, BUFS)):
                        c.start()
            return carry

        lax.fori_loop(0, group_experts // 2, body, 0)
        send_blocks(g, ret_idx, of_rows, rsend, rrecv, rssem, rrsem)

    for g in range(GROUPS):
        take_blocks(g, rrecv, retf, rsend, g * groups * span, rssem, rrsem)

    def combine(c, carry):
        got = []
        for r in range(16):
            t = c * 16 + r
            row = xr_rows[t]
            for j in range(2):
                row = row + gates[j * tokens + t] * retf_rows[comb_idx[j * tokens + t]]
            got.append(row)
        xr[pl.ds(pl.multiple_of(c * 16 * sub, 16 * sub), 16 * sub), :] = jnp.concatenate(got, axis=0)
        return carry

    lax.fori_loop(0, tokens // 16, combine, 0)
    for k in range(sub):
        out_ref[:, k * LANES:(k + 1) * LANES] = xr[pl.ds(k, tokens, stride=sub), :].astype(jnp.bfloat16)
    for g in range(GROUPS):
        for k in range(1, groups):
            copy_to(send, recv, g, k, ssem, rsem).wait_send()
            copy_to(rsend, rrecv, g, k, rssem, rrsem).wait_send()


def compact_step(groups, capacity, pack, lhs, ret, comb, gates, token_rows, w_in, w_out):
    tokens, model_dim = token_rows.shape
    local_experts, _, hidden_dim = w_in.shape
    group_experts = local_experts // GROUPS
    rows = pack.shape[0] // (GROUPS * groups)
    sub = model_dim // LANES
    span = rows * sub
    smem = pl.BlockSpec(memory_space=pltpu.SMEM)
    vmem = pl.BlockSpec(memory_space=pltpu.VMEM)
    hbm = pl.BlockSpec(memory_space=pl.ANY)
    wire = pltpu.VMEM((GROUPS, groups, span, LANES), jnp.bfloat16)
    sems = pltpu.SemaphoreType.DMA((GROUPS, groups))
    return pl.pallas_call(
        functools.partial(exchange_kernel, groups, rows, capacity),
        out_shape=jax.ShapeDtypeStruct((tokens, model_dim), jnp.bfloat16),
        in_specs=[smem] * 5 + [vmem, hbm, hbm],
        out_specs=vmem,
        scratch_shapes=[
            pltpu.VMEM((tokens, sub, LANES), jnp.float32),
            wire,
            wire,
            pltpu.VMEM((groups * rows, sub, LANES), jnp.float32),
            pltpu.VMEM((capacity * sub, LANES), jnp.float32),
            pltpu.VMEM((capacity * sub, LANES), jnp.float32),
            pltpu.VMEM((group_experts * capacity, sub, LANES), jnp.float32),
            wire,
            wire,
            pltpu.VMEM((GROUPS * groups * rows + 8, sub, LANES), jnp.float32),
            pltpu.VMEM((BUFS, model_dim, hidden_dim), jnp.bfloat16),
            pltpu.VMEM((BUFS, hidden_dim, model_dim), jnp.bfloat16),
            pltpu.SemaphoreType.DMA((BUFS, 2)),
            sems, sems, sems, sems,
        ],
        compiler_params=pltpu.CompilerParams(collective_id=0, has_side_effects=True, vmem_limit_bytes=64000000),
        name="expert_exchange",
    )(pack, lhs, ret, comb, gates, token_rows, w_in, w_out)


def solution(mesh):
    groups = mesh.shape["expert"]
    row_spec = P(("data", "expert"), None)
    weight_spec = P("expert", None, None)

    def device_step(token_rows, expert_ids, gate_weights, w_in, w_out):
        tokens, top_k = expert_ids.shape
        local_experts = w_in.shape[0]
        capacity = tokens * top_k // local_experts
        overflow, pack, lhs, ret, comb = routing(groups, expert_ids, local_experts, capacity)
        fast = compact_step(groups, capacity, pack, lhs, ret, comb, gate_weights.T.reshape(-1), token_rows, w_in, w_out)
        return lax.cond(
            overflow,
            lambda f: padded_step(groups, token_rows, expert_ids, gate_weights, w_in, w_out),
            lambda f: f,
            fast,
        )

    return jax.shard_map(device_step, mesh=mesh, in_specs=(row_spec, row_spec, row_spec, weight_spec, weight_spec), out_specs=row_spec, check_vma=False)
```

```python
import functools

import jax
import jax.numpy as jnp
from jax import lax
from jax.experimental import pallas as pl
from jax.experimental.pallas import tpu as pltpu
from jax.sharding import PartitionSpec as P

GROUPS = 2
BUFS = 3
LANES = 128
MESH = pl.DeviceIdType.MESH


def route_local(expert_ids, experts):
    ids_t = expert_ids.T
    onehot = (ids_t[:, :, None] == jnp.arange(experts, dtype=jnp.int32)).astype(jnp.int32)
    running = jnp.cumsum(onehot, axis=1)
    counts = running[:, -1, :]
    rank_local = jnp.sum(onehot * running, axis=2) - 1
    return ids_t, counts, rank_local


def padded_step(groups, token_rows, expert_ids, gate_weights, w_in, w_out):
    tokens, top_k = expert_ids.shape
    local_experts, model_dim = w_in.shape[0], w_in.shape[1]
    experts = local_experts * groups
    mean_load = tokens * top_k // experts
    send_cap = -(-(7 * mean_load // 4) // 16) * 16
    capacity = groups * mean_load
    rows_total = experts * send_cap
    ids_t, counts, rank_local = route_local(expert_ids, experts)
    inclusive = counts
    shift = 1
    while shift < groups:
        pairs_list = [(source, source + shift) for source in range(groups - shift)]
        inclusive = inclusive + lax.ppermute(inclusive, "expert", pairs_list)
        shift = shift * 2
    before = inclusive - counts
    totals = lax.psum(counts, "expert")
    prior = jnp.cumsum(totals, axis=0) - totals
    within = jnp.cumsum(counts, axis=0) - counts
    slot = jnp.take_along_axis(prior + before, ids_t, axis=1) + rank_local
    keep = slot < capacity
    target = ids_t * send_cap + jnp.take_along_axis(within, ids_t, axis=1) + rank_local
    token_ids = jnp.broadcast_to(jnp.arange(tokens, dtype=jnp.int32), (top_k, tokens))
    source_row = jnp.full((rows_total,), tokens, jnp.int32).at[jnp.where(keep, target, rows_total).reshape(-1)].set(token_ids.reshape(-1), mode="drop")
    padded = jnp.concatenate([token_rows, jnp.zeros((1, model_dim), token_rows.dtype)], axis=0)
    outbound = jnp.take(padded, source_row, axis=0).reshape(experts, send_cap, model_dim)
    inbound = lax.all_to_all(outbound, "expert", 0, 0, tiled=True).reshape(groups, local_experts, send_cap, model_dim)

    def one_expert(e, total):
        rows = lax.dynamic_index_in_dim(inbound, e, 1, keepdims=False).reshape(groups * send_cap, model_dim)
        hidden = jax.nn.gelu(jnp.dot(rows, w_in[e], preferred_element_type=jnp.float32)).astype(jnp.bfloat16)
        out = jnp.dot(hidden, w_out[e], preferred_element_type=jnp.float32).astype(jnp.bfloat16)
        return lax.dynamic_update_index_in_dim(total, out.reshape(groups, send_cap, model_dim), e, 1)

    expert_out = lax.fori_loop(0, local_experts, one_expert, jnp.zeros_like(inbound))
    returned = lax.all_to_all(expert_out.reshape(experts, send_cap, model_dim), "expert", 0, 0, tiled=True).reshape(rows_total, model_dim)
    picked = jnp.take(returned, target, axis=0)
    weight = jnp.where(keep, gate_weights.T, 0.0)
    mixed = jnp.sum(weight[:, :, None] * picked.astype(jnp.float32), axis=0)
    return (token_rows.astype(jnp.float32) + mixed).astype(jnp.bfloat16)


def block_rows(tokens, top_k, groups):
    mean = tokens * top_k // (groups * GROUPS)
    return (mean * 19 // 16 + 15) // 16 * 16


def dot_f32(a, b):
    return jnp.dot(a, b, preferred_element_type=jnp.float32)


def dot_nt(a, b):
    return lax.dot_general(a, b, (((1,), (1,)), ((), ())), preferred_element_type=jnp.float32)


def iota(shape, axis):
    return lax.broadcasted_iota(jnp.int32, shape, axis)


def as_bf16(mask):
    return jnp.where(mask, 1.0, 0.0).astype(jnp.bfloat16)


def pad_rows(rows, total):
    have = sum(r.shape[0] for r in rows)
    if have < total:
        rows = rows + [jnp.zeros((total - have, rows[0].shape[1]), rows[0].dtype)]
    return jnp.concatenate(rows, axis=0)


def local_positions(groups, rows, group_experts, ids_ref, hot, same, count_ref, rank_ref, pos_ref, pack_ref):
    tokens = ids_ref.shape[1]
    experts = hot.shape[1]
    blocks = tokens // LANES
    local_experts = experts // groups

    def fill(b, carry):
        at = pl.ds(pl.multiple_of(b * LANES, LANES), LANES)
        for j in range(2):
            hot[j, :, at] = as_bf16(iota((experts, LANES), 0) == ids_ref[j:j + 1, at])
        return carry

    lax.fori_loop(0, blocks, fill, 0)
    part = as_bf16(iota((blocks, tokens), 0) == iota((blocks, tokens), 1) // LANES)
    below = as_bf16(iota((blocks, blocks), 0) > iota((blocks, blocks), 1))
    base, count = [], []
    for j in range(2):
        per_block = dot_nt(part, hot[j])
        base.append(dot_f32(below, per_block.astype(jnp.bfloat16)))
        count.append(jnp.sum(per_block, axis=0, keepdims=True))
    count_ref[...] = pad_rows(count, 8)
    return base, count


def place_pairs(groups, rows, group_experts, base, count, ids_ref, hot, same, rank_ref, pos_ref, pack_ref):
    tokens = ids_ref.shape[1]
    experts = hot.shape[1]
    blocks = tokens // LANES
    local_experts = experts // groups
    both = pad_rows([count[0] + count[1]], 8)
    start = dot_f32(both.astype(jnp.bfloat16), same[...])[0:1]
    lane = iota((1, experts), 1)
    block_of = (lane % local_experts // group_experts) * groups + lane // local_experts
    first = (block_of * rows).astype(jnp.float32) + start
    earlier = iota((LANES, LANES), 0) < iota((LANES, LANES), 1)
    found = None
    table_rows = pack_ref.shape[0]
    for j in range(2):
        at = first if j == 0 else first + count[0]
        high = jnp.floor(at * (1.0 / 64.0))
        look = dot_f32(pad_rows([base[j], high, at - 64.0 * high], 32).astype(jnp.bfloat16), hot[j])
        for b in range(blocks):
            cols = slice(b * LANES, (b + 1) * LANES)
            row = ids_ref[j:j + 1, cols]
            wide = jnp.broadcast_to(row.astype(jnp.float32), (LANES, LANES))
            same_id = (wide.T == wide) & earlier
            rank = jnp.sum(jnp.where(same_id, 1.0, 0.0), axis=0, keepdims=True) + look[b:b + 1, cols]
            rank_ref[j:j + 1, cols] = rank
            pos_ref[j:j + 1, cols] = rank + 64.0 * look[blocks:blocks + 1, cols] + look[blocks + 1:blocks + 2, cols]
        pos = pos_ref[j:j + 1, :].astype(jnp.int32)
        token = iota((LANES, tokens), 1)
        high_t = as_bf16(iota((table_rows, tokens), 0) == pos // LANES)
        low = iota((LANES, tokens), 0) == pos % LANES
        low_hi = jnp.where(low, (token // 8).astype(jnp.float32), 0.0).astype(jnp.bfloat16)
        low_lo = jnp.where(low, (token % 8).astype(jnp.float32), 0.0).astype(jnp.bfloat16)
        hit = 8.0 * dot_nt(high_t, low_hi) + dot_nt(high_t, low_lo)
        found = hit if found is None else found + hit
    pack_ref[...] = jnp.clip(found.astype(jnp.int32), 0, tokens - 1)


def group_tables(me, groups, rows, group_experts, capacity, every, hot, same, rank_ref, pos_ref, lhs_ref, ret_ref, comb_ref, load_ref):
    experts = hot.shape[1]
    tokens = hot.shape[2]
    local_experts = experts // groups
    blocks = tokens // LANES
    c = [[every[s, j:j + 1, :] for s in range(groups)] for j in range(2)]
    both = pad_rows([c[0][s] + c[1][s] for s in range(groups)], 8)
    start = dot_f32(both.astype(jnp.bfloat16), same[...])
    load_ref[...] = jnp.broadcast_to(jnp.max(start + both), load_ref.shape)
    kept = [[None] * groups, [None] * groups]
    used = jnp.zeros((1, experts), jnp.float32)
    for j in range(2):
        for s in range(groups):
            kept[j][s] = jnp.clip(capacity - used, 0.0, c[j][s])
            used = used + c[j][s]
    lane = iota((1, experts), 1)
    in_group = lane % group_experts
    slot = jnp.zeros((1, experts), jnp.float32)
    slots, steps, edges, jumps = [], [], [], []
    last = jnp.zeros((1, experts), jnp.float32)
    for s in range(groups):
        ret_v = []
        for j in range(2):
            edge = start[s:s + 1] if j == 0 else start[s:s + 1] + c[0][s]
            v = s * rows + edge - slot
            slots.append(slot)
            steps.append(v - last)
            last = v
            edges.append(edge)
            ret_v.append((in_group * capacity).astype(jnp.float32) + slot - edge)
            slot = slot + kept[j][s]
        before = jnp.concatenate([jnp.zeros((1, 1), jnp.float32), ret_v[1][:, :-1]], axis=1)
        jumps.append(ret_v[0] - jnp.where(in_group == 0, 0.0, before))
        jumps.append(ret_v[1] - ret_v[0])

    def mine(parts):
        a = jnp.concatenate(parts, axis=0)
        total = jnp.zeros((a.shape[0], local_experts), jnp.float32)
        for d in range(groups):
            total = total + jnp.where(me == d, a[:, d * local_experts:(d + 1) * local_experts], 0.0)
        return total

    slots, steps, edges, jumps = mine(slots), mine(steps), mine(edges), mine(jumps)
    q = iota((capacity, local_experts), 0).astype(jnp.float32)
    lhs = q
    for i in range(2 * groups):
        lhs = lhs + jnp.where(q >= slots[i:i + 1], steps[i:i + 1], 0.0)
    lhs = jnp.clip(lhs.astype(jnp.int32), 0, groups * rows - 1)
    lhs_ref[...] = jnp.concatenate([lhs, jnp.zeros((capacity, LANES - local_experts), jnp.int32)], axis=1) if local_experts < LANES else lhs

    tall = pad_rows([edges, jumps], LANES)
    tall = jnp.concatenate([tall, jnp.zeros((LANES, LANES - local_experts), jnp.float32)], axis=1).T if local_experts < LANES else tall.T
    width = -(-rows // LANES) * LANES
    p = iota((1, width), 1).astype(jnp.float32)
    for g in range(GROUPS):
        part = tall[g * group_experts:(g + 1) * group_experts]
        for s in range(groups):
            total = jnp.zeros((group_experts, width), jnp.float32)
            for j in range(2):
                i = 2 * s + j
                total = total + jnp.where(p >= part[:, i:i + 1], part[:, 2 * groups + i:2 * groups + i + 1], 0.0)
            row = p + jnp.sum(total, axis=0, keepdims=True)
            row = jnp.clip(row.astype(jnp.int32), 0, group_experts * capacity - 1)
            for i in range(width // LANES):
                at = (g * groups + s) * (width // LANES) + i
                ret_ref[at:at + 1, :] = row[:, i * LANES:(i + 1) * LANES]

    for j in range(2):
        own = jnp.zeros((1, experts), jnp.float32)
        for s in range(groups):
            own = own + jnp.where(me == s, kept[j][s], 0.0)
        bound = dot_f32(pad_rows([own], 16).astype(jnp.bfloat16), hot[j])
        none = float(GROUPS * groups * rows)
        for b in range(blocks):
            cols = slice(b * LANES, (b + 1) * LANES)
            take = jnp.where(rank_ref[j:j + 1, cols] < bound[0:1, cols], pos_ref[j:j + 1, cols], none)
            comb_ref[j * blocks + b:j * blocks + b + 1, :] = jnp.clip(take.astype(jnp.int32), 0, GROUPS * groups * rows)


def exchange_kernel(
    groups, rows, capacity,
    gates, ids_ref, x_ref, win_ref, wout_ref, out_ref, load_ref,
    hot, same, count, every, rank_ref, pos_ref, pack_v, lhs_v, ret_v, comb_v, pack_idx, lhs_idx, ret_idx, comb_idx,
    xr_rows, send, recv, rf_rows, stage0, stage1, of_rows, rsend, rrecv, retf_rows, wi, wo,
    wsem, ssem, rsem, rssem, rrsem, csend, crecv, tsem,
):
    tokens, model_dim = x_ref.shape
    sub = model_dim // LANES
    local_experts = win_ref.shape[0]
    group_experts = local_experts // GROUPS
    me = lax.axis_index("expert")
    span = rows * sub
    stages = (stage0, stage1)
    xr, rf, of, retf = (r.reshape(r.shape[0] * sub, LANES) for r in (xr_rows, rf_rows, of_rows, retf_rows))

    def fetch(e, slot):
        a = pltpu.make_async_copy(win_ref.at[e], wi.at[slot], wsem.at[slot, 0])
        b = pltpu.make_async_copy(wout_ref.at[e], wo.at[slot], wsem.at[slot, 1])
        return a, b

    for e in range(BUFS):
        for c in fetch(e, e):
            c.start()
    barrier = pltpu.get_barrier_semaphore()
    for k in range(1, groups):
        pl.semaphore_signal(barrier, inc=1, device_id={"expert": lax.rem(me + k, groups)}, device_id_type=MESH)
    for k in range(sub):
        xr[pl.ds(k, tokens, stride=sub), :] = x_ref[:, k * LANES:(k + 1) * LANES].astype(jnp.float32)
    retf[pl.ds(GROUPS * groups * span, 8 * sub), :] = jnp.zeros((8 * sub, LANES), jnp.float32)
    experts = hot.shape[1]
    i_e, i_f = iota((experts, experts), 0), iota((experts, experts), 1)
    same[...] = as_bf16((i_e // group_experts == i_f // group_experts) & (i_e < i_f))
    base, counts = local_positions(groups, rows, group_experts, ids_ref, hot, same, count, rank_ref, pos_ref, pack_v)
    place_pairs(groups, rows, group_experts, base, counts, ids_ref, hot, same, rank_ref, pos_ref, pack_v)
    pack_copy = pltpu.make_async_copy(pack_v, pack_idx, tsem.at[0])
    pack_copy.start()
    pl.semaphore_wait(barrier, groups - 1)

    def count_copy(k):
        return pltpu.make_async_remote_copy(
            src_ref=count, dst_ref=every.at[me], send_sem=csend.at[k], recv_sem=crecv.at[k],
            device_id={"expert": lax.rem(me + k, groups)}, device_id_type=MESH)

    for k in range(1, groups):
        count_copy(k).start()
    pack_copy.wait()

    def gather_block(idx, first, table, dst):
        def body(c, carry):
            at = first + c * 16
            line, col = at // LANES, at % LANES
            got = [table[idx[line, col + r]] for r in range(16)]
            dst[pl.ds(pl.multiple_of(c * 16 * sub, 16 * sub), 16 * sub), :] = jnp.concatenate(got, axis=0).astype(jnp.bfloat16)
            return carry
        lax.fori_loop(0, rows // 16, body, 0)

    def widen(src, dst, first):
        def body(c, carry):
            part = pl.multiple_of(c * 16 * sub, 16 * sub)
            dst[pl.ds(pl.multiple_of(first + part, 16), 16 * sub), :] = src[pl.ds(part, 16 * sub), :].astype(jnp.float32)
            return carry
        lax.fori_loop(0, rows // 16, body, 0)

    def copy_to(src, dst, g, k, s_sem, r_sem):
        peer = lax.rem(me + k, groups)
        return pltpu.make_async_remote_copy(
            src_ref=src.at[g, peer], dst_ref=dst.at[g, me], send_sem=s_sem.at[g, k], recv_sem=r_sem.at[g, k],
            device_id={"expert": peer}, device_id_type=MESH)

    def send_blocks(g, idx, stride, table, src, dst, s_sem, r_sem):
        late = None
        for k in list(range(1, groups)) + [0]:
            peer = lax.rem(me + k, groups)
            gather_block(idx, (g * groups + peer) * stride, table, src.at[g, peer])
            if late is not None:
                late.start()
            late = copy_to(src, dst, g, k, s_sem, r_sem) if k else None

    def take_blocks(g, src, dst, own, first, s_sem, r_sem):
        for k in range(groups):
            peer = lax.rem(me - k + groups, groups)
            if k:
                pltpu.make_async_remote_copy(
                    src_ref=own.at[g, peer], dst_ref=src.at[g, peer], send_sem=s_sem.at[g, k], recv_sem=r_sem.at[g, k],
                    device_id={"expert": peer}, device_id_type=MESH).wait_recv()
                widen(src.at[g, peer], dst, first + peer * span)
            else:
                widen(own.at[g, peer], dst, first + peer * span)

    for g in range(GROUPS):
        send_blocks(g, pack_idx, rows, xr_rows, send, recv, ssem, rsem)

    every[me] = count[...]
    for k in range(1, groups):
        source = lax.rem(me - k + groups, groups)
        pltpu.make_async_remote_copy(
            src_ref=count, dst_ref=every.at[source], send_sem=csend.at[k], recv_sem=crecv.at[k],
            device_id={"expert": source}, device_id_type=MESH).wait_recv()
    group_tables(me, groups, rows, group_experts, capacity, every, hot, same, rank_ref, pos_ref, lhs_v, ret_v, comb_v, load_ref)
    tables = [pltpu.make_async_copy(a, b, tsem.at[i + 1]) for i, (a, b) in enumerate(((lhs_v, lhs_idx), (ret_v, ret_idx), (comb_v, comb_idx)))]
    for t in tables:
        t.start()
    for t in tables:
        t.wait()

    for g in range(GROUPS):
        take_blocks(g, recv, rf, send, 0, ssem, rsem)

        def gather_lhs(e, stage):
            for q in range(capacity):
                stage[pl.ds(q * sub, sub), :] = rf_rows[lhs_idx[q, e]]

        def ffn(e, stage):
            slot = lax.rem(e, BUFS)
            for c in fetch(e, slot):
                c.wait()
            lhs = jnp.concatenate([stage[pl.ds(k, capacity, stride=sub), :] for k in range(sub)], axis=1).astype(jnp.bfloat16)
            hidden = jax.nn.gelu(dot_f32(lhs, wi[slot])).astype(jnp.bfloat16)
            out = dot_f32(hidden, wo[slot]).astype(jnp.bfloat16).astype(jnp.float32)
            at = (e - g * group_experts) * capacity * sub
            for k in range(sub):
                of[pl.ds(at + k, capacity, stride=sub), :] = out[:, k * LANES:(k + 1) * LANES]

        def body(i, carry):
            for half in range(2):
                e = g * group_experts + i * 2 + half
                gather_lhs(e, stages[half])
                ffn(e, stages[half])

                @pl.when(e + BUFS < local_experts)
                def _():
                    for c in fetch(e + BUFS, lax.rem(e, BUFS)):
                        c.start()
            return carry

        lax.fori_loop(0, group_experts // 2, body, 0)
        send_blocks(g, ret_idx, -(-rows // LANES) * LANES, of_rows, rsend, rrecv, rssem, rrsem)

    for g in range(GROUPS):
        take_blocks(g, rrecv, retf, rsend, g * groups * span, rssem, rrsem)

    def combine(c, carry):
        got = []
        line, col = c // (LANES // 16), c % (LANES // 16) * 16
        for r in range(16):
            row = xr_rows[c * 16 + r]
            for j in range(2):
                row = row + gates[j * (tokens // LANES) + line, col + r] * retf_rows[comb_idx[j * (tokens // LANES) + line, col + r]]
            got.append(row)
        xr[pl.ds(pl.multiple_of(c * 16 * sub, 16 * sub), 16 * sub), :] = jnp.concatenate(got, axis=0)
        return carry

    lax.fori_loop(0, tokens // 16, combine, 0)
    for k in range(sub):
        out_ref[:, k * LANES:(k + 1) * LANES] = xr[pl.ds(k, tokens, stride=sub), :].astype(jnp.bfloat16)
    for g in range(GROUPS):
        for k in range(1, groups):
            if g == 0:
                count_copy(k).wait_send()
            copy_to(send, recv, g, k, ssem, rsem).wait_send()
            copy_to(rsend, rrecv, g, k, rssem, rrsem).wait_send()


def compact_step(groups, rows, capacity, gates, ids, token_rows, w_in, w_out):
    tokens, model_dim = token_rows.shape
    local_experts, _, hidden_dim = w_in.shape
    experts = local_experts * groups
    group_experts = local_experts // GROUPS
    sub = model_dim // LANES
    span = rows * sub
    smem = pl.BlockSpec(memory_space=pltpu.SMEM)
    vmem = pl.BlockSpec(memory_space=pltpu.VMEM)
    hbm = pl.BlockSpec(memory_space=pl.ANY)
    wire = pltpu.VMEM((GROUPS, groups, span, LANES), jnp.bfloat16)
    sems = pltpu.SemaphoreType.DMA((GROUPS, groups))
    table_rows = (
        -(-(GROUPS * groups * rows) // (8 * LANES)) * 8,
        capacity,
        GROUPS * groups * -(-rows // LANES),
        2 * tokens // LANES,
    )
    return pl.pallas_call(
        functools.partial(exchange_kernel, groups, rows, capacity),
        out_shape=(jax.ShapeDtypeStruct((tokens, model_dim), jnp.bfloat16), jax.ShapeDtypeStruct((8, LANES), jnp.float32)),
        in_specs=[smem, vmem, vmem, hbm, hbm],
        out_specs=(vmem, vmem),
        scratch_shapes=[
            pltpu.VMEM((2, experts, tokens), jnp.bfloat16),
            pltpu.VMEM((experts, experts), jnp.bfloat16),
            pltpu.VMEM((8, experts), jnp.float32),
            pltpu.VMEM((groups, 8, experts), jnp.float32),
            pltpu.VMEM((8, tokens), jnp.float32),
            pltpu.VMEM((8, tokens), jnp.float32),
            *[pltpu.VMEM((r, LANES), jnp.int32) for r in table_rows],
            *[pltpu.SMEM((r, LANES), jnp.int32) for r in table_rows],
            pltpu.VMEM((tokens, sub, LANES), jnp.float32),
            wire,
            wire,
            pltpu.VMEM((groups * rows, sub, LANES), jnp.float32),
            pltpu.VMEM((capacity * sub, LANES), jnp.float32),
            pltpu.VMEM((capacity * sub, LANES), jnp.float32),
            pltpu.VMEM((group_experts * capacity, sub, LANES), jnp.float32),
            wire,
            wire,
            pltpu.VMEM((GROUPS * groups * rows + 8, sub, LANES), jnp.float32),
            pltpu.VMEM((BUFS, model_dim, hidden_dim), jnp.bfloat16),
            pltpu.VMEM((BUFS, hidden_dim, model_dim), jnp.bfloat16),
            pltpu.SemaphoreType.DMA((BUFS, 2)),
            sems, sems, sems, sems,
            pltpu.SemaphoreType.DMA((groups,)),
            pltpu.SemaphoreType.DMA((groups,)),
            pltpu.SemaphoreType.DMA((4,)),
        ],
        compiler_params=pltpu.CompilerParams(collective_id=0, has_side_effects=True, vmem_limit_bytes=67043328),
        name="expert_exchange",
    )(gates, ids, token_rows, w_in, w_out)


def solution(mesh):
    groups = mesh.shape["expert"]
    row_spec = P(("data", "expert"), None)
    weight_spec = P("expert", None, None)

    def device_step(token_rows, expert_ids, gate_weights, w_in, w_out):
        tokens, top_k = expert_ids.shape
        local_experts = w_in.shape[0]
        capacity = tokens * top_k // local_experts
        rows = block_rows(tokens, top_k, groups)
        gates = gate_weights.T.reshape(-1, LANES)
        fast, load = compact_step(groups, rows, capacity, gates, expert_ids.T, token_rows, w_in, w_out)
        overflow = load[0, 0] > rows
        return lax.cond(
            overflow,
            lambda f: padded_step(groups, token_rows, expert_ids, gate_weights, w_in, w_out),
            lambda f: f,
            fast,
        )

    return jax.shard_map(device_step, mesh=mesh, in_specs=(row_spec, row_spec, row_spec, weight_spec, weight_spec), out_specs=row_spec, check_vma=False)
```

```python
import functools

import jax
import jax.numpy as jnp
from jax import lax
from jax.experimental import pallas as pl
from jax.experimental.pallas import tpu as pltpu
from jax.sharding import PartitionSpec as P

GROUPS = 2
BUFS = 3
LANES = 128
MESH = pl.DeviceIdType.MESH


def route_local(expert_ids, experts):
    ids_t = expert_ids.T
    onehot = (ids_t[:, :, None] == jnp.arange(experts, dtype=jnp.int32)).astype(jnp.int32)
    running = jnp.cumsum(onehot, axis=1)
    counts = running[:, -1, :]
    rank_local = jnp.sum(onehot * running, axis=2) - 1
    return ids_t, counts, rank_local


def padded_step(groups, token_rows, expert_ids, gate_weights, w_in, w_out):
    tokens, top_k = expert_ids.shape
    local_experts, model_dim = w_in.shape[0], w_in.shape[1]
    experts = local_experts * groups
    mean_load = tokens * top_k // experts
    send_cap = -(-(7 * mean_load // 4) // 16) * 16
    capacity = groups * mean_load
    rows_total = experts * send_cap
    ids_t, counts, rank_local = route_local(expert_ids, experts)
    inclusive = counts
    shift = 1
    while shift < groups:
        pairs_list = [(source, source + shift) for source in range(groups - shift)]
        inclusive = inclusive + lax.ppermute(inclusive, "expert", pairs_list)
        shift = shift * 2
    before = inclusive - counts
    totals = lax.psum(counts, "expert")
    prior = jnp.cumsum(totals, axis=0) - totals
    within = jnp.cumsum(counts, axis=0) - counts
    slot = jnp.take_along_axis(prior + before, ids_t, axis=1) + rank_local
    keep = slot < capacity
    target = ids_t * send_cap + jnp.take_along_axis(within, ids_t, axis=1) + rank_local
    token_ids = jnp.broadcast_to(jnp.arange(tokens, dtype=jnp.int32), (top_k, tokens))
    source_row = jnp.full((rows_total,), tokens, jnp.int32).at[jnp.where(keep, target, rows_total).reshape(-1)].set(token_ids.reshape(-1), mode="drop")
    padded = jnp.concatenate([token_rows, jnp.zeros((1, model_dim), token_rows.dtype)], axis=0)
    outbound = jnp.take(padded, source_row, axis=0).reshape(experts, send_cap, model_dim)
    inbound = lax.all_to_all(outbound, "expert", 0, 0, tiled=True).reshape(groups, local_experts, send_cap, model_dim)

    def one_expert(e, total):
        rows = lax.dynamic_index_in_dim(inbound, e, 1, keepdims=False).reshape(groups * send_cap, model_dim)
        hidden = jax.nn.gelu(jnp.dot(rows, w_in[e], preferred_element_type=jnp.float32)).astype(jnp.bfloat16)
        out = jnp.dot(hidden, w_out[e], preferred_element_type=jnp.float32).astype(jnp.bfloat16)
        return lax.dynamic_update_index_in_dim(total, out.reshape(groups, send_cap, model_dim), e, 1)

    expert_out = lax.fori_loop(0, local_experts, one_expert, jnp.zeros_like(inbound))
    returned = lax.all_to_all(expert_out.reshape(experts, send_cap, model_dim), "expert", 0, 0, tiled=True).reshape(rows_total, model_dim)
    picked = jnp.take(returned, target, axis=0)
    weight = jnp.where(keep, gate_weights.T, 0.0)
    mixed = jnp.sum(weight[:, :, None] * picked.astype(jnp.float32), axis=0)
    return (token_rows.astype(jnp.float32) + mixed).astype(jnp.bfloat16)


def block_rows(tokens, top_k, groups):
    mean = tokens * top_k // (groups * GROUPS)
    return (mean * 19 // 16 + 15) // 16 * 16


def dot_f32(a, b):
    return jnp.dot(a, b, preferred_element_type=jnp.float32)


def dot_nt(a, b):
    return lax.dot_general(a, b, (((1,), (1,)), ((), ())), preferred_element_type=jnp.float32)


def iota(shape, axis):
    return lax.broadcasted_iota(jnp.int32, shape, axis)


def as_bf16(mask):
    return jnp.where(mask, 1.0, 0.0).astype(jnp.bfloat16)


def pad_rows(rows, total):
    have = sum(r.shape[0] for r in rows)
    if have < total:
        rows = rows + [jnp.zeros((total - have, rows[0].shape[1]), rows[0].dtype)]
    return jnp.concatenate(rows, axis=0)


def local_positions(groups, rows, group_experts, ids_ref, hot, same, count_ref, rank_ref, pos_ref, pack_ref):
    tokens = ids_ref.shape[1]
    experts = hot.shape[1]
    blocks = tokens // LANES
    local_experts = experts // groups

    def fill(b, carry):
        at = pl.ds(pl.multiple_of(b * LANES, LANES), LANES)
        for j in range(2):
            hot[j, :, at] = as_bf16(iota((experts, LANES), 0) == ids_ref[j:j + 1, at])
        return carry

    lax.fori_loop(0, blocks, fill, 0)
    part = as_bf16(iota((blocks, tokens), 0) == iota((blocks, tokens), 1) // LANES)
    below = as_bf16(iota((blocks, blocks), 0) > iota((blocks, blocks), 1))
    base, count = [], []
    for j in range(2):
        per_block = dot_nt(part, hot[j])
        base.append(dot_f32(below, per_block.astype(jnp.bfloat16)))
        count.append(jnp.sum(per_block, axis=0, keepdims=True))
    count_ref[...] = pad_rows(count, 8)
    return base, count


def place_pairs(groups, rows, group_experts, base, count, ids_ref, hot, same, rank_ref, pos_ref, pack_ref):
    tokens = ids_ref.shape[1]
    experts = hot.shape[1]
    blocks = tokens // LANES
    local_experts = experts // groups
    both = pad_rows([count[0] + count[1]], 8)
    start = dot_f32(both.astype(jnp.bfloat16), same[...])[0:1]
    lane = iota((1, experts), 1)
    block_of = (lane % local_experts // group_experts) * groups + lane // local_experts
    stride = -(-rows // LANES) * LANES
    first = (block_of * stride).astype(jnp.float32) + start
    earlier = iota((LANES, LANES), 0) < iota((LANES, LANES), 1)
    found = None
    table_rows = pack_ref.shape[0]
    for j in range(2):
        at = first if j == 0 else first + count[0]
        high = jnp.floor(at * (1.0 / 64.0))
        look = dot_f32(pad_rows([base[j], high, at - 64.0 * high], 32).astype(jnp.bfloat16), hot[j])
        for b in range(blocks):
            cols = slice(b * LANES, (b + 1) * LANES)
            row = ids_ref[j:j + 1, cols]
            wide = jnp.broadcast_to(row.astype(jnp.float32), (LANES, LANES))
            same_id = (wide.T == wide) & earlier
            rank = jnp.sum(jnp.where(same_id, 1.0, 0.0), axis=0, keepdims=True) + look[b:b + 1, cols]
            rank_ref[j:j + 1, cols] = rank
            pos_ref[j:j + 1, cols] = rank + 64.0 * look[blocks:blocks + 1, cols] + look[blocks + 1:blocks + 2, cols]
        pos = pos_ref[j:j + 1, :]
        pos_ref[j:j + 1, :] = pos - (stride - rows) * jnp.floor((pos + 0.5) * (1.0 / stride))
        pos = pos.astype(jnp.int32)
        token = iota((LANES, tokens), 1)
        high_t = as_bf16(iota((table_rows, tokens), 0) == pos // LANES)
        low = iota((LANES, tokens), 0) == pos % LANES
        low_hi = jnp.where(low, (token // 8).astype(jnp.float32), 0.0).astype(jnp.bfloat16)
        low_lo = jnp.where(low, (token % 8).astype(jnp.float32), 0.0).astype(jnp.bfloat16)
        hit = 8.0 * dot_nt(high_t, low_hi) + dot_nt(high_t, low_lo)
        found = hit if found is None else found + hit
    pack_ref[...] = jnp.clip(found.astype(jnp.int32), 0, tokens - 1)


def group_tables(me, groups, rows, group_experts, capacity, every, hot, same, rank_ref, pos_ref, lhs_ref, ret_ref, comb_ref, load_ref):
    experts = hot.shape[1]
    tokens = hot.shape[2]
    local_experts = experts // groups
    blocks = tokens // LANES
    c = [[every[s, j:j + 1, :] for s in range(groups)] for j in range(2)]
    both = pad_rows([c[0][s] + c[1][s] for s in range(groups)], 8)
    start = dot_f32(both.astype(jnp.bfloat16), same[...])
    load_ref[...] = jnp.broadcast_to(jnp.max(start + both), load_ref.shape)
    kept = [[None] * groups, [None] * groups]
    used = jnp.zeros((1, experts), jnp.float32)
    for j in range(2):
        for s in range(groups):
            kept[j][s] = jnp.clip(capacity - used, 0.0, c[j][s])
            used = used + c[j][s]
    lane = iota((1, experts), 1)
    in_group = lane % group_experts
    slot = jnp.zeros((1, experts), jnp.float32)
    slots, steps, edges, jumps = [], [], [], []
    last = jnp.zeros((1, experts), jnp.float32)
    for s in range(groups):
        ret_v = []
        for j in range(2):
            edge = start[s:s + 1] if j == 0 else start[s:s + 1] + c[0][s]
            v = s * rows + edge - slot
            slots.append(slot)
            steps.append(v - last)
            last = v
            edges.append(edge)
            ret_v.append((in_group * capacity).astype(jnp.float32) + slot - edge)
            slot = slot + kept[j][s]
        before = jnp.concatenate([jnp.zeros((1, 1), jnp.float32), ret_v[1][:, :-1]], axis=1)
        jumps.append(ret_v[0] - jnp.where(in_group == 0, 0.0, before))
        jumps.append(ret_v[1] - ret_v[0])

    def mine(parts):
        a = jnp.concatenate(parts, axis=0)
        total = jnp.zeros((a.shape[0], local_experts), jnp.float32)
        for d in range(groups):
            total = total + jnp.where(me == d, a[:, d * local_experts:(d + 1) * local_experts], 0.0)
        return total

    slots, steps, edges, jumps = mine(slots), mine(steps), mine(edges), mine(jumps)
    tall = pad_rows([edges, jumps, slots, steps], LANES)
    tall = jnp.concatenate([tall, jnp.zeros((LANES, LANES - local_experts), jnp.float32)], axis=1).T if local_experts < LANES else tall.T
    q = iota((local_experts, LANES), 1).astype(jnp.float32)
    lhs = q
    for i in range(2 * groups):
        at = 4 * groups + i
        lhs = lhs + jnp.where(q >= tall[:local_experts, at:at + 1], tall[:local_experts, at + 2 * groups:at + 2 * groups + 1], 0.0)
    lhs_ref[...] = jnp.clip(lhs.astype(jnp.int32), 0, groups * rows - 1)

    width = -(-rows // LANES) * LANES
    p = iota((1, width), 1).astype(jnp.float32)
    for g in range(GROUPS):
        part = tall[g * group_experts:(g + 1) * group_experts]
        for s in range(groups):
            total = jnp.zeros((group_experts, width), jnp.float32)
            for j in range(2):
                i = 2 * s + j
                total = total + jnp.where(p >= part[:, i:i + 1], part[:, 2 * groups + i:2 * groups + i + 1], 0.0)
            row = p + jnp.sum(total, axis=0, keepdims=True)
            row = jnp.clip(row.astype(jnp.int32), 0, group_experts * capacity - 1)
            for i in range(width // LANES):
                at = (g * groups + s) * (width // LANES) + i
                ret_ref[at:at + 1, :] = row[:, i * LANES:(i + 1) * LANES]

    for j in range(2):
        own = jnp.zeros((1, experts), jnp.float32)
        for s in range(groups):
            own = own + jnp.where(me == s, kept[j][s], 0.0)
        bound = dot_f32(pad_rows([own], 16).astype(jnp.bfloat16), hot[j])
        none = float(GROUPS * groups * rows)
        for b in range(blocks):
            cols = slice(b * LANES, (b + 1) * LANES)
            take = jnp.where(rank_ref[j:j + 1, cols] < bound[0:1, cols], pos_ref[j:j + 1, cols], none)
            comb_ref[j * blocks + b:j * blocks + b + 1, :] = jnp.clip(take.astype(jnp.int32), 0, GROUPS * groups * rows)


def exchange_kernel(
    groups, rows, capacity,
    gates_ref, ids_ref, x_ref, win_ref, wout_ref, out_ref, load_ref,
    hot, same, count, every, rank_ref, pos_ref, pack_v, lhs_v, ret_v, comb_v, gates_v, pack_idx, lhs_idx, ret_idx, comb_idx, gates,
    xr_rows, send, recv, rf_rows, stage0, stage1, of_rows, rsend, rrecv, retf_rows, wi, wo,
    wsem, ssem, rsem, rssem, rrsem, csend, crecv, tsem,
):
    tokens, model_dim = x_ref.shape
    sub = model_dim // LANES
    local_experts = win_ref.shape[0]
    group_experts = local_experts // GROUPS
    me = lax.axis_index("expert")
    span = rows * sub
    stages = (stage0, stage1)
    xr, rf, of, retf = (r.reshape(r.shape[0] * sub, LANES) for r in (xr_rows, rf_rows, of_rows, retf_rows))

    def fetch(e, slot):
        a = pltpu.make_async_copy(win_ref.at[e], wi.at[slot], wsem.at[slot, 0])
        b = pltpu.make_async_copy(wout_ref.at[e], wo.at[slot], wsem.at[slot, 1])
        return a, b

    for e in range(BUFS):
        for c in fetch(e, e):
            c.start()
    barrier = pltpu.get_barrier_semaphore()
    for k in range(1, groups):
        pl.semaphore_signal(barrier, inc=1, device_id={"expert": lax.rem(me + k, groups)}, device_id_type=MESH)
    for k in range(sub):
        xr[pl.ds(k, tokens, stride=sub), :] = x_ref[:, k * LANES:(k + 1) * LANES].astype(jnp.float32)
    retf[pl.ds(GROUPS * groups * span, 8 * sub), :] = jnp.zeros((8 * sub, LANES), jnp.float32)
    experts = hot.shape[1]
    i_e, i_f = iota((experts, experts), 0), iota((experts, experts), 1)
    same[...] = as_bf16((i_e // group_experts == i_f // group_experts) & (i_e < i_f))
    base, counts = local_positions(groups, rows, group_experts, ids_ref, hot, same, count, rank_ref, pos_ref, pack_v)
    place_pairs(groups, rows, group_experts, base, counts, ids_ref, hot, same, rank_ref, pos_ref, pack_v)
    pack_copy = pltpu.make_async_copy(pack_v, pack_idx, tsem.at[0])
    pack_copy.start()
    pl.semaphore_wait(barrier, groups - 1)

    def count_copy(k):
        return pltpu.make_async_remote_copy(
            src_ref=count, dst_ref=every.at[me], send_sem=csend.at[k], recv_sem=crecv.at[k],
            device_id={"expert": lax.rem(me + k, groups)}, device_id_type=MESH)

    for k in range(1, groups):
        count_copy(k).start()
    pack_copy.wait()

    lines, rest = divmod(rows, LANES)

    def gather_block(idx, line, table, dst):
        def some(at, first, count):
            for c in range(count // 16):
                got = [table[idx[at, c * 16 + r]] for r in range(16)]
                dst[pl.ds(pl.multiple_of((first + c * 16) * sub, 16 * sub), 16 * sub), :] = jnp.concatenate(got, axis=0).astype(jnp.bfloat16)

        def body(i, carry):
            some(line + i, i * LANES, LANES)
            return carry

        lax.fori_loop(0, lines, body, 0)
        if rest:
            some(line + lines, lines * LANES, rest)

    def widen(src, dst, first):
        def body(c, carry):
            part = pl.multiple_of(c * 16 * sub, 16 * sub)
            dst[pl.ds(pl.multiple_of(first + part, 16), 16 * sub), :] = src[pl.ds(part, 16 * sub), :].astype(jnp.float32)
            return carry
        lax.fori_loop(0, rows // 16, body, 0)

    def copy_to(src, dst, g, k, s_sem, r_sem):
        peer = lax.rem(me + k, groups)
        return pltpu.make_async_remote_copy(
            src_ref=src.at[g, peer], dst_ref=dst.at[g, me], send_sem=s_sem.at[g, k], recv_sem=r_sem.at[g, k],
            device_id={"expert": peer}, device_id_type=MESH)

    def send_blocks(g, idx, table, src, dst, s_sem, r_sem):
        def body(i, carry):
            peer = lax.rem(me + i + 1, groups)
            gather_block(idx, (g * groups + peer) * (lines + (rest > 0)), table, src.at[g, peer])

            @pl.when(i >= 1)
            def _():
                copy_to(src, dst, g, i, s_sem, r_sem).start()

            return carry

        lax.fori_loop(0, groups, body, 0)

    def take_blocks(g, src, dst, own, first, s_sem, r_sem):
        widen(own.at[g, me], dst, first + me * span)

        def body(k, carry):
            peer = lax.rem(me - k + groups, groups)
            pltpu.make_async_remote_copy(
                src_ref=own.at[g, peer], dst_ref=src.at[g, peer], send_sem=s_sem.at[g, k], recv_sem=r_sem.at[g, k],
                device_id={"expert": peer}, device_id_type=MESH).wait_recv()
            widen(src.at[g, peer], dst, first + peer * span)
            return carry

        lax.fori_loop(1, groups, body, 0)

    for g in range(GROUPS):
        send_blocks(g, pack_idx, xr_rows, send, recv, ssem, rsem)

    every[me] = count[...]
    for j in range(2):
        for b in range(tokens // LANES):
            gates_v[j * (tokens // LANES) + b:j * (tokens // LANES) + b + 1, :] = gates_ref[j:j + 1, b * LANES:(b + 1) * LANES]
    for k in range(1, groups):
        source = lax.rem(me - k + groups, groups)
        pltpu.make_async_remote_copy(
            src_ref=count, dst_ref=every.at[source], send_sem=csend.at[k], recv_sem=crecv.at[k],
            device_id={"expert": source}, device_id_type=MESH).wait_recv()
    group_tables(me, groups, rows, group_experts, capacity, every, hot, same, rank_ref, pos_ref, lhs_v, ret_v, comb_v, load_ref)
    tables = [pltpu.make_async_copy(a, b, tsem.at[i + 1]) for i, (a, b) in enumerate(((lhs_v, lhs_idx), (ret_v, ret_idx), (comb_v, comb_idx), (gates_v, gates)))]
    for t in tables:
        t.start()
    for t in tables:
        t.wait()

    for g in range(GROUPS):
        take_blocks(g, recv, rf, send, 0, ssem, rsem)

        def gather_lhs(e, stage):
            for q in range(capacity):
                stage[pl.ds(q * sub, sub), :] = rf_rows[lhs_idx[e, q]]

        def ffn(e, stage):
            slot = lax.rem(e, BUFS)
            for c in fetch(e, slot):
                c.wait()
            lhs = jnp.concatenate([stage[pl.ds(k, capacity, stride=sub), :] for k in range(sub)], axis=1).astype(jnp.bfloat16)
            hidden = jax.nn.gelu(dot_f32(lhs, wi[slot])).astype(jnp.bfloat16)
            out = dot_f32(hidden, wo[slot]).astype(jnp.bfloat16).astype(jnp.float32)
            at = (e - g * group_experts) * capacity * sub
            for k in range(sub):
                of[pl.ds(at + k, capacity, stride=sub), :] = out[:, k * LANES:(k + 1) * LANES]

        def body(i, carry):
            for half in range(2):
                e = g * group_experts + i * 2 + half
                gather_lhs(e, stages[half])
                ffn(e, stages[half])

                @pl.when(e + BUFS < local_experts)
                def _():
                    for c in fetch(e + BUFS, lax.rem(e, BUFS)):
                        c.start()
            return carry

        lax.fori_loop(0, group_experts // 2, body, 0)
        send_blocks(g, ret_idx, of_rows, rsend, rrecv, rssem, rrsem)

    for g in range(GROUPS):
        take_blocks(g, rrecv, retf, rsend, g * groups * span, rssem, rrsem)

    half = tokens // LANES

    def combine(line, carry):
        for c in range(LANES // 16):
            got = []
            for r in range(16):
                col = c * 16 + r
                row = xr_rows[line * LANES + col]
                for j in range(2):
                    row = row + gates[j * half + line, col] * retf_rows[comb_idx[j * half + line, col]]
                got.append(row)
            xr[pl.ds(pl.multiple_of((line * LANES + c * 16) * sub, 16 * sub), 16 * sub), :] = jnp.concatenate(got, axis=0)
        return carry

    lax.fori_loop(0, half, combine, 0)
    for k in range(sub):
        out_ref[:, k * LANES:(k + 1) * LANES] = xr[pl.ds(k, tokens, stride=sub), :].astype(jnp.bfloat16)
    for g in range(GROUPS):
        for k in range(1, groups):
            if g == 0:
                count_copy(k).wait_send()
            copy_to(send, recv, g, k, ssem, rsem).wait_send()
            copy_to(rsend, rrecv, g, k, rssem, rrsem).wait_send()


def compact_step(groups, rows, capacity, gates, ids, token_rows, w_in, w_out):
    tokens, model_dim = token_rows.shape
    local_experts, _, hidden_dim = w_in.shape
    experts = local_experts * groups
    group_experts = local_experts // GROUPS
    sub = model_dim // LANES
    span = rows * sub
    vmem = pl.BlockSpec(memory_space=pltpu.VMEM)
    hbm = pl.BlockSpec(memory_space=pl.ANY)
    wire = pltpu.VMEM((GROUPS, groups, span, LANES), jnp.bfloat16)
    sems = pltpu.SemaphoreType.DMA((GROUPS, groups))
    table_rows = (
        GROUPS * groups * -(-rows // LANES),
        local_experts,
        GROUPS * groups * -(-rows // LANES),
        2 * tokens // LANES,
    )
    return pl.pallas_call(
        functools.partial(exchange_kernel, groups, rows, capacity),
        out_shape=(jax.ShapeDtypeStruct((tokens, model_dim), jnp.bfloat16), jax.ShapeDtypeStruct((8, LANES), jnp.float32)),
        in_specs=[vmem, vmem, vmem, hbm, hbm],
        out_specs=(vmem, vmem),
        scratch_shapes=[
            pltpu.VMEM((2, experts, tokens), jnp.bfloat16),
            pltpu.VMEM((experts, experts), jnp.bfloat16),
            pltpu.VMEM((8, experts), jnp.float32),
            pltpu.VMEM((groups, 8, experts), jnp.float32),
            pltpu.VMEM((8, tokens), jnp.float32),
            pltpu.VMEM((8, tokens), jnp.float32),
            *[pltpu.VMEM((r, LANES), jnp.int32) for r in table_rows],
            pltpu.VMEM((2 * tokens // LANES, LANES), jnp.float32),
            *[pltpu.SMEM((r, LANES), jnp.int32) for r in table_rows],
            pltpu.SMEM((2 * tokens // LANES, LANES), jnp.float32),
            pltpu.VMEM((tokens, sub, LANES), jnp.float32),
            wire,
            wire,
            pltpu.VMEM((groups * rows, sub, LANES), jnp.float32),
            pltpu.VMEM((capacity * sub, LANES), jnp.float32),
            pltpu.VMEM((capacity * sub, LANES), jnp.float32),
            pltpu.VMEM((group_experts * capacity, sub, LANES), jnp.float32),
            wire,
            wire,
            pltpu.VMEM((GROUPS * groups * rows + 8, sub, LANES), jnp.float32),
            pltpu.VMEM((BUFS, model_dim, hidden_dim), jnp.bfloat16),
            pltpu.VMEM((BUFS, hidden_dim, model_dim), jnp.bfloat16),
            pltpu.SemaphoreType.DMA((BUFS, 2)),
            sems, sems, sems, sems,
            pltpu.SemaphoreType.DMA((groups,)),
            pltpu.SemaphoreType.DMA((groups,)),
            pltpu.SemaphoreType.DMA((5,)),
        ],
        compiler_params=pltpu.CompilerParams(collective_id=0, has_side_effects=True, vmem_limit_bytes=67043328),
        name="expert_exchange",
    )(gates, ids, token_rows, w_in, w_out)


def solution(mesh):
    groups = mesh.shape["expert"]
    row_spec = P(("data", "expert"), None)
    weight_spec = P("expert", None, None)

    def device_step(token_rows, expert_ids, gate_weights, w_in, w_out):
        tokens, top_k = expert_ids.shape
        local_experts = w_in.shape[0]
        capacity = tokens * top_k // local_experts
        rows = block_rows(tokens, top_k, groups)
        fast, load = compact_step(groups, rows, capacity, gate_weights.T, expert_ids.T, token_rows, w_in, w_out)
        overflow = load[0, 0] > rows
        general = lambda state: (jnp.array(False), padded_step(groups, token_rows, expert_ids, gate_weights, w_in, w_out))
        return lax.while_loop(lambda state: state[0], general, (overflow, fast))[1]

    return jax.shard_map(device_step, mesh=mesh, in_specs=(row_spec, row_spec, row_spec, weight_spec, weight_spec), out_specs=row_spec, check_vma=False)
```

```python
import functools

import jax
import jax.numpy as jnp
from jax import lax
from jax.experimental import pallas as pl
from jax.experimental.pallas import tpu as pltpu
from jax.sharding import PartitionSpec as P

GROUPS = 2
BUFS = 3
LANES = 128
MESH = pl.DeviceIdType.MESH


def route_local(expert_ids, experts):
    ids_t = expert_ids.T
    onehot = (ids_t[:, :, None] == jnp.arange(experts, dtype=jnp.int32)).astype(jnp.int32)
    running = jnp.cumsum(onehot, axis=1)
    counts = running[:, -1, :]
    rank_local = jnp.sum(onehot * running, axis=2) - 1
    return ids_t, counts, rank_local


def padded_step(groups, token_rows, expert_ids, gate_weights, w_in, w_out):
    tokens, top_k = expert_ids.shape
    local_experts, model_dim = w_in.shape[0], w_in.shape[1]
    experts = local_experts * groups
    mean_load = tokens * top_k // experts
    send_cap = -(-(7 * mean_load // 4) // 16) * 16
    capacity = groups * mean_load
    rows_total = experts * send_cap
    ids_t, counts, rank_local = route_local(expert_ids, experts)
    inclusive = counts
    shift = 1
    while shift < groups:
        pairs_list = [(source, source + shift) for source in range(groups - shift)]
        inclusive = inclusive + lax.ppermute(inclusive, "expert", pairs_list)
        shift = shift * 2
    before = inclusive - counts
    totals = lax.psum(counts, "expert")
    prior = jnp.cumsum(totals, axis=0) - totals
    within = jnp.cumsum(counts, axis=0) - counts
    slot = jnp.take_along_axis(prior + before, ids_t, axis=1) + rank_local
    keep = slot < capacity
    target = ids_t * send_cap + jnp.take_along_axis(within, ids_t, axis=1) + rank_local
    token_ids = jnp.broadcast_to(jnp.arange(tokens, dtype=jnp.int32), (top_k, tokens))
    source_row = jnp.full((rows_total,), tokens, jnp.int32).at[jnp.where(keep, target, rows_total).reshape(-1)].set(token_ids.reshape(-1), mode="drop")
    padded = jnp.concatenate([token_rows, jnp.zeros((1, model_dim), token_rows.dtype)], axis=0)
    outbound = jnp.take(padded, source_row, axis=0).reshape(experts, send_cap, model_dim)
    inbound = lax.all_to_all(outbound, "expert", 0, 0, tiled=True).reshape(groups, local_experts, send_cap, model_dim)

    def one_expert(e, total):
        rows = lax.dynamic_index_in_dim(inbound, e, 1, keepdims=False).reshape(groups * send_cap, model_dim)
        hidden = jax.nn.gelu(jnp.dot(rows, w_in[e], preferred_element_type=jnp.float32)).astype(jnp.bfloat16)
        out = jnp.dot(hidden, w_out[e], preferred_element_type=jnp.float32).astype(jnp.bfloat16)
        return lax.dynamic_update_index_in_dim(total, out.reshape(groups, send_cap, model_dim), e, 1)

    expert_out = lax.fori_loop(0, local_experts, one_expert, jnp.zeros_like(inbound))
    returned = lax.all_to_all(expert_out.reshape(experts, send_cap, model_dim), "expert", 0, 0, tiled=True).reshape(rows_total, model_dim)
    picked = jnp.take(returned, target, axis=0)
    weight = jnp.where(keep, gate_weights.T, 0.0)
    mixed = jnp.sum(weight[:, :, None] * picked.astype(jnp.float32), axis=0)
    return (token_rows.astype(jnp.float32) + mixed).astype(jnp.bfloat16)


def block_rows(tokens, top_k, groups):
    mean = tokens * top_k // (groups * GROUPS)
    return (mean * 19 // 16 + 15) // 16 * 16


def dot_f32(a, b):
    return jnp.dot(a, b, preferred_element_type=jnp.float32)


def dot_nt(a, b):
    return lax.dot_general(a, b, (((1,), (1,)), ((), ())), preferred_element_type=jnp.float32)


def iota(shape, axis):
    return lax.broadcasted_iota(jnp.int32, shape, axis)


def as_bf16(mask):
    return jnp.where(mask, 1.0, 0.0).astype(jnp.bfloat16)


def pad_rows(rows, total):
    have = sum(r.shape[0] for r in rows)
    if have < total:
        rows = rows + [jnp.zeros((total - have, rows[0].shape[1]), rows[0].dtype)]
    return jnp.concatenate(rows, axis=0)


def local_positions(groups, rows, group_experts, ids_ref, hot, same, count_ref, rank_ref, pos_ref, pack_ref):
    tokens = ids_ref.shape[1]
    experts = hot.shape[1]
    blocks = tokens // LANES
    local_experts = experts // groups

    def fill(b, carry):
        at = pl.ds(pl.multiple_of(b * LANES, LANES), LANES)
        for j in range(2):
            hot[j, :, at] = as_bf16(iota((experts, LANES), 0) == ids_ref[j:j + 1, at])
        return carry

    lax.fori_loop(0, blocks, fill, 0)
    part = as_bf16(iota((blocks, tokens), 0) == iota((blocks, tokens), 1) // LANES)
    below = as_bf16(iota((blocks, blocks), 0) > iota((blocks, blocks), 1))
    base, count = [], []
    for j in range(2):
        per_block = dot_nt(part, hot[j])
        base.append(dot_f32(below, per_block.astype(jnp.bfloat16)))
        count.append(jnp.sum(per_block, axis=0, keepdims=True))
    count_ref[...] = pad_rows(count, 8)
    return base, count


def place_pairs(groups, rows, group_experts, base, count, ids_ref, hot, same, rank_ref, pos_ref, pack_ref):
    tokens = ids_ref.shape[1]
    experts = hot.shape[1]
    blocks = tokens // LANES
    local_experts = experts // groups
    both = pad_rows([count[0] + count[1]], 8)
    start = dot_f32(both.astype(jnp.bfloat16), same[...])[0:1]
    lane = iota((1, experts), 1)
    block_of = (lane % local_experts // group_experts) * groups + lane // local_experts
    stride = -(-rows // LANES) * LANES
    first = (block_of * stride).astype(jnp.float32) + start
    earlier = iota((LANES, LANES), 0) < iota((LANES, LANES), 1)
    found = None
    table_rows = pack_ref.shape[0]
    for j in range(2):
        at = first if j == 0 else first + count[0]
        high = jnp.floor(at * (1.0 / 64.0))
        look = dot_f32(pad_rows([base[j], high, at - 64.0 * high], 32).astype(jnp.bfloat16), hot[j])
        for b in range(blocks):
            cols = slice(b * LANES, (b + 1) * LANES)
            row = ids_ref[j:j + 1, cols]
            wide = jnp.broadcast_to(row.astype(jnp.float32), (LANES, LANES))
            same_id = (wide.T == wide) & earlier
            rank = jnp.sum(jnp.where(same_id, 1.0, 0.0), axis=0, keepdims=True) + look[b:b + 1, cols]
            rank_ref[j:j + 1, cols] = rank
            pos_ref[j:j + 1, cols] = rank + 64.0 * look[blocks:blocks + 1, cols] + look[blocks + 1:blocks + 2, cols]
        pos = pos_ref[j:j + 1, :]
        pos_ref[j:j + 1, :] = pos - (stride - rows) * jnp.floor((pos + 0.5) * (1.0 / stride))
        pos = pos.astype(jnp.int32)
        token = iota((LANES, tokens), 1)
        high_t = as_bf16(iota((table_rows, tokens), 0) == pos // LANES)
        low = iota((LANES, tokens), 0) == pos % LANES
        low_hi = jnp.where(low, (token // 8).astype(jnp.float32), 0.0).astype(jnp.bfloat16)
        low_lo = jnp.where(low, (token % 8).astype(jnp.float32), 0.0).astype(jnp.bfloat16)
        hit = 8.0 * dot_nt(high_t, low_hi) + dot_nt(high_t, low_lo)
        found = hit if found is None else found + hit
    pack_ref[...] = jnp.clip(found.astype(jnp.int32), 0, tokens - 1)


def group_tables(me, groups, rows, group_experts, capacity, every, hot, same, rank_ref, pos_ref, lhs_ref, ret_ref, comb_ref, load_ref):
    experts = hot.shape[1]
    tokens = hot.shape[2]
    local_experts = experts // groups
    blocks = tokens // LANES
    c = [[every[s, j:j + 1, :] for s in range(groups)] for j in range(2)]
    both = pad_rows([c[0][s] + c[1][s] for s in range(groups)], 8)
    start = dot_f32(both.astype(jnp.bfloat16), same[...])
    load_ref[...] = jnp.broadcast_to(jnp.max(start + both), load_ref.shape)
    kept = [[None] * groups, [None] * groups]
    used = jnp.zeros((1, experts), jnp.float32)
    for j in range(2):
        for s in range(groups):
            kept[j][s] = jnp.clip(capacity - used, 0.0, c[j][s])
            used = used + c[j][s]
    lane = iota((1, experts), 1)
    in_group = lane % group_experts
    slot = jnp.zeros((1, experts), jnp.float32)
    slots, steps, edges, jumps = [], [], [], []
    last = jnp.zeros((1, experts), jnp.float32)
    for s in range(groups):
        ret_v = []
        for j in range(2):
            edge = start[s:s + 1] if j == 0 else start[s:s + 1] + c[0][s]
            v = s * rows + edge - slot
            slots.append(slot)
            steps.append(v - last)
            last = v
            edges.append(edge)
            ret_v.append((in_group * capacity).astype(jnp.float32) + slot - edge)
            slot = slot + kept[j][s]
        before = jnp.concatenate([jnp.zeros((1, 1), jnp.float32), ret_v[1][:, :-1]], axis=1)
        jumps.append(ret_v[0] - jnp.where(in_group == 0, 0.0, before))
        jumps.append(ret_v[1] - ret_v[0])

    def mine(parts):
        a = jnp.concatenate(parts, axis=0)
        total = jnp.zeros((a.shape[0], local_experts), jnp.float32)
        for d in range(groups):
            total = total + jnp.where(me == d, a[:, d * local_experts:(d + 1) * local_experts], 0.0)
        return total

    slots, steps, edges, jumps = mine(slots), mine(steps), mine(edges), mine(jumps)
    tall = pad_rows([edges, jumps, slots, steps], LANES)
    tall = jnp.concatenate([tall, jnp.zeros((LANES, LANES - local_experts), jnp.float32)], axis=1).T if local_experts < LANES else tall.T
    q = iota((local_experts, LANES), 1).astype(jnp.float32)
    lhs = q
    for i in range(2 * groups):
        at = 4 * groups + i
        lhs = lhs + jnp.where(q >= tall[:local_experts, at:at + 1], tall[:local_experts, at + 2 * groups:at + 2 * groups + 1], 0.0)
    lhs_ref[...] = jnp.clip(lhs.astype(jnp.int32), 0, groups * rows - 1)

    width = -(-rows // LANES) * LANES
    p = iota((1, width), 1).astype(jnp.float32)
    for g in range(GROUPS):
        part = tall[g * group_experts:(g + 1) * group_experts]
        for s in range(groups):
            total = jnp.zeros((group_experts, width), jnp.float32)
            for j in range(2):
                i = 2 * s + j
                total = total + jnp.where(p >= part[:, i:i + 1], part[:, 2 * groups + i:2 * groups + i + 1], 0.0)
            row = p + jnp.sum(total, axis=0, keepdims=True)
            row = jnp.clip(row.astype(jnp.int32), 0, group_experts * capacity - 1)
            for i in range(width // LANES):
                at = (g * groups + s) * (width // LANES) + i
                ret_ref[at:at + 1, :] = row[:, i * LANES:(i + 1) * LANES]

    for j in range(2):
        own = jnp.zeros((1, experts), jnp.float32)
        for s in range(groups):
            own = own + jnp.where(me == s, kept[j][s], 0.0)
        bound = dot_f32(pad_rows([own], 16).astype(jnp.bfloat16), hot[j])
        none = float(GROUPS * groups * rows)
        for b in range(blocks):
            cols = slice(b * LANES, (b + 1) * LANES)
            take = jnp.where(rank_ref[j:j + 1, cols] < bound[0:1, cols], pos_ref[j:j + 1, cols], none)
            comb_ref[j * blocks + b:j * blocks + b + 1, :] = jnp.clip(take.astype(jnp.int32), 0, GROUPS * groups * rows)


def exchange_kernel(
    groups, rows, capacity,
    gates_ref, ids_ref, x_hbm, win_ref, wout_ref, out_hbm, load_ref,
    hot, same, count, every, rank_ref, pos_ref, pack_v, lhs_v, ret_v, comb_v, pack_idx, lhs_idx, ret_idx, comb_idx, wide_gates, x_ref,
    xr_rows, send, recv, rf_rows, stage0, stage1, of_rows, rsend, rrecv, retf_rows, wi, wo,
    wsem, ssem, rsem, rssem, rrsem, csend, crecv, tsem, osem,
):
    tokens, model_dim = x_hbm.shape
    sub = model_dim // LANES
    local_experts = win_ref.shape[0]
    group_experts = local_experts // GROUPS
    me = lax.axis_index("expert")
    span = rows * sub
    stages = (stage0, stage1)
    xr, rf, of, retf = (r.reshape(r.shape[0] * sub, LANES) for r in (xr_rows, rf_rows, of_rows, retf_rows))

    def fetch(e, slot):
        a = pltpu.make_async_copy(win_ref.at[e], wi.at[slot], wsem.at[slot, 0])
        b = pltpu.make_async_copy(wout_ref.at[e], wo.at[slot], wsem.at[slot, 1])
        return a, b

    x_copy = pltpu.make_async_copy(x_hbm, x_ref, tsem.at[4])
    x_copy.start()
    for e in range(BUFS):
        for c in fetch(e, e):
            c.start()
    barrier = pltpu.get_barrier_semaphore()
    for k in range(1, groups):
        pl.semaphore_signal(barrier, inc=1, device_id={"expert": lax.rem(me + k, groups)}, device_id_type=MESH)
    retf[pl.ds(GROUPS * groups * span, 8 * sub), :] = jnp.zeros((8 * sub, LANES), jnp.float32)
    experts = hot.shape[1]
    i_e, i_f = iota((experts, experts), 0), iota((experts, experts), 1)
    same[...] = as_bf16((i_e // group_experts == i_f // group_experts) & (i_e < i_f))
    base, counts = local_positions(groups, rows, group_experts, ids_ref, hot, same, count, rank_ref, pos_ref, pack_v)
    x_copy.wait()
    for k in range(sub):
        xr[pl.ds(k, tokens, stride=sub), :] = x_ref[:, k * LANES:(k + 1) * LANES].astype(jnp.float32)
    place_pairs(groups, rows, group_experts, base, counts, ids_ref, hot, same, rank_ref, pos_ref, pack_v)
    pack_copy = pltpu.make_async_copy(pack_v, pack_idx, tsem.at[0])
    pack_copy.start()
    pl.semaphore_wait(barrier, groups - 1)

    def count_copy(k):
        return pltpu.make_async_remote_copy(
            src_ref=count, dst_ref=every.at[me], send_sem=csend.at[k], recv_sem=crecv.at[k],
            device_id={"expert": lax.rem(me + k, groups)}, device_id_type=MESH)

    for k in range(1, groups):
        count_copy(k).start()
    pack_copy.wait()

    lines, rest = divmod(rows, LANES)

    def gather_block(idx, line, table, dst):
        def some(at, first, count):
            for c in range(count // 16):
                got = [table[idx[at, c * 16 + r]] for r in range(16)]
                dst[pl.ds(pl.multiple_of((first + c * 16) * sub, 16 * sub), 16 * sub), :] = jnp.concatenate(got, axis=0).astype(jnp.bfloat16)

        def body(i, carry):
            some(line + i, i * LANES, LANES)
            return carry

        lax.fori_loop(0, lines, body, 0)
        if rest:
            some(line + lines, lines * LANES, rest)

    def widen(src, dst, first):
        def body(c, carry):
            part = pl.multiple_of(c * 16 * sub, 16 * sub)
            dst[pl.ds(pl.multiple_of(first + part, 16), 16 * sub), :] = src[pl.ds(part, 16 * sub), :].astype(jnp.float32)
            return carry
        lax.fori_loop(0, rows // 16, body, 0)

    def copy_to(src, dst, g, k, s_sem, r_sem):
        peer = lax.rem(me + k, groups)
        return pltpu.make_async_remote_copy(
            src_ref=src.at[g, peer], dst_ref=dst.at[g, me], send_sem=s_sem.at[g, k], recv_sem=r_sem.at[g, k],
            device_id={"expert": peer}, device_id_type=MESH)

    def send_blocks(g, idx, table, src, dst, s_sem, r_sem):
        def body(i, carry):
            peer = lax.rem(me + i + 1, groups)
            gather_block(idx, (g * groups + peer) * (lines + (rest > 0)), table, src.at[g, peer])

            @pl.when(i >= 1)
            def _():
                copy_to(src, dst, g, i, s_sem, r_sem).start()

            return carry

        lax.fori_loop(0, groups, body, 0)

    def take_blocks(g, src, dst, own, first, s_sem, r_sem):
        widen(own.at[g, me], dst, first + me * span)

        def body(k, carry):
            peer = lax.rem(me - k + groups, groups)
            pltpu.make_async_remote_copy(
                src_ref=own.at[g, peer], dst_ref=src.at[g, peer], send_sem=s_sem.at[g, k], recv_sem=r_sem.at[g, k],
                device_id={"expert": peer}, device_id_type=MESH).wait_recv()
            widen(src.at[g, peer], dst, first + peer * span)
            return carry

        lax.fori_loop(1, groups, body, 0)

    for g in range(GROUPS):
        send_blocks(g, pack_idx, xr_rows, send, recv, ssem, rsem)

    every[me] = count[...]
    for j in range(2):
        for b in range(tokens // LANES):
            part = slice(b * LANES, (b + 1) * LANES)
            wide_gates[j, part, :] = jnp.broadcast_to(gates_ref[j:j + 1, part], (LANES, LANES)).T
    for k in range(1, groups):
        source = lax.rem(me - k + groups, groups)
        pltpu.make_async_remote_copy(
            src_ref=count, dst_ref=every.at[source], send_sem=csend.at[k], recv_sem=crecv.at[k],
            device_id={"expert": source}, device_id_type=MESH).wait_recv()
    group_tables(me, groups, rows, group_experts, capacity, every, hot, same, rank_ref, pos_ref, lhs_v, ret_v, comb_v, load_ref)
    tables = [pltpu.make_async_copy(a, b, tsem.at[i + 1]) for i, (a, b) in enumerate(((lhs_v, lhs_idx), (ret_v, ret_idx), (comb_v, comb_idx)))]
    for t in tables:
        t.start()
    for t in tables:
        t.wait()

    for g in range(GROUPS):
        take_blocks(g, recv, rf, send, 0, ssem, rsem)

        def gather_lhs(e, stage):
            for q in range(capacity):
                stage[pl.ds(q * sub, sub), :] = rf_rows[lhs_idx[e, q]]

        def ffn(e, stage):
            slot = lax.rem(e, BUFS)
            for c in fetch(e, slot):
                c.wait()
            lhs = jnp.concatenate([stage[pl.ds(k, capacity, stride=sub), :] for k in range(sub)], axis=1).astype(jnp.bfloat16)
            hidden = jax.nn.gelu(dot_f32(lhs, wi[slot])).astype(jnp.bfloat16)
            out = dot_f32(hidden, wo[slot]).astype(jnp.bfloat16).astype(jnp.float32)
            at = (e - g * group_experts) * capacity * sub
            for k in range(sub):
                of[pl.ds(at + k, capacity, stride=sub), :] = out[:, k * LANES:(k + 1) * LANES]

        def body(i, carry):
            for half in range(2):
                e = g * group_experts + i * 2 + half
                gather_lhs(e, stages[half])
                ffn(e, stages[half])

                @pl.when(e + BUFS < local_experts)
                def _():
                    for c in fetch(e + BUFS, lax.rem(e, BUFS)):
                        c.start()
            return carry

        lax.fori_loop(0, group_experts // 2, body, 0)
        send_blocks(g, ret_idx, of_rows, rsend, rrecv, rssem, rrsem)

    for g in range(GROUPS):
        take_blocks(g, rrecv, retf, rsend, g * groups * span, rssem, rrsem)

    half = tokens // LANES

    def combine(line, carry):
        for c in range(LANES // 16):
            got = []
            for r in range(16):
                col = c * 16 + r
                row = xr_rows[line * LANES + col]
                for j in range(2):
                    row = row + wide_gates[j, pl.ds(pl.multiple_of(line * LANES, LANES) + col, 1), :] * retf_rows[comb_idx[j * half + line, col]]
                got.append(row)
            xr[pl.ds(pl.multiple_of((line * LANES + c * 16) * sub, 16 * sub), 16 * sub), :] = jnp.concatenate(got, axis=0)
        part = pl.ds(pl.multiple_of(line * LANES, LANES), LANES)
        for k in range(sub):
            x_ref[part, k * LANES:(k + 1) * LANES] = xr[pl.ds(line * LANES * sub + k, LANES, stride=sub), :].astype(jnp.bfloat16)

        @pl.when(line >= 1)
        def _():
            put(line - 1).start()

        return carry

    def put(line):
        part = pl.ds(pl.multiple_of(line * LANES, LANES), LANES)
        return pltpu.make_async_copy(x_ref.at[part], out_hbm.at[part], osem.at[line])

    lax.fori_loop(0, half, combine, 0)
    put(half - 1).start()
    for line in range(half):
        put(line).wait()
    for g in range(GROUPS):
        for k in range(1, groups):
            if g == 0:
                count_copy(k).wait_send()
            copy_to(send, recv, g, k, ssem, rsem).wait_send()
            copy_to(rsend, rrecv, g, k, rssem, rrsem).wait_send()


def compact_step(groups, rows, capacity, gates, ids, token_rows, w_in, w_out):
    tokens, model_dim = token_rows.shape
    local_experts, _, hidden_dim = w_in.shape
    experts = local_experts * groups
    group_experts = local_experts // GROUPS
    sub = model_dim // LANES
    span = rows * sub
    vmem = pl.BlockSpec(memory_space=pltpu.VMEM)
    hbm = pl.BlockSpec(memory_space=pl.ANY)
    wire = pltpu.VMEM((GROUPS, groups, span, LANES), jnp.bfloat16)
    sems = pltpu.SemaphoreType.DMA((GROUPS, groups))
    table_rows = (
        GROUPS * groups * -(-rows // LANES),
        local_experts,
        GROUPS * groups * -(-rows // LANES),
        2 * tokens // LANES,
    )
    return pl.pallas_call(
        functools.partial(exchange_kernel, groups, rows, capacity),
        out_shape=(jax.ShapeDtypeStruct((tokens, model_dim), jnp.bfloat16), jax.ShapeDtypeStruct((1, 1), jnp.float32)),
        in_specs=[vmem, vmem, hbm, hbm, hbm],
        out_specs=(hbm, vmem),
        scratch_shapes=[
            pltpu.VMEM((2, experts, tokens), jnp.bfloat16),
            pltpu.VMEM((experts, experts), jnp.bfloat16),
            pltpu.VMEM((8, experts), jnp.float32),
            pltpu.VMEM((groups, 8, experts), jnp.float32),
            pltpu.VMEM((8, tokens), jnp.float32),
            pltpu.VMEM((8, tokens), jnp.float32),
            *[pltpu.VMEM((r, LANES), jnp.int32) for r in table_rows],
            *[pltpu.SMEM((r, LANES), jnp.int32) for r in table_rows],
            pltpu.VMEM((2, tokens, LANES), jnp.float32),
            pltpu.VMEM((tokens, model_dim), jnp.bfloat16),
            pltpu.VMEM((tokens, sub, LANES), jnp.float32),
            wire,
            wire,
            pltpu.VMEM((groups * rows, sub, LANES), jnp.float32),
            pltpu.VMEM((capacity * sub, LANES), jnp.float32),
            pltpu.VMEM((capacity * sub, LANES), jnp.float32),
            pltpu.VMEM((group_experts * capacity, sub, LANES), jnp.float32),
            wire,
            wire,
            pltpu.VMEM((GROUPS * groups * rows + 8, sub, LANES), jnp.float32),
            pltpu.VMEM((BUFS, model_dim, hidden_dim), jnp.bfloat16),
            pltpu.VMEM((BUFS, hidden_dim, model_dim), jnp.bfloat16),
            pltpu.SemaphoreType.DMA((BUFS, 2)),
            sems, sems, sems, sems,
            pltpu.SemaphoreType.DMA((groups,)),
            pltpu.SemaphoreType.DMA((groups,)),
            pltpu.SemaphoreType.DMA((5,)),
            pltpu.SemaphoreType.DMA((tokens // LANES,)),
        ],
        compiler_params=pltpu.CompilerParams(collective_id=0, has_side_effects=True, vmem_limit_bytes=67043328),
        name="expert_exchange",
    )(gates, ids, token_rows, w_in, w_out)


def hand_over(rows):
    def kernel(a_ref, o_ref):
        o_ref[...] = a_ref[...]

    block = pl.BlockSpec((rows.shape[0] // 4, rows.shape[1]), lambda i: (i, 0))
    return pl.pallas_call(kernel, grid=(4,), in_specs=[block], out_specs=block, out_shape=jax.ShapeDtypeStruct(rows.shape, rows.dtype), name="hand_over")(rows)


def solution(mesh):
    groups = mesh.shape["expert"]
    row_spec = P(("data", "expert"), None)
    weight_spec = P("expert", None, None)

    def device_step(token_rows, expert_ids, gate_weights, w_in, w_out):
        tokens, top_k = expert_ids.shape
        local_experts = w_in.shape[0]
        capacity = tokens * top_k // local_experts
        rows = block_rows(tokens, top_k, groups)
        fast, load = compact_step(groups, rows, capacity, gate_weights.T, expert_ids.T, token_rows, w_in, w_out)
        fast = hand_over(fast)
        overflow = load[0, 0] > rows
        general = lambda state: (jnp.array(False), padded_step(groups, token_rows, expert_ids, gate_weights, w_in, w_out))
        return lax.while_loop(lambda state: state[0], general, (overflow, fast))[1]

    return jax.shard_map(device_step, mesh=mesh, in_specs=(row_spec, row_spec, row_spec, weight_spec, weight_spec), out_specs=row_spec, check_vma=False)
```

```python
import functools

import jax
import jax.numpy as jnp
from jax import lax
from jax.experimental import pallas as pl
from jax.experimental.pallas import tpu as pltpu
from jax.sharding import PartitionSpec as P

GROUPS = 2
BUFS = 3
LANES = 128
MESH = pl.DeviceIdType.MESH


def route_local(expert_ids, experts):
    ids_t = expert_ids.T
    onehot = (ids_t[:, :, None] == jnp.arange(experts, dtype=jnp.int32)).astype(jnp.int32)
    running = jnp.cumsum(onehot, axis=1)
    counts = running[:, -1, :]
    rank_local = jnp.sum(onehot * running, axis=2) - 1
    return ids_t, counts, rank_local


def padded_step(groups, token_rows, expert_ids, gate_weights, w_in, w_out):
    tokens, top_k = expert_ids.shape
    local_experts, model_dim = w_in.shape[0], w_in.shape[1]
    experts = local_experts * groups
    mean_load = tokens * top_k // experts
    send_cap = -(-(7 * mean_load // 4) // 16) * 16
    capacity = groups * mean_load
    rows_total = experts * send_cap
    ids_t, counts, rank_local = route_local(expert_ids, experts)
    inclusive = counts
    shift = 1
    while shift < groups:
        pairs_list = [(source, source + shift) for source in range(groups - shift)]
        inclusive = inclusive + lax.ppermute(inclusive, "expert", pairs_list)
        shift = shift * 2
    before = inclusive - counts
    totals = lax.psum(counts, "expert")
    prior = jnp.cumsum(totals, axis=0) - totals
    within = jnp.cumsum(counts, axis=0) - counts
    slot = jnp.take_along_axis(prior + before, ids_t, axis=1) + rank_local
    keep = slot < capacity
    target = ids_t * send_cap + jnp.take_along_axis(within, ids_t, axis=1) + rank_local
    token_ids = jnp.broadcast_to(jnp.arange(tokens, dtype=jnp.int32), (top_k, tokens))
    source_row = jnp.full((rows_total,), tokens, jnp.int32).at[jnp.where(keep, target, rows_total).reshape(-1)].set(token_ids.reshape(-1), mode="drop")
    padded = jnp.concatenate([token_rows, jnp.zeros((1, model_dim), token_rows.dtype)], axis=0)
    outbound = jnp.take(padded, source_row, axis=0).reshape(experts, send_cap, model_dim)
    inbound = lax.all_to_all(outbound, "expert", 0, 0, tiled=True).reshape(groups, local_experts, send_cap, model_dim)

    def one_expert(e, total):
        rows = lax.dynamic_index_in_dim(inbound, e, 1, keepdims=False).reshape(groups * send_cap, model_dim)
        hidden = jax.nn.gelu(jnp.dot(rows, w_in[e], preferred_element_type=jnp.float32)).astype(jnp.bfloat16)
        out = jnp.dot(hidden, w_out[e], preferred_element_type=jnp.float32).astype(jnp.bfloat16)
        return lax.dynamic_update_index_in_dim(total, out.reshape(groups, send_cap, model_dim), e, 1)

    expert_out = lax.fori_loop(0, local_experts, one_expert, jnp.zeros_like(inbound))
    returned = lax.all_to_all(expert_out.reshape(experts, send_cap, model_dim), "expert", 0, 0, tiled=True).reshape(rows_total, model_dim)
    picked = jnp.take(returned, target, axis=0)
    weight = jnp.where(keep, gate_weights.T, 0.0)
    mixed = jnp.sum(weight[:, :, None] * picked.astype(jnp.float32), axis=0)
    return (token_rows.astype(jnp.float32) + mixed).astype(jnp.bfloat16)


def block_rows(tokens, top_k, groups):
    mean = tokens * top_k // (groups * GROUPS)
    return (mean * 19 // 16 + 15) // 16 * 16


def dot_f32(a, b):
    return jnp.dot(a, b, preferred_element_type=jnp.float32)


def dot_nt(a, b):
    return lax.dot_general(a, b, (((1,), (1,)), ((), ())), preferred_element_type=jnp.float32)


def iota(shape, axis):
    return lax.broadcasted_iota(jnp.int32, shape, axis)


def as_bf16(mask):
    return jnp.where(mask, 1.0, 0.0).astype(jnp.bfloat16)


def pad_rows(rows, total):
    have = sum(r.shape[0] for r in rows)
    if have < total:
        rows = rows + [jnp.zeros((total - have, rows[0].shape[1]), rows[0].dtype)]
    return jnp.concatenate(rows, axis=0)


def select_row(rows, high_row):
    total = jnp.zeros_like(rows[0])
    for i, row in enumerate(rows):
        total = total + jnp.where(high_row == i, row, 0.0)
    return total


def split_lanes(row):
    return [row[:, i * LANES:(i + 1) * LANES] for i in range(row.shape[1] // LANES)]


def local_counts(experts, ids_ref, hot, count_ref):
    tokens = ids_ref.shape[1]
    blocks = tokens // LANES
    highs = experts // LANES

    def fill(b, carry):
        at = pl.ds(pl.multiple_of(b * LANES, LANES), LANES)
        for j in range(2):
            hot[j, :, at] = as_bf16(iota((LANES, LANES), 0) == ids_ref[j:j + 1, at] % LANES)
        return carry

    lax.fori_loop(0, blocks, fill, 0)
    n = highs * blocks
    row, col = iota((n, n), 0), iota((n, n), 1)
    below = as_bf16((row // blocks == col // blocks) & (row > col))
    in_block = iota((n, tokens), 0) % blocks == iota((n, tokens), 1) // LANES
    base, count = [], []
    for j in range(2):
        part = as_bf16(in_block & (iota((n, tokens), 0) // blocks == ids_ref[j:j + 1, :] // LANES))
        per_block = dot_nt(part, hot[j])
        base.append(dot_f32(below, per_block.astype(jnp.bfloat16)))
        count.append(jnp.concatenate([jnp.sum(per_block[i * blocks:(i + 1) * blocks], axis=0, keepdims=True) for i in range(highs)], axis=1))
    count_ref[...] = pad_rows(count, 8)
    return base, count


def place_pairs(groups, rows, group_experts, base, count, ids_ref, hot, same, rank_ref, pos_ref, pack_ref):
    tokens = ids_ref.shape[1]
    experts = same.shape[0]
    blocks = tokens // LANES
    highs = experts // LANES
    local_experts = experts // groups
    both = pad_rows([count[0] + count[1]], 8)
    start = dot_f32(both.astype(jnp.bfloat16), same[...])[0:1]
    lane = iota((1, experts), 1)
    block_of = (lane % local_experts // group_experts) * groups + lane // local_experts
    stride = -(-rows // LANES) * LANES
    first = (block_of * stride).astype(jnp.float32) + start
    earlier = iota((LANES, LANES), 0) < iota((LANES, LANES), 1)
    found = None
    table_rows = pack_ref.shape[0]
    n = highs * blocks
    for j in range(2):
        at = first if j == 0 else first + count[0]
        coarse = jnp.floor(at * (1.0 / 64.0))
        lhs = [base[j]] + split_lanes(coarse) + split_lanes(at - 64.0 * coarse)
        look = dot_f32(pad_rows(lhs, -(-(n + 2 * highs) // 16) * 16).astype(jnp.bfloat16), hot[j])
        for b in range(blocks):
            cols = slice(b * LANES, (b + 1) * LANES)
            row = ids_ref[j:j + 1, cols]
            high_row = row // LANES
            wide = jnp.broadcast_to(row.astype(jnp.float32), (LANES, LANES))
            same_id = (wide.T == wide) & earlier
            rank = jnp.sum(jnp.where(same_id, 1.0, 0.0), axis=0, keepdims=True)
            rank = rank + select_row([look[i * blocks + b:i * blocks + b + 1, cols] for i in range(highs)], high_row)
            offset = select_row([64.0 * look[n + i:n + i + 1, cols] + look[n + highs + i:n + highs + i + 1, cols] for i in range(highs)], high_row)
            rank_ref[j:j + 1, cols] = rank
            pos_ref[j:j + 1, cols] = rank + offset
        pos = pos_ref[j:j + 1, :]
        pos_ref[j:j + 1, :] = pos - (stride - rows) * jnp.floor((pos + 0.5) * (1.0 / stride))
        pos = pos.astype(jnp.int32)
        token = iota((LANES, tokens), 1)
        high_t = as_bf16(iota((table_rows, tokens), 0) == pos // LANES)
        low = iota((LANES, tokens), 0) == pos % LANES
        low_hi = jnp.where(low, (token // 8).astype(jnp.float32), 0.0).astype(jnp.bfloat16)
        low_lo = jnp.where(low, (token % 8).astype(jnp.float32), 0.0).astype(jnp.bfloat16)
        hit = 8.0 * dot_nt(high_t, low_hi) + dot_nt(high_t, low_lo)
        found = hit if found is None else found + hit
    pack_ref[...] = jnp.clip(found.astype(jnp.int32), 0, tokens - 1)


def group_tables(me, groups, rows, group_experts, capacity, every, ids_ref, hot, same, rank_ref, pos_ref, lhs_ref, ret_ref, comb_ref, load_ref):
    experts = same.shape[0]
    tokens = hot.shape[2]
    local_experts = experts // groups
    blocks = tokens // LANES
    c = [[every[s, j:j + 1, :] for s in range(groups)] for j in range(2)]
    both = pad_rows([c[0][s] + c[1][s] for s in range(groups)], 8)
    start = dot_f32(both.astype(jnp.bfloat16), same[...])
    load_ref[...] = jnp.broadcast_to(jnp.max(start + both), load_ref.shape)
    kept = [[None] * groups, [None] * groups]
    used = jnp.zeros((1, experts), jnp.float32)
    for j in range(2):
        for s in range(groups):
            kept[j][s] = jnp.clip(capacity - used, 0.0, c[j][s])
            used = used + c[j][s]
    lane = iota((1, experts), 1)
    in_group = lane % group_experts
    slot = jnp.zeros((1, experts), jnp.float32)
    slots, steps, edges, jumps = [], [], [], []
    last = jnp.zeros((1, experts), jnp.float32)
    for s in range(groups):
        ret_v = []
        for j in range(2):
            edge = start[s:s + 1] if j == 0 else start[s:s + 1] + c[0][s]
            v = s * rows + edge - slot
            slots.append(slot)
            steps.append(v - last)
            last = v
            edges.append(edge)
            ret_v.append((in_group * capacity).astype(jnp.float32) + slot - edge)
            slot = slot + kept[j][s]
        before = jnp.concatenate([jnp.zeros((1, 1), jnp.float32), ret_v[1][:, :-1]], axis=1)
        jumps.append(ret_v[0] - jnp.where(in_group == 0, 0.0, before))
        jumps.append(ret_v[1] - ret_v[0])

    def mine(parts):
        a = jnp.concatenate(parts, axis=0)
        total = jnp.zeros((a.shape[0], local_experts), jnp.float32)
        for d in range(groups):
            total = total + jnp.where(me == d, a[:, d * local_experts:(d + 1) * local_experts], 0.0)
        return total

    slots, steps, edges, jumps = mine(slots), mine(steps), mine(edges), mine(jumps)
    tall = pad_rows([edges, jumps, slots, steps], LANES)
    tall = jnp.concatenate([tall, jnp.zeros((LANES, LANES - local_experts), jnp.float32)], axis=1).T if local_experts < LANES else tall.T
    q = iota((local_experts, LANES), 1).astype(jnp.float32)
    lhs = q
    for i in range(2 * groups):
        at = 4 * groups + i
        lhs = lhs + jnp.where(q >= tall[:local_experts, at:at + 1], tall[:local_experts, at + 2 * groups:at + 2 * groups + 1], 0.0)
    lhs_ref[...] = jnp.clip(lhs.astype(jnp.int32), 0, groups * rows - 1)

    width = -(-rows // LANES) * LANES
    p = iota((1, width), 1).astype(jnp.float32)
    for g in range(GROUPS):
        part = tall[g * group_experts:(g + 1) * group_experts]
        for s in range(groups):
            total = jnp.zeros((group_experts, width), jnp.float32)
            for j in range(2):
                i = 2 * s + j
                total = total + jnp.where(p >= part[:, i:i + 1], part[:, 2 * groups + i:2 * groups + i + 1], 0.0)
            row = p + jnp.sum(total, axis=0, keepdims=True)
            row = jnp.clip(row.astype(jnp.int32), 0, group_experts * capacity - 1)
            for i in range(width // LANES):
                at = (g * groups + s) * (width // LANES) + i
                ret_ref[at:at + 1, :] = row[:, i * LANES:(i + 1) * LANES]

    for j in range(2):
        own = jnp.zeros((1, experts), jnp.float32)
        for s in range(groups):
            own = own + jnp.where(me == s, kept[j][s], 0.0)
        bound = dot_f32(pad_rows(split_lanes(own), 16).astype(jnp.bfloat16), hot[j])
        bound = select_row([bound[i:i + 1] for i in range(experts // LANES)], ids_ref[j:j + 1, :] // LANES)
        none = float(GROUPS * groups * rows)
        for b in range(blocks):
            cols = slice(b * LANES, (b + 1) * LANES)
            take = jnp.where(rank_ref[j:j + 1, cols] < bound[:, cols], pos_ref[j:j + 1, cols], none)
            comb_ref[j * blocks + b:j * blocks + b + 1, :] = jnp.clip(take.astype(jnp.int32), 0, GROUPS * groups * rows)


def exchange_kernel(
    groups, rows, capacity,
    gates_ref, ids_ref, x_hbm, win_ref, wout_ref, out_hbm, load_ref,
    hot, same, count, every, rank_ref, pos_ref, pack_v, lhs_v, ret_v, comb_v, pack_idx, lhs_idx, ret_idx, comb_idx, wide_gates, x_ref,
    xr_rows, send, recv, rf_rows, stage0, stage1, of_rows, rsend, rrecv, retf_rows, wi, wo,
    wsem, ssem, rsem, rssem, rrsem, csend, crecv, tsem, osem,
):
    tokens, model_dim = x_hbm.shape
    sub = model_dim // LANES
    local_experts = win_ref.shape[0]
    group_experts = local_experts // GROUPS
    me = lax.axis_index("expert")
    span = rows * sub
    stages = (stage0, stage1)
    xr, rf, of, retf = (r.reshape(r.shape[0] * sub, LANES) for r in (xr_rows, rf_rows, of_rows, retf_rows))

    def fetch(e, slot):
        a = pltpu.make_async_copy(win_ref.at[e], wi.at[slot], wsem.at[slot, 0])
        b = pltpu.make_async_copy(wout_ref.at[e], wo.at[slot], wsem.at[slot, 1])
        return a, b

    x_copy = pltpu.make_async_copy(x_hbm, x_ref, tsem.at[4])
    x_copy.start()
    for e in range(BUFS):
        for c in fetch(e, e):
            c.start()
    barrier = pltpu.get_barrier_semaphore()
    for k in range(1, groups):
        pl.semaphore_signal(barrier, inc=1, device_id={"expert": lax.rem(me + k, groups)}, device_id_type=MESH)
    retf[pl.ds(GROUPS * groups * span, 8 * sub), :] = jnp.zeros((8 * sub, LANES), jnp.float32)
    experts = same.shape[0]
    i_e, i_f = iota((experts, experts), 0), iota((experts, experts), 1)
    same[...] = as_bf16((i_e // group_experts == i_f // group_experts) & (i_e < i_f))
    base, counts = local_counts(experts, ids_ref, hot, count)
    x_copy.wait()
    for k in range(sub):
        xr[pl.ds(k, tokens, stride=sub), :] = x_ref[:, k * LANES:(k + 1) * LANES].astype(jnp.float32)
    place_pairs(groups, rows, group_experts, base, counts, ids_ref, hot, same, rank_ref, pos_ref, pack_v)
    pack_copy = pltpu.make_async_copy(pack_v, pack_idx, tsem.at[0])
    pack_copy.start()
    pl.semaphore_wait(barrier, groups - 1)

    def count_copy(k):
        return pltpu.make_async_remote_copy(
            src_ref=count, dst_ref=every.at[me], send_sem=csend.at[k], recv_sem=crecv.at[k],
            device_id={"expert": lax.rem(me + k, groups)}, device_id_type=MESH)

    for k in range(1, groups):
        count_copy(k).start()
    pack_copy.wait()

    lines, rest = divmod(rows, LANES)

    def gather_block(idx, line, table, dst):
        def some(at, first, count):
            for c in range(count // 16):
                got = [table[idx[at, c * 16 + r]] for r in range(16)]
                dst[pl.ds(pl.multiple_of((first + c * 16) * sub, 16 * sub), 16 * sub), :] = jnp.concatenate(got, axis=0).astype(jnp.bfloat16)

        def body(i, carry):
            some(line + i, i * LANES, LANES)
            return carry

        lax.fori_loop(0, lines, body, 0)
        if rest:
            some(line + lines, lines * LANES, rest)

    def widen(src, dst, first):
        def body(c, carry):
            part = pl.multiple_of(c * 16 * sub, 16 * sub)
            dst[pl.ds(pl.multiple_of(first + part, 16), 16 * sub), :] = src[pl.ds(part, 16 * sub), :].astype(jnp.float32)
            return carry
        lax.fori_loop(0, rows // 16, body, 0)

    def copy_to(src, dst, g, k, s_sem, r_sem):
        peer = lax.rem(me + k, groups)
        return pltpu.make_async_remote_copy(
            src_ref=src.at[g, peer], dst_ref=dst.at[g, me], send_sem=s_sem.at[g, k], recv_sem=r_sem.at[g, k],
            device_id={"expert": peer}, device_id_type=MESH)

    def send_blocks(g, idx, table, src, dst, s_sem, r_sem):
        def body(i, carry):
            peer = lax.rem(me + i + 1, groups)
            gather_block(idx, (g * groups + peer) * (lines + (rest > 0)), table, src.at[g, peer])

            @pl.when(i >= 1)
            def _():
                copy_to(src, dst, g, i, s_sem, r_sem).start()

            return carry

        lax.fori_loop(0, groups, body, 0)

    def take_blocks(g, src, dst, own, first, s_sem, r_sem):
        widen(own.at[g, me], dst, first + me * span)

        def body(k, carry):
            peer = lax.rem(me - k + groups, groups)
            pltpu.make_async_remote_copy(
                src_ref=own.at[g, peer], dst_ref=src.at[g, peer], send_sem=s_sem.at[g, k], recv_sem=r_sem.at[g, k],
                device_id={"expert": peer}, device_id_type=MESH).wait_recv()
            widen(src.at[g, peer], dst, first + peer * span)
            return carry

        lax.fori_loop(1, groups, body, 0)

    for g in range(GROUPS):
        send_blocks(g, pack_idx, xr_rows, send, recv, ssem, rsem)

    every[me] = count[...]
    for j in range(2):
        for b in range(tokens // LANES):
            part = slice(b * LANES, (b + 1) * LANES)
            wide_gates[j, part, :] = jnp.broadcast_to(gates_ref[j:j + 1, part], (LANES, LANES)).T
    for k in range(1, groups):
        source = lax.rem(me - k + groups, groups)
        pltpu.make_async_remote_copy(
            src_ref=count, dst_ref=every.at[source], send_sem=csend.at[k], recv_sem=crecv.at[k],
            device_id={"expert": source}, device_id_type=MESH).wait_recv()
    group_tables(me, groups, rows, group_experts, capacity, every, ids_ref, hot, same, rank_ref, pos_ref, lhs_v, ret_v, comb_v, load_ref)
    tables = [pltpu.make_async_copy(a, b, tsem.at[i + 1]) for i, (a, b) in enumerate(((lhs_v, lhs_idx), (ret_v, ret_idx), (comb_v, comb_idx)))]
    for t in tables:
        t.start()
    for t in tables:
        t.wait()

    for g in range(GROUPS):
        take_blocks(g, recv, rf, send, 0, ssem, rsem)

        def gather_lhs(e, stage):
            for q in range(capacity):
                stage[pl.ds(q * sub, sub), :] = rf_rows[lhs_idx[e, q]]

        def ffn(e, stage):
            slot = lax.rem(e, BUFS)
            for c in fetch(e, slot):
                c.wait()
            lhs = jnp.concatenate([stage[pl.ds(k, capacity, stride=sub), :] for k in range(sub)], axis=1).astype(jnp.bfloat16)
            hidden = jax.nn.gelu(dot_f32(lhs, wi[slot])).astype(jnp.bfloat16)
            out = dot_f32(hidden, wo[slot]).astype(jnp.bfloat16).astype(jnp.float32)
            at = (e - g * group_experts) * capacity * sub
            for k in range(sub):
                of[pl.ds(at + k, capacity, stride=sub), :] = out[:, k * LANES:(k + 1) * LANES]

        def body(i, carry):
            for half in range(2):
                e = g * group_experts + i * 2 + half
                gather_lhs(e, stages[half])
                ffn(e, stages[half])

                @pl.when(e + BUFS < local_experts)
                def _():
                    for c in fetch(e + BUFS, lax.rem(e, BUFS)):
                        c.start()
            return carry

        lax.fori_loop(0, group_experts // 2, body, 0)
        send_blocks(g, ret_idx, of_rows, rsend, rrecv, rssem, rrsem)

    for g in range(GROUPS):
        take_blocks(g, rrecv, retf, rsend, g * groups * span, rssem, rrsem)

    half = tokens // LANES

    def combine(line, carry):
        for c in range(LANES // 16):
            got = []
            for r in range(16):
                col = c * 16 + r
                row = xr_rows[line * LANES + col]
                for j in range(2):
                    row = row + wide_gates[j, pl.ds(pl.multiple_of(line * LANES, LANES) + col, 1), :] * retf_rows[comb_idx[j * half + line, col]]
                got.append(row)
            xr[pl.ds(pl.multiple_of((line * LANES + c * 16) * sub, 16 * sub), 16 * sub), :] = jnp.concatenate(got, axis=0)
        part = pl.ds(pl.multiple_of(line * LANES, LANES), LANES)
        for k in range(sub):
            x_ref[part, k * LANES:(k + 1) * LANES] = xr[pl.ds(line * LANES * sub + k, LANES, stride=sub), :].astype(jnp.bfloat16)

        @pl.when(line >= 1)
        def _():
            put(line - 1).start()

        return carry

    def put(line):
        part = pl.ds(pl.multiple_of(line * LANES, LANES), LANES)
        return pltpu.make_async_copy(x_ref.at[part], out_hbm.at[part], osem.at[line])

    lax.fori_loop(0, half, combine, 0)
    put(half - 1).start()
    for line in range(half):
        put(line).wait()
    for g in range(GROUPS):
        for k in range(1, groups):
            if g == 0:
                count_copy(k).wait_send()
            copy_to(send, recv, g, k, ssem, rsem).wait_send()
            copy_to(rsend, rrecv, g, k, rssem, rrsem).wait_send()


def compact_step(groups, rows, capacity, gates, ids, token_rows, w_in, w_out):
    tokens, model_dim = token_rows.shape
    local_experts, _, hidden_dim = w_in.shape
    experts = local_experts * groups
    group_experts = local_experts // GROUPS
    sub = model_dim // LANES
    span = rows * sub
    vmem = pl.BlockSpec(memory_space=pltpu.VMEM)
    hbm = pl.BlockSpec(memory_space=pl.ANY)
    wire = pltpu.VMEM((GROUPS, groups, span, LANES), jnp.bfloat16)
    sems = pltpu.SemaphoreType.DMA((GROUPS, groups))
    table_rows = (
        GROUPS * groups * -(-rows // LANES),
        local_experts,
        GROUPS * groups * -(-rows // LANES),
        2 * tokens // LANES,
    )
    return pl.pallas_call(
        functools.partial(exchange_kernel, groups, rows, capacity),
        out_shape=(jax.ShapeDtypeStruct((tokens, model_dim), jnp.bfloat16), jax.ShapeDtypeStruct((1, 1), jnp.float32)),
        in_specs=[vmem, vmem, hbm, hbm, hbm],
        out_specs=(hbm, vmem),
        scratch_shapes=[
            pltpu.VMEM((2, LANES, tokens), jnp.bfloat16),
            pltpu.VMEM((experts, experts), jnp.bfloat16),
            pltpu.VMEM((8, experts), jnp.float32),
            pltpu.VMEM((groups, 8, experts), jnp.float32),
            pltpu.VMEM((8, tokens), jnp.float32),
            pltpu.VMEM((8, tokens), jnp.float32),
            *[pltpu.VMEM((r, LANES), jnp.int32) for r in table_rows],
            *[pltpu.SMEM((r, LANES), jnp.int32) for r in table_rows],
            pltpu.VMEM((2, tokens, LANES), jnp.float32),
            pltpu.VMEM((tokens, model_dim), jnp.bfloat16),
            pltpu.VMEM((tokens, sub, LANES), jnp.float32),
            wire,
            wire,
            pltpu.VMEM((groups * rows, sub, LANES), jnp.float32),
            pltpu.VMEM((capacity * sub, LANES), jnp.float32),
            pltpu.VMEM((capacity * sub, LANES), jnp.float32),
            pltpu.VMEM((group_experts * capacity, sub, LANES), jnp.float32),
            wire,
            wire,
            pltpu.VMEM((GROUPS * groups * rows + 8, sub, LANES), jnp.float32),
            pltpu.VMEM((BUFS, model_dim, hidden_dim), jnp.bfloat16),
            pltpu.VMEM((BUFS, hidden_dim, model_dim), jnp.bfloat16),
            pltpu.SemaphoreType.DMA((BUFS, 2)),
            sems, sems, sems, sems,
            pltpu.SemaphoreType.DMA((groups,)),
            pltpu.SemaphoreType.DMA((groups,)),
            pltpu.SemaphoreType.DMA((5,)),
            pltpu.SemaphoreType.DMA((tokens // LANES,)),
        ],
        compiler_params=pltpu.CompilerParams(collective_id=0, has_side_effects=True, vmem_limit_bytes=67043328),
        name="expert_exchange",
    )(gates, ids, token_rows, w_in, w_out)


def hand_over(rows):
    parts = 8
    size = rows.shape[0] // parts

    def kernel(a_ref, o_ref, buf, sem_in, sem_out):
        part = [pl.ds(i * size, size) for i in range(parts)]
        take = [pltpu.make_async_copy(a_ref.at[p], buf.at[p], sem_in.at[i]) for i, p in enumerate(part)]
        give = [pltpu.make_async_copy(buf.at[p], o_ref.at[p], sem_out.at[i]) for i, p in enumerate(part)]
        for t in take:
            t.start()
        for t, g in zip(take, give):
            t.wait()
            g.start()
        for g in give:
            g.wait()

    return pl.pallas_call(
        kernel,
        in_specs=[pl.BlockSpec(memory_space=pl.ANY)],
        out_specs=pl.BlockSpec(memory_space=pl.ANY),
        out_shape=jax.ShapeDtypeStruct(rows.shape, rows.dtype),
        scratch_shapes=[pltpu.VMEM(rows.shape, rows.dtype), pltpu.SemaphoreType.DMA((parts,)), pltpu.SemaphoreType.DMA((parts,))],
        name="hand_over",
    )(rows)


def solution(mesh):
    groups = mesh.shape["expert"]
    row_spec = P(("data", "expert"), None)
    weight_spec = P("expert", None, None)

    def device_step(token_rows, expert_ids, gate_weights, w_in, w_out):
        tokens, top_k = expert_ids.shape
        local_experts = w_in.shape[0]
        capacity = tokens * top_k // local_experts
        rows = block_rows(tokens, top_k, groups)
        fast, load = compact_step(groups, rows, capacity, gate_weights.T, expert_ids.T, token_rows, w_in, w_out)
        fast = hand_over(fast)
        overflow = load[0, 0] > rows
        general = lambda state: (jnp.array(False), padded_step(groups, token_rows, expert_ids, gate_weights, w_in, w_out))
        return lax.while_loop(lambda state: state[0], general, (overflow, fast))[1]

    return jax.shard_map(device_step, mesh=mesh, in_specs=(row_spec, row_spec, row_spec, weight_spec, weight_spec), out_specs=row_spec, check_vma=False)
```

```python
import functools

import jax
import jax.numpy as jnp
from jax import lax
from jax.experimental import pallas as pl
from jax.experimental.pallas import tpu as pltpu
from jax.sharding import PartitionSpec as P

GROUPS = 2
BUFS = 5
LANES = 128
MESH = pl.DeviceIdType.MESH


def route_local(expert_ids, experts):
    ids_t = expert_ids.T
    onehot = (ids_t[:, :, None] == jnp.arange(experts, dtype=jnp.int32)).astype(jnp.int32)
    running = jnp.cumsum(onehot, axis=1)
    counts = running[:, -1, :]
    rank_local = jnp.sum(onehot * running, axis=2) - 1
    return ids_t, counts, rank_local


def padded_step(groups, token_rows, expert_ids, gate_weights, w_in, w_out):
    tokens, top_k = expert_ids.shape
    local_experts, model_dim = w_in.shape[0], w_in.shape[1]
    experts = local_experts * groups
    mean_load = tokens * top_k // experts
    send_cap = -(-(7 * mean_load // 4) // 16) * 16
    capacity = groups * mean_load
    rows_total = experts * send_cap
    ids_t, counts, rank_local = route_local(expert_ids, experts)
    inclusive = counts
    shift = 1
    while shift < groups:
        pairs_list = [(source, source + shift) for source in range(groups - shift)]
        inclusive = inclusive + lax.ppermute(inclusive, "expert", pairs_list)
        shift = shift * 2
    before = inclusive - counts
    totals = lax.psum(counts, "expert")
    prior = jnp.cumsum(totals, axis=0) - totals
    within = jnp.cumsum(counts, axis=0) - counts
    slot = jnp.take_along_axis(prior + before, ids_t, axis=1) + rank_local
    keep = slot < capacity
    target = ids_t * send_cap + jnp.take_along_axis(within, ids_t, axis=1) + rank_local
    token_ids = jnp.broadcast_to(jnp.arange(tokens, dtype=jnp.int32), (top_k, tokens))
    source_row = jnp.full((rows_total,), tokens, jnp.int32).at[jnp.where(keep, target, rows_total).reshape(-1)].set(token_ids.reshape(-1), mode="drop")
    padded = jnp.concatenate([token_rows, jnp.zeros((1, model_dim), token_rows.dtype)], axis=0)
    outbound = jnp.take(padded, source_row, axis=0).reshape(experts, send_cap, model_dim)
    inbound = lax.all_to_all(outbound, "expert", 0, 0, tiled=True).reshape(groups, local_experts, send_cap, model_dim)

    def one_expert(e, total):
        rows = lax.dynamic_index_in_dim(inbound, e, 1, keepdims=False).reshape(groups * send_cap, model_dim)
        hidden = jax.nn.gelu(jnp.dot(rows, w_in[e], preferred_element_type=jnp.float32)).astype(jnp.bfloat16)
        out = jnp.dot(hidden, w_out[e], preferred_element_type=jnp.float32).astype(jnp.bfloat16)
        return lax.dynamic_update_index_in_dim(total, out.reshape(groups, send_cap, model_dim), e, 1)

    expert_out = lax.fori_loop(0, local_experts, one_expert, jnp.zeros_like(inbound))
    returned = lax.all_to_all(expert_out.reshape(experts, send_cap, model_dim), "expert", 0, 0, tiled=True).reshape(rows_total, model_dim)
    picked = jnp.take(returned, target, axis=0)
    weight = jnp.where(keep, gate_weights.T, 0.0)
    mixed = jnp.sum(weight[:, :, None] * picked.astype(jnp.float32), axis=0)
    return (token_rows.astype(jnp.float32) + mixed).astype(jnp.bfloat16)


def block_rows(tokens, top_k, groups):
    mean = tokens * top_k // (groups * GROUPS)
    return (mean * 19 // 16 + 15) // 16 * 16


def total_rows(tokens, top_k, groups):
    return (tokens * top_k // groups * 9 // 8 + 15) // 16 * 16


def dot_f32(a, b):
    return jnp.dot(a, b, preferred_element_type=jnp.float32)


def dot_nt(a, b):
    return lax.dot_general(a, b, (((1,), (1,)), ((), ())), preferred_element_type=jnp.float32)


def iota(shape, axis):
    return lax.broadcasted_iota(jnp.int32, shape, axis)


def as_bf16(mask):
    return jnp.where(mask, 1.0, 0.0).astype(jnp.bfloat16)


def pad_rows(rows, total):
    have = sum(r.shape[0] for r in rows)
    if have < total:
        rows = rows + [jnp.zeros((total - have, rows[0].shape[1]), rows[0].dtype)]
    return jnp.concatenate(rows, axis=0)


def select_row(rows, high_row):
    total = jnp.zeros_like(rows[0])
    for i, row in enumerate(rows):
        total = total + jnp.where(high_row == i, row, 0.0)
    return total


def split_lanes(row):
    return [row[:, i * LANES:(i + 1) * LANES] for i in range(row.shape[1] // LANES)]


def local_counts(experts, ids_ref, hot, count_ref):
    tokens = ids_ref.shape[1]
    blocks = tokens // LANES
    highs = experts // LANES

    def fill(b, carry):
        at = pl.ds(pl.multiple_of(b * LANES, LANES), LANES)
        for j in range(2):
            hot[j, :, at] = as_bf16(iota((LANES, LANES), 0) == ids_ref[j:j + 1, at] % LANES)
        return carry

    lax.fori_loop(0, blocks, fill, 0)
    n = highs * blocks
    row, col = iota((n, n), 0), iota((n, n), 1)
    below = as_bf16((row // blocks == col // blocks) & (row > col))
    in_block = iota((n, tokens), 0) % blocks == iota((n, tokens), 1) // LANES
    base, count = [], []
    for j in range(2):
        part = as_bf16(in_block & (iota((n, tokens), 0) // blocks == ids_ref[j:j + 1, :] // LANES))
        per_block = dot_nt(part, hot[j])
        base.append(dot_f32(below, per_block.astype(jnp.bfloat16)))
        count.append(jnp.concatenate([jnp.sum(per_block[i * blocks:(i + 1) * blocks], axis=0, keepdims=True) for i in range(highs)], axis=1))
    count_ref[...] = pad_rows(count, 8)
    return base, count


def place_pairs(groups, rows, out_rows, group_experts, base, count, ids_ref, hot, same, rank_ref, pos_ref, pack_ref):
    tokens = ids_ref.shape[1]
    experts = same.shape[0]
    blocks = tokens // LANES
    highs = experts // LANES
    local_experts = experts // groups
    both = pad_rows([count[0] + count[1]], 8)
    start = dot_f32(both.astype(jnp.bfloat16), same[...])[0:1]
    lane = iota((1, experts), 1)
    block_of = (lane % local_experts // group_experts) * groups + lane // local_experts
    stride = -(-out_rows // LANES) * LANES
    back_first = (block_of * rows).astype(jnp.float32) + start[:, :experts]
    out_first = (lane // local_experts * stride).astype(jnp.float32) + start[:, experts:]
    earlier = iota((LANES, LANES), 0) < iota((LANES, LANES), 1)
    found = None
    table_rows = pack_ref.shape[0]
    n = highs * blocks
    for j in range(2):
        lhs = [base[j]]
        for first in (out_first, back_first):
            at = first if j == 0 else first + count[0]
            coarse = jnp.floor(at * (1.0 / 64.0))
            lhs += split_lanes(coarse) + split_lanes(at - 64.0 * coarse)
        look = dot_f32(pad_rows(lhs, -(-(n + 4 * highs) // 16) * 16).astype(jnp.bfloat16), hot[j])
        for b in range(blocks):
            cols = slice(b * LANES, (b + 1) * LANES)
            row = ids_ref[j:j + 1, cols]
            high_row = row // LANES
            wide = jnp.broadcast_to(row.astype(jnp.float32), (LANES, LANES))
            same_id = (wide.T == wide) & earlier
            rank = jnp.sum(jnp.where(same_id, 1.0, 0.0), axis=0, keepdims=True)
            rank = rank + select_row([look[i * blocks + b:i * blocks + b + 1, cols] for i in range(highs)], high_row)
            offsets = []
            for m in (n, n + 2 * highs):
                offsets.append(select_row([64.0 * look[m + i:m + i + 1, cols] + look[m + highs + i:m + highs + i + 1, cols] for i in range(highs)], high_row))
            rank_ref[j:j + 1, cols] = rank
            pos_ref[j + 2:j + 3, cols] = rank + offsets[0]
            pos_ref[j:j + 1, cols] = rank + offsets[1]
        pos = pos_ref[j + 2:j + 3, :].astype(jnp.int32)
        token = iota((LANES, tokens), 1)
        high_t = as_bf16(iota((table_rows, tokens), 0) == pos // LANES)
        low = iota((LANES, tokens), 0) == pos % LANES
        low_hi = jnp.where(low, (token // 8).astype(jnp.float32), 0.0).astype(jnp.bfloat16)
        low_lo = jnp.where(low, (token % 8).astype(jnp.float32), 0.0).astype(jnp.bfloat16)
        hit = 8.0 * dot_nt(high_t, low_hi) + dot_nt(high_t, low_lo)
        found = hit if found is None else found + hit
    pack_ref[...] = jnp.clip(found.astype(jnp.int32), 0, tokens - 1)


def group_tables(me, groups, rows, out_rows, group_experts, capacity, every, ids_ref, hot, same, rank_ref, pos_ref, lhs_ref, ret_ref, comb_ref, load_ref):
    experts = same.shape[0]
    tokens = hot.shape[2]
    local_experts = experts // groups
    blocks = tokens // LANES
    c = [[every[s, j:j + 1, :] for s in range(groups)] for j in range(2)]
    both = pad_rows([c[0][s] + c[1][s] for s in range(groups)], 8)
    starts = dot_f32(both.astype(jnp.bfloat16), same[...])
    start, out_start = starts[:, :experts], starts[:, experts:]
    over = jnp.maximum(jnp.max(start + both) - rows, jnp.max(out_start + both) - out_rows)
    load_ref[...] = jnp.broadcast_to(over, load_ref.shape)
    kept = [[None] * groups, [None] * groups]
    used = jnp.zeros((1, experts), jnp.float32)
    for j in range(2):
        for s in range(groups):
            kept[j][s] = jnp.clip(capacity - used, 0.0, c[j][s])
            used = used + c[j][s]
    lane = iota((1, experts), 1)
    in_group = lane % group_experts
    slot = jnp.zeros((1, experts), jnp.float32)
    slots, steps, edges, jumps = [], [], [], []
    last = jnp.zeros((1, experts), jnp.float32)
    for s in range(groups):
        ret_v = []
        for j in range(2):
            edge = start[s:s + 1] if j == 0 else start[s:s + 1] + c[0][s]
            v = s * out_rows + edge + out_start[s:s + 1] - start[s:s + 1] - slot
            slots.append(slot)
            steps.append(v - last)
            last = v
            edges.append(edge)
            ret_v.append((in_group * capacity).astype(jnp.float32) + slot - edge)
            slot = slot + kept[j][s]
        before = jnp.concatenate([jnp.zeros((1, 1), jnp.float32), ret_v[1][:, :-1]], axis=1)
        jumps.append(ret_v[0] - jnp.where(in_group == 0, 0.0, before))
        jumps.append(ret_v[1] - ret_v[0])

    def mine(parts):
        a = jnp.concatenate(parts, axis=0)
        total = jnp.zeros((a.shape[0], local_experts), jnp.float32)
        for d in range(groups):
            total = total + jnp.where(me == d, a[:, d * local_experts:(d + 1) * local_experts], 0.0)
        return total

    slots, steps, edges, jumps = mine(slots), mine(steps), mine(edges), mine(jumps)
    tall = pad_rows([edges, jumps, slots, steps], LANES)
    tall = jnp.concatenate([tall, jnp.zeros((LANES, LANES - local_experts), jnp.float32)], axis=1).T if local_experts < LANES else tall.T
    q = iota((local_experts, LANES), 1).astype(jnp.float32)
    lhs = q
    for i in range(2 * groups):
        at = 4 * groups + i
        lhs = lhs + jnp.where(q >= tall[:local_experts, at:at + 1], tall[:local_experts, at + 2 * groups:at + 2 * groups + 1], 0.0)
    lhs_ref[...] = jnp.clip(lhs.astype(jnp.int32), 0, groups * out_rows - 1)

    width = -(-rows // LANES) * LANES
    p = iota((1, width), 1).astype(jnp.float32)
    for g in range(GROUPS):
        part = tall[g * group_experts:(g + 1) * group_experts]
        for s in range(groups):
            total = jnp.zeros((group_experts, width), jnp.float32)
            for j in range(2):
                i = 2 * s + j
                total = total + jnp.where(p >= part[:, i:i + 1], part[:, 2 * groups + i:2 * groups + i + 1], 0.0)
            row = p + jnp.sum(total, axis=0, keepdims=True)
            row = jnp.clip(row.astype(jnp.int32), 0, group_experts * capacity - 1)
            for i in range(width // LANES):
                at = (g * groups + s) * (width // LANES) + i
                ret_ref[at:at + 1, :] = row[:, i * LANES:(i + 1) * LANES]

    for j in range(2):
        own = jnp.zeros((1, experts), jnp.float32)
        for s in range(groups):
            own = own + jnp.where(me == s, kept[j][s], 0.0)
        bound = dot_f32(pad_rows(split_lanes(own), 16).astype(jnp.bfloat16), hot[j])
        bound = select_row([bound[i:i + 1] for i in range(experts // LANES)], ids_ref[j:j + 1, :] // LANES)
        none = float(GROUPS * groups * rows)
        for b in range(blocks):
            cols = slice(b * LANES, (b + 1) * LANES)
            take = jnp.where(rank_ref[j:j + 1, cols] < bound[:, cols], pos_ref[j:j + 1, cols], none)
            comb_ref[j * blocks + b:j * blocks + b + 1, :] = jnp.clip(take.astype(jnp.int32), 0, GROUPS * groups * rows)


def exchange_kernel(
    groups, rows, out_rows, capacity,
    gates_ref, ids_ref, x_hbm, win_ref, wout_ref, out_hbm, load_ref,
    hot, same, count, every, rank_ref, pos_ref, pack_v, lhs_v, ret_v, comb_v, pack_idx, lhs_idx, ret_idx, comb_idx, wide_gates, x_ref,
    xr_rows, send, recv, rf_rows, stage0, stage1, of_rows, rsend, rrecv, retf_rows, wi, wo,
    wsem, ssem, rsem, rssem, rrsem, csend, crecv, tsem, osem,
):
    tokens, model_dim = x_hbm.shape
    sub = model_dim // LANES
    local_experts = win_ref.shape[0]
    group_experts = local_experts // GROUPS
    me = lax.axis_index("expert")
    span = rows * sub
    stages = (stage0, stage1)
    xr, rf, of, retf = (r.reshape(r.shape[0] * sub, LANES) for r in (xr_rows, rf_rows, of_rows, retf_rows))

    def fetch(e, slot):
        a = pltpu.make_async_copy(win_ref.at[e], wi.at[slot], wsem.at[slot, 0])
        b = pltpu.make_async_copy(wout_ref.at[e], wo.at[slot], wsem.at[slot, 1])
        return a, b

    x_copy = pltpu.make_async_copy(x_hbm, x_ref, tsem.at[4])
    x_copy.start()
    for e in range(BUFS):
        for c in fetch(e, e):
            c.start()
    barrier = pltpu.get_barrier_semaphore()
    for k in range(1, groups):
        pl.semaphore_signal(barrier, inc=1, device_id={"expert": lax.rem(me + k, groups)}, device_id_type=MESH)
    retf[pl.ds(GROUPS * groups * span, 8 * sub), :] = jnp.zeros((8 * sub, LANES), jnp.float32)
    experts = same.shape[0]
    i_e, i_f = iota((experts, experts), 0), iota((experts, experts), 1)
    same[:, :experts] = as_bf16((i_e // group_experts == i_f // group_experts) & (i_e < i_f))
    same[:, experts:] = as_bf16((i_e // local_experts == i_f // local_experts) & (i_e < i_f))
    base, counts = local_counts(experts, ids_ref, hot, count)
    x_copy.wait()
    for k in range(sub):
        xr[pl.ds(k, tokens, stride=sub), :] = x_ref[:, k * LANES:(k + 1) * LANES].astype(jnp.float32)
    place_pairs(groups, rows, out_rows, group_experts, base, counts, ids_ref, hot, same, rank_ref, pos_ref, pack_v)
    pack_copy = pltpu.make_async_copy(pack_v, pack_idx, tsem.at[0])
    pack_copy.start()
    pl.semaphore_wait(barrier, groups - 1)

    def count_copy(k):
        return pltpu.make_async_remote_copy(
            src_ref=count, dst_ref=every.at[me], send_sem=csend.at[k], recv_sem=crecv.at[k],
            device_id={"expert": lax.rem(me + k, groups)}, device_id_type=MESH)

    for k in range(1, groups):
        count_copy(k).start()
    pack_copy.wait()

    def gather_rows(idx, line, low, high, table, dst):
        def some(at, col, first, size):
            for c in range(size // 16):
                got = [table[idx[at, col + c * 16 + r]] for r in range(16)]
                dst[pl.ds(pl.multiple_of((first + c * 16) * sub, 16 * sub), 16 * sub), :] = jnp.concatenate(got, axis=0).astype(jnp.bfloat16)

        head = -low % LANES
        if head:
            some(line + low // LANES, low % LANES, 0, head)
        lines, rest = divmod(high - low - head, LANES)
        first = (low + head) // LANES

        def body(i, carry):
            some(line + first + i, 0, head + i * LANES, LANES)
            return carry

        lax.fori_loop(0, lines, body, 0)
        if rest:
            some(line + first + lines, 0, head + lines * LANES, rest)

    def widen(src, dst, first):
        def body(c, carry):
            part = pl.multiple_of(c * 16 * sub, 16 * sub)
            dst[pl.ds(pl.multiple_of(first + part, 16), 16 * sub), :] = src[pl.ds(part, 16 * sub), :].astype(jnp.float32)
            return carry
        lax.fori_loop(0, src.shape[0] // (16 * sub), body, 0)

    def out_part(ref, g, peer):
        low, high = ((0, rows), (rows, out_rows))[g]
        return ref.at[peer, pl.ds(low * sub, (high - low) * sub)]

    def back_part(ref, g, peer):
        return ref.at[g, peer]

    def copy_to(part, src, dst, g, k, s_sem, r_sem):
        peer = lax.rem(me + k, groups)
        return pltpu.make_async_remote_copy(
            src_ref=part(src, g, peer), dst_ref=part(dst, g, me), send_sem=s_sem.at[g, k], recv_sem=r_sem.at[g, k],
            device_id={"expert": peer}, device_id_type=MESH)

    def send_blocks(g, part, gather, src, dst, s_sem, r_sem):
        def body(i, carry):
            peer = lax.rem(me + i + 1, groups)
            gather(peer, part(src, g, peer))

            @pl.when(i >= 1)
            def _():
                copy_to(part, src, dst, g, i, s_sem, r_sem).start()

            return carry

        lax.fori_loop(0, groups, body, 0)

    def take_blocks(g, part, src, dst, own, first, s_sem, r_sem):
        widen(part(own, g, me), dst, first(me))

        def body(k, carry):
            peer = lax.rem(me - k + groups, groups)
            pltpu.make_async_remote_copy(
                src_ref=part(own, g, peer), dst_ref=part(src, g, peer), send_sem=s_sem.at[g, k], recv_sem=r_sem.at[g, k],
                device_id={"expert": peer}, device_id_type=MESH).wait_recv()
            widen(part(src, g, peer), dst, first(peer))
            return carry

        lax.fori_loop(1, groups, body, 0)

    out_lines, back_lines = -(-out_rows // LANES), -(-rows // LANES)
    for g in range(GROUPS):
        low, high = ((0, rows), (rows, out_rows))[g]
        send_blocks(g, out_part, lambda peer, dst: gather_rows(pack_idx, peer * out_lines, low, high, xr_rows, dst), send, recv, ssem, rsem)

    every[me] = count[...]
    for j in range(2):
        for b in range(tokens // LANES):
            part = slice(b * LANES, (b + 1) * LANES)
            wide_gates[j, part, :] = jnp.broadcast_to(gates_ref[j:j + 1, part], (LANES, LANES)).T
    for k in range(1, groups):
        source = lax.rem(me - k + groups, groups)
        pltpu.make_async_remote_copy(
            src_ref=count, dst_ref=every.at[source], send_sem=csend.at[k], recv_sem=crecv.at[k],
            device_id={"expert": source}, device_id_type=MESH).wait_recv()
    group_tables(me, groups, rows, out_rows, group_experts, capacity, every, ids_ref, hot, same, rank_ref, pos_ref, lhs_v, ret_v, comb_v, load_ref)
    tables = [pltpu.make_async_copy(a, b, tsem.at[i + 1]) for i, (a, b) in enumerate(((lhs_v, lhs_idx), (ret_v, ret_idx), (comb_v, comb_idx)))]
    for t in tables:
        t.start()
    for t in tables:
        t.wait()

    for g in range(GROUPS):
        take_blocks(g, out_part, recv, rf, send, lambda peer: (peer * out_rows + g * rows) * sub, ssem, rsem)

        def gather_lhs(e, stage):
            for q in range(capacity):
                stage[pl.ds(q * sub, sub), :] = rf_rows[lhs_idx[e, q]]

        def ffn(e, stage):
            slot = lax.rem(e, BUFS)
            for c in fetch(e, slot):
                c.wait()
            lhs = jnp.concatenate([stage[pl.ds(k, capacity, stride=sub), :] for k in range(sub)], axis=1).astype(jnp.bfloat16)
            hidden = jax.nn.gelu(dot_f32(lhs, wi[slot])).astype(jnp.bfloat16)
            out = dot_f32(hidden, wo[slot]).astype(jnp.bfloat16).astype(jnp.float32)
            at = (e - g * group_experts) * capacity * sub
            for k in range(sub):
                of[pl.ds(at + k, capacity, stride=sub), :] = out[:, k * LANES:(k + 1) * LANES]

        def body(i, carry):
            for half in range(2):
                e = g * group_experts + i * 2 + half
                gather_lhs(e, stages[half])
                ffn(e, stages[half])

                @pl.when(e + BUFS < local_experts)
                def _():
                    for c in fetch(e + BUFS, lax.rem(e, BUFS)):
                        c.start()
            return carry

        lax.fori_loop(0, group_experts // 2, body, 0)
        send_blocks(g, back_part, lambda peer, dst: gather_rows(ret_idx, (g * groups + peer) * back_lines, 0, rows, of_rows, dst), rsend, rrecv, rssem, rrsem)

    for g in range(GROUPS):
        take_blocks(g, back_part, rrecv, retf, rsend, lambda peer: (g * groups + peer) * span, rssem, rrsem)

    half = tokens // LANES

    def combine(line, carry):
        for c in range(LANES // 16):
            got = []
            for r in range(16):
                col = c * 16 + r
                row = xr_rows[line * LANES + col]
                for j in range(2):
                    row = row + wide_gates[j, pl.ds(pl.multiple_of(line * LANES, LANES) + col, 1), :] * retf_rows[comb_idx[j * half + line, col]]
                got.append(row)
            xr[pl.ds(pl.multiple_of((line * LANES + c * 16) * sub, 16 * sub), 16 * sub), :] = jnp.concatenate(got, axis=0)
        part = pl.ds(pl.multiple_of(line * LANES, LANES), LANES)
        for k in range(sub):
            x_ref[part, k * LANES:(k + 1) * LANES] = xr[pl.ds(line * LANES * sub + k, LANES, stride=sub), :].astype(jnp.bfloat16)

        @pl.when(line >= 1)
        def _():
            put(line - 1).start()

        return carry

    def put(line):
        part = pl.ds(pl.multiple_of(line * LANES, LANES), LANES)
        return pltpu.make_async_copy(x_ref.at[part], out_hbm.at[part], osem.at[line])

    lax.fori_loop(0, half, combine, 0)
    put(half - 1).start()
    for line in range(half):
        put(line).wait()
    for g in range(GROUPS):
        for k in range(1, groups):
            if g == 0:
                count_copy(k).wait_send()
            copy_to(out_part, send, recv, g, k, ssem, rsem).wait_send()
            copy_to(back_part, rsend, rrecv, g, k, rssem, rrsem).wait_send()


def compact_step(groups, rows, out_rows, capacity, gates, ids, token_rows, w_in, w_out):
    tokens, model_dim = token_rows.shape
    local_experts, _, hidden_dim = w_in.shape
    experts = local_experts * groups
    group_experts = local_experts // GROUPS
    sub = model_dim // LANES
    span = rows * sub
    vmem = pl.BlockSpec(memory_space=pltpu.VMEM)
    hbm = pl.BlockSpec(memory_space=pl.ANY)
    wire = pltpu.VMEM((GROUPS, groups, span, LANES), jnp.bfloat16)
    sems = pltpu.SemaphoreType.DMA((GROUPS, groups))
    table_rows = (
        groups * -(-out_rows // LANES),
        local_experts,
        GROUPS * groups * -(-rows // LANES),
        2 * tokens // LANES,
    )
    return pl.pallas_call(
        functools.partial(exchange_kernel, groups, rows, out_rows, capacity),
        out_shape=(jax.ShapeDtypeStruct((tokens, model_dim), jnp.bfloat16), jax.ShapeDtypeStruct((1, 1), jnp.float32)),
        in_specs=[vmem, vmem, hbm, hbm, hbm],
        out_specs=(hbm, vmem),
        scratch_shapes=[
            pltpu.VMEM((2, LANES, tokens), jnp.bfloat16),
            pltpu.VMEM((experts, 2 * experts), jnp.bfloat16),
            pltpu.VMEM((8, experts), jnp.float32),
            pltpu.VMEM((groups, 8, experts), jnp.float32),
            pltpu.VMEM((8, tokens), jnp.float32),
            pltpu.VMEM((8, tokens), jnp.float32),
            *[pltpu.VMEM((r, LANES), jnp.int32) for r in table_rows],
            *[pltpu.SMEM((r, LANES), jnp.int32) for r in table_rows],
            pltpu.VMEM((2, tokens, LANES), jnp.float32),
            pltpu.VMEM((tokens, model_dim), jnp.bfloat16),
            pltpu.VMEM((tokens, sub, LANES), jnp.float32),
            pltpu.VMEM((groups, out_rows * sub, LANES), jnp.bfloat16),
            pltpu.VMEM((groups, out_rows * sub, LANES), jnp.bfloat16),
            pltpu.VMEM((groups * out_rows, sub, LANES), jnp.float32),
            pltpu.VMEM((capacity * sub, LANES), jnp.float32),
            pltpu.VMEM((capacity * sub, LANES), jnp.float32),
            pltpu.VMEM((group_experts * capacity, sub, LANES), jnp.float32),
            wire,
            wire,
            pltpu.VMEM((GROUPS * groups * rows + 8, sub, LANES), jnp.float32),
            pltpu.VMEM((BUFS, model_dim, hidden_dim), jnp.bfloat16),
            pltpu.VMEM((BUFS, hidden_dim, model_dim), jnp.bfloat16),
            pltpu.SemaphoreType.DMA((BUFS, 2)),
            sems, sems, sems, sems,
            pltpu.SemaphoreType.DMA((groups,)),
            pltpu.SemaphoreType.DMA((groups,)),
            pltpu.SemaphoreType.DMA((5,)),
            pltpu.SemaphoreType.DMA((tokens // LANES,)),
        ],
        compiler_params=pltpu.CompilerParams(collective_id=0, has_side_effects=True, vmem_limit_bytes=67043328),
        name="expert_exchange",
    )(gates, ids, token_rows, w_in, w_out)


def hand_over(rows):
    parts = 8
    size = rows.shape[0] // parts

    def kernel(a_ref, o_ref, buf, sem_in, sem_out):
        part = [pl.ds(i * size, size) for i in range(parts)]
        take = [pltpu.make_async_copy(a_ref.at[p], buf.at[p], sem_in.at[i]) for i, p in enumerate(part)]
        give = [pltpu.make_async_copy(buf.at[p], o_ref.at[p], sem_out.at[i]) for i, p in enumerate(part)]
        for t in take:
            t.start()
        for t, g in zip(take, give):
            t.wait()
            g.start()
        for g in give:
            g.wait()

    return pl.pallas_call(
        kernel,
        in_specs=[pl.BlockSpec(memory_space=pl.ANY)],
        out_specs=pl.BlockSpec(memory_space=pl.ANY),
        out_shape=jax.ShapeDtypeStruct(rows.shape, rows.dtype),
        scratch_shapes=[pltpu.VMEM(rows.shape, rows.dtype), pltpu.SemaphoreType.DMA((parts,)), pltpu.SemaphoreType.DMA((parts,))],
        name="hand_over",
    )(rows)


def solution(mesh):
    groups = mesh.shape["expert"]
    row_spec = P(("data", "expert"), None)
    weight_spec = P("expert", None, None)

    def device_step(token_rows, expert_ids, gate_weights, w_in, w_out):
        tokens, top_k = expert_ids.shape
        local_experts = w_in.shape[0]
        capacity = tokens * top_k // local_experts
        rows = block_rows(tokens, top_k, groups)
        fast, load = compact_step(groups, rows, total_rows(tokens, top_k, groups), capacity, gate_weights.T, expert_ids.T, token_rows, w_in, w_out)
        fast = hand_over(fast)
        overflow = load[0, 0] > 0.0
        general = lambda state: (jnp.array(False), padded_step(groups, token_rows, expert_ids, gate_weights, w_in, w_out))
        return lax.while_loop(lambda state: state[0], general, (overflow, fast))[1]

    return jax.shard_map(device_step, mesh=mesh, in_specs=(row_spec, row_spec, row_spec, weight_spec, weight_spec), out_specs=row_spec, check_vma=False)
```

```python
import functools

import jax
import jax.numpy as jnp
from jax import lax
from jax.experimental import pallas as pl
from jax.experimental.pallas import tpu as pltpu
from jax.sharding import PartitionSpec as P

GROUPS = 2
BUFS = 5
LANES = 128
MESH = pl.DeviceIdType.MESH


def route_local(expert_ids, experts):
    ids_t = expert_ids.T
    onehot = (ids_t[:, :, None] == jnp.arange(experts, dtype=jnp.int32)).astype(jnp.int32)
    running = jnp.cumsum(onehot, axis=1)
    counts = running[:, -1, :]
    rank_local = jnp.sum(onehot * running, axis=2) - 1
    return ids_t, counts, rank_local


def padded_step(groups, token_rows, expert_ids, gate_weights, w_in, w_out):
    tokens, top_k = expert_ids.shape
    local_experts, model_dim = w_in.shape[0], w_in.shape[1]
    experts = local_experts * groups
    mean_load = tokens * top_k // experts
    send_cap = -(-(7 * mean_load // 4) // 16) * 16
    capacity = groups * mean_load
    rows_total = experts * send_cap
    ids_t, counts, rank_local = route_local(expert_ids, experts)
    inclusive = counts
    shift = 1
    while shift < groups:
        pairs_list = [(source, source + shift) for source in range(groups - shift)]
        inclusive = inclusive + lax.ppermute(inclusive, "expert", pairs_list)
        shift = shift * 2
    before = inclusive - counts
    totals = lax.psum(counts, "expert")
    prior = jnp.cumsum(totals, axis=0) - totals
    within = jnp.cumsum(counts, axis=0) - counts
    slot = jnp.take_along_axis(prior + before, ids_t, axis=1) + rank_local
    keep = slot < capacity
    target = ids_t * send_cap + jnp.take_along_axis(within, ids_t, axis=1) + rank_local
    token_ids = jnp.broadcast_to(jnp.arange(tokens, dtype=jnp.int32), (top_k, tokens))
    source_row = jnp.full((rows_total,), tokens, jnp.int32).at[jnp.where(keep, target, rows_total).reshape(-1)].set(token_ids.reshape(-1), mode="drop")
    padded = jnp.concatenate([token_rows, jnp.zeros((1, model_dim), token_rows.dtype)], axis=0)
    outbound = jnp.take(padded, source_row, axis=0).reshape(experts, send_cap, model_dim)
    inbound = lax.all_to_all(outbound, "expert", 0, 0, tiled=True).reshape(groups, local_experts, send_cap, model_dim)

    def one_expert(e, total):
        rows = lax.dynamic_index_in_dim(inbound, e, 1, keepdims=False).reshape(groups * send_cap, model_dim)
        hidden = jax.nn.gelu(jnp.dot(rows, w_in[e], preferred_element_type=jnp.float32)).astype(jnp.bfloat16)
        out = jnp.dot(hidden, w_out[e], preferred_element_type=jnp.float32).astype(jnp.bfloat16)
        return lax.dynamic_update_index_in_dim(total, out.reshape(groups, send_cap, model_dim), e, 1)

    expert_out = lax.fori_loop(0, local_experts, one_expert, jnp.zeros_like(inbound))
    returned = lax.all_to_all(expert_out.reshape(experts, send_cap, model_dim), "expert", 0, 0, tiled=True).reshape(rows_total, model_dim)
    picked = jnp.take(returned, target, axis=0)
    weight = jnp.where(keep, gate_weights.T, 0.0)
    mixed = jnp.sum(weight[:, :, None] * picked.astype(jnp.float32), axis=0)
    return (token_rows.astype(jnp.float32) + mixed).astype(jnp.bfloat16)


def block_rows(tokens, top_k, groups):
    mean = tokens * top_k // (groups * GROUPS)
    return (mean * 19 // 16 + 15) // 16 * 16


def total_rows(tokens, top_k, groups):
    return (tokens * top_k // groups * 9 // 8 + 15) // 16 * 16


def dot_f32(a, b):
    return jnp.dot(a, b, preferred_element_type=jnp.float32)


def dot_nt(a, b):
    return lax.dot_general(a, b, (((1,), (1,)), ((), ())), preferred_element_type=jnp.float32)


def iota(shape, axis):
    return lax.broadcasted_iota(jnp.int32, shape, axis)


def as_bf16(mask):
    return jnp.where(mask, 1.0, 0.0).astype(jnp.bfloat16)


def pad_rows(rows, total):
    have = sum(r.shape[0] for r in rows)
    if have < total:
        rows = rows + [jnp.zeros((total - have, rows[0].shape[1]), rows[0].dtype)]
    return jnp.concatenate(rows, axis=0)


def select_row(rows, high_row):
    total = jnp.zeros_like(rows[0])
    for i, row in enumerate(rows):
        total = total + jnp.where(high_row == i, row, 0.0)
    return total


def split_lanes(row):
    return [row[:, i * LANES:(i + 1) * LANES] for i in range(row.shape[1] // LANES)]


def local_counts(experts, ids_ref, hot, count_ref):
    tokens = ids_ref.shape[1]
    blocks = tokens // LANES
    highs = experts // LANES

    def fill(b, carry):
        at = pl.ds(pl.multiple_of(b * LANES, LANES), LANES)
        for j in range(2):
            hot[j, :, at] = as_bf16(iota((LANES, LANES), 0) == ids_ref[j:j + 1, at] % LANES)
        return carry

    lax.fori_loop(0, blocks, fill, 0)
    n = highs * blocks
    row, col = iota((n, n), 0), iota((n, n), 1)
    below = as_bf16((row // blocks == col // blocks) & (row > col))
    in_block = iota((n, tokens), 0) % blocks == iota((n, tokens), 1) // LANES
    base, count = [], []
    for j in range(2):
        part = as_bf16(in_block & (iota((n, tokens), 0) // blocks == ids_ref[j:j + 1, :] // LANES))
        per_block = dot_nt(part, hot[j])
        base.append(dot_f32(below, per_block.astype(jnp.bfloat16)))
        count.append(jnp.concatenate([jnp.sum(per_block[i * blocks:(i + 1) * blocks], axis=0, keepdims=True) for i in range(highs)], axis=1))
    count_ref[...] = pad_rows(count, 8)
    return base, count


def place_pairs(groups, rows, out_rows, group_experts, base, count, ids_ref, hot, same, rank_ref, pos_ref, pack_ref):
    tokens = ids_ref.shape[1]
    experts = same.shape[0]
    blocks = tokens // LANES
    highs = experts // LANES
    local_experts = experts // groups
    both = pad_rows([count[0] + count[1]], 8)
    start = dot_f32(both.astype(jnp.bfloat16), same[...])[0:1]
    lane = iota((1, experts), 1)
    block_of = (lane % local_experts // group_experts) * groups + lane // local_experts
    stride = -(-out_rows // LANES) * LANES
    back_first = (block_of * rows).astype(jnp.float32) + start[:, :experts]
    out_first = (lane // local_experts * stride).astype(jnp.float32) + start[:, experts:]
    earlier = iota((LANES, LANES), 0) < iota((LANES, LANES), 1)
    found = None
    table_rows = pack_ref.shape[0]
    n = highs * blocks
    for j in range(2):
        lhs = [base[j]]
        for first in (out_first, back_first):
            at = first if j == 0 else first + count[0]
            coarse = jnp.floor(at * (1.0 / 64.0))
            lhs += split_lanes(coarse) + split_lanes(at - 64.0 * coarse)
        look = dot_f32(pad_rows(lhs, -(-(n + 4 * highs) // 16) * 16).astype(jnp.bfloat16), hot[j])
        for b in range(blocks):
            cols = slice(b * LANES, (b + 1) * LANES)
            row = ids_ref[j:j + 1, cols]
            high_row = row // LANES
            wide = jnp.broadcast_to(row.astype(jnp.float32), (LANES, LANES))
            same_id = (wide.T == wide) & earlier
            rank = jnp.sum(jnp.where(same_id, 1.0, 0.0), axis=0, keepdims=True)
            rank = rank + select_row([look[i * blocks + b:i * blocks + b + 1, cols] for i in range(highs)], high_row)
            offsets = []
            for m in (n, n + 2 * highs):
                offsets.append(select_row([64.0 * look[m + i:m + i + 1, cols] + look[m + highs + i:m + highs + i + 1, cols] for i in range(highs)], high_row))
            rank_ref[j:j + 1, cols] = rank
            pos_ref[j + 2:j + 3, cols] = rank + offsets[0]
            pos_ref[j:j + 1, cols] = rank + offsets[1]
        pos = pos_ref[j + 2:j + 3, :].astype(jnp.int32)
        token = iota((LANES, tokens), 1)
        high_t = as_bf16(iota((table_rows, tokens), 0) == pos // LANES)
        low = iota((LANES, tokens), 0) == pos % LANES
        low_hi = jnp.where(low, (token // 8).astype(jnp.float32), 0.0).astype(jnp.bfloat16)
        low_lo = jnp.where(low, (token % 8).astype(jnp.float32), 0.0).astype(jnp.bfloat16)
        hit = 8.0 * dot_nt(high_t, low_hi) + dot_nt(high_t, low_lo)
        found = hit if found is None else found + hit
    pack_ref[...] = jnp.clip(found.astype(jnp.int32), 0, tokens - 1)


def group_tables(me, groups, rows, out_rows, group_experts, capacity, every, ids_ref, hot, same, rank_ref, pos_ref, lhs_ref, ret_ref, comb_ref, load_ref):
    experts = same.shape[0]
    tokens = hot.shape[2]
    local_experts = experts // groups
    blocks = tokens // LANES
    c = [[every[s, j:j + 1, :] for s in range(groups)] for j in range(2)]
    both = pad_rows([c[0][s] + c[1][s] for s in range(groups)], 8)
    starts = dot_f32(both.astype(jnp.bfloat16), same[...])
    start, out_start = starts[:, :experts], starts[:, experts:]
    over = jnp.maximum(jnp.max(start + both) - rows, jnp.max(out_start + both) - out_rows)
    load_ref[...] = jnp.broadcast_to(over, load_ref.shape)
    kept = [[None] * groups, [None] * groups]
    used = jnp.zeros((1, experts), jnp.float32)
    for j in range(2):
        for s in range(groups):
            kept[j][s] = jnp.clip(capacity - used, 0.0, c[j][s])
            used = used + c[j][s]
    lane = iota((1, experts), 1)
    in_group = lane % group_experts
    slot = jnp.zeros((1, experts), jnp.float32)
    slots, steps, edges, jumps = [], [], [], []
    last = jnp.zeros((1, experts), jnp.float32)
    for s in range(groups):
        ret_v = []
        for j in range(2):
            edge = start[s:s + 1] if j == 0 else start[s:s + 1] + c[0][s]
            v = s * out_rows + edge + out_start[s:s + 1] - start[s:s + 1] - slot
            slots.append(slot)
            steps.append(v - last)
            last = v
            edges.append(edge)
            ret_v.append((in_group * capacity).astype(jnp.float32) + slot - edge)
            slot = slot + kept[j][s]
        before = jnp.concatenate([jnp.zeros((1, 1), jnp.float32), ret_v[1][:, :-1]], axis=1)
        jumps.append(ret_v[0] - jnp.where(in_group == 0, 0.0, before))
        jumps.append(ret_v[1] - ret_v[0])

    def mine(parts):
        a = jnp.concatenate(parts, axis=0)
        total = jnp.zeros((a.shape[0], local_experts), jnp.float32)
        for d in range(groups):
            total = total + jnp.where(me == d, a[:, d * local_experts:(d + 1) * local_experts], 0.0)
        return total

    slots, steps, edges, jumps = mine(slots), mine(steps), mine(edges), mine(jumps)
    tall = pad_rows([edges, jumps, slots, steps], LANES)
    tall = jnp.concatenate([tall, jnp.zeros((LANES, LANES - local_experts), jnp.float32)], axis=1).T if local_experts < LANES else tall.T
    q = iota((local_experts, LANES), 1).astype(jnp.float32)
    lhs = q
    for i in range(2 * groups):
        at = 4 * groups + i
        lhs = lhs + jnp.where(q >= tall[:local_experts, at:at + 1], tall[:local_experts, at + 2 * groups:at + 2 * groups + 1], 0.0)
    lhs_ref[...] = jnp.clip(lhs.astype(jnp.int32), 0, groups * out_rows - 1)

    width = -(-rows // LANES) * LANES
    p = iota((1, width), 1).astype(jnp.float32)
    for g in range(GROUPS):
        part = tall[g * group_experts:(g + 1) * group_experts]
        for s in range(groups):
            total = jnp.zeros((group_experts, width), jnp.float32)
            for j in range(2):
                i = 2 * s + j
                total = total + jnp.where(p >= part[:, i:i + 1], part[:, 2 * groups + i:2 * groups + i + 1], 0.0)
            row = p + jnp.sum(total, axis=0, keepdims=True)
            row = jnp.clip(row.astype(jnp.int32), 0, group_experts * capacity - 1)
            for i in range(width // LANES):
                at = (g * groups + s) * (width // LANES) + i
                ret_ref[at:at + 1, :] = row[:, i * LANES:(i + 1) * LANES]

    for j in range(2):
        own = jnp.zeros((1, experts), jnp.float32)
        for s in range(groups):
            own = own + jnp.where(me == s, kept[j][s], 0.0)
        bound = dot_f32(pad_rows(split_lanes(own), 16).astype(jnp.bfloat16), hot[j])
        bound = select_row([bound[i:i + 1] for i in range(experts // LANES)], ids_ref[j:j + 1, :] // LANES)
        none = float(GROUPS * groups * rows)
        for b in range(blocks):
            cols = slice(b * LANES, (b + 1) * LANES)
            take = jnp.where(rank_ref[j:j + 1, cols] < bound[:, cols], pos_ref[j:j + 1, cols], none)
            comb_ref[j * blocks + b:j * blocks + b + 1, :] = jnp.clip(take.astype(jnp.int32), 0, GROUPS * groups * rows)


def exchange_kernel(
    groups, rows, out_rows, capacity,
    gates_ref, ids_ref, x_hbm, win_ref, wout_ref, out_hbm, load_ref,
    hot, same, count, every, rank_ref, pos_ref, pack_v, lhs_v, ret_v, comb_v, pack_idx, lhs_idx, ret_idx, comb_idx, wide_gates, x_ref,
    xr_rows, send, recv, rf_rows, stage0, stage1, of_rows, rsend, rrecv, retf_rows, wi, wo,
    wsem, ssem, rsem, rssem, rrsem, csend, crecv, tsem, osem,
):
    tokens, model_dim = x_hbm.shape
    sub = model_dim // LANES
    local_experts = win_ref.shape[0]
    group_experts = local_experts // GROUPS
    me = lax.axis_index("expert")
    span = rows * sub
    bits = [2 ** b for b in range(groups.bit_length() - 1)]
    stages = (stage0, stage1)
    xr, rf, of, retf = (r.reshape(r.shape[0] * sub, LANES) for r in (xr_rows, rf_rows, of_rows, retf_rows))

    def fetch(e, slot):
        a = pltpu.make_async_copy(win_ref.at[e], wi.at[slot], wsem.at[slot, 0])
        b = pltpu.make_async_copy(wout_ref.at[e], wo.at[slot], wsem.at[slot, 1])
        return a, b

    x_copy = pltpu.make_async_copy(x_hbm, x_ref, tsem.at[4])
    x_copy.start()
    for e in range(BUFS):
        for c in fetch(e, e):
            c.start()
    barrier = pltpu.get_barrier_semaphore()
    for k in range(1, groups):
        pl.semaphore_signal(barrier, inc=1, device_id={"expert": lax.rem(me + k, groups)}, device_id_type=MESH)
    retf[pl.ds(GROUPS * groups * span, 8 * sub), :] = jnp.zeros((8 * sub, LANES), jnp.float32)
    experts = same.shape[0]
    i_e, i_f = iota((experts, experts), 0), iota((experts, experts), 1)
    same[:, :experts] = as_bf16((i_e // group_experts == i_f // group_experts) & (i_e < i_f))
    same[:, experts:] = as_bf16((i_e // local_experts == i_f // local_experts) & (i_e < i_f))
    base, counts = local_counts(experts, ids_ref, hot, count)
    x_copy.wait()
    for k in range(sub):
        xr[pl.ds(k, tokens, stride=sub), :] = x_ref[:, k * LANES:(k + 1) * LANES].astype(jnp.float32)
    place_pairs(groups, rows, out_rows, group_experts, base, counts, ids_ref, hot, same, rank_ref, pos_ref, pack_v)
    pack_copy = pltpu.make_async_copy(pack_v, pack_idx, tsem.at[0])
    pack_copy.start()
    pl.semaphore_wait(barrier, groups - 1)

    def count_copy(k):
        return pltpu.make_async_remote_copy(
            src_ref=count, dst_ref=every.at[me], send_sem=csend.at[k], recv_sem=crecv.at[k],
            device_id={"expert": lax.rem(me + k, groups)}, device_id_type=MESH)

    for k in range(1, groups):
        count_copy(k).start()
    pack_copy.wait()

    def gather_rows(idx, line, low, high, table, dst):
        def some(at, col, first, size):
            for c in range(size // 16):
                got = [table[idx[at, col + c * 16 + r]] for r in range(16)]
                dst[pl.ds(pl.multiple_of((first + c * 16) * sub, 16 * sub), 16 * sub), :] = jnp.concatenate(got, axis=0).astype(jnp.bfloat16)

        head = -low % LANES
        if head:
            some(line + low // LANES, low % LANES, 0, head)
        lines, rest = divmod(high - low - head, LANES)
        first = (low + head) // LANES

        def body(i, carry):
            some(line + first + i, 0, head + i * LANES, LANES)
            return carry

        lax.fori_loop(0, lines, body, 0)
        if rest:
            some(line + first + lines, 0, head + lines * LANES, rest)

    def widen(src, dst, first):
        def body(c, carry):
            part = pl.multiple_of(c * 16 * sub, 16 * sub)
            dst[pl.ds(pl.multiple_of(first + part, 16), 16 * sub), :] = src[pl.ds(part, 16 * sub), :].astype(jnp.float32)
            return carry
        lax.fori_loop(0, src.shape[0] // (16 * sub), body, 0)

    def out_part(ref, g, peer):
        low, high = ((0, rows), (rows, out_rows))[g]
        return ref.at[peer, pl.ds(low * sub, (high - low) * sub)]

    def back_part(ref, g, peer):
        return ref.at[g, peer]

    def turn(i):
        k = groups - 1 - 2 * (i % (groups // 2)) - i // (groups // 2)
        peer = 0
        for size in bits:
            peer = peer + size * ((me // size + k // size) % 2)
        return k, peer

    def copy_to(part, src, dst, g, i, s_sem, r_sem):
        k, peer = turn(i)
        return pltpu.make_async_remote_copy(
            src_ref=part(src, g, peer), dst_ref=part(dst, g, me), send_sem=s_sem.at[g, k], recv_sem=r_sem.at[g, k],
            device_id={"expert": peer}, device_id_type=MESH)

    def send_blocks(g, part, gather, src, dst, s_sem, r_sem):
        def body(i, carry):
            peer = turn(i)[1]
            gather(peer, part(src, g, peer))

            @pl.when(i >= 1)
            def _():
                copy_to(part, src, dst, g, i - 1, s_sem, r_sem).start()

            return carry

        lax.fori_loop(0, groups, body, 0)

    def take_blocks(g, part, src, dst, own, first, s_sem, r_sem):
        widen(part(own, g, me), dst, first(me))

        def body(i, carry):
            k, peer = turn(i)
            pltpu.make_async_remote_copy(
                src_ref=part(own, g, peer), dst_ref=part(src, g, peer), send_sem=s_sem.at[g, k], recv_sem=r_sem.at[g, k],
                device_id={"expert": peer}, device_id_type=MESH).wait_recv()
            widen(part(src, g, peer), dst, first(peer))
            return carry

        lax.fori_loop(0, groups - 1, body, 0)

    out_lines, back_lines = -(-out_rows // LANES), -(-rows // LANES)
    for g in range(GROUPS):
        low, high = ((0, rows), (rows, out_rows))[g]
        send_blocks(g, out_part, lambda peer, dst: gather_rows(pack_idx, peer * out_lines, low, high, xr_rows, dst), send, recv, ssem, rsem)

    every[me] = count[...]
    for j in range(2):
        for b in range(tokens // LANES):
            part = slice(b * LANES, (b + 1) * LANES)
            wide_gates[j, part, :] = jnp.broadcast_to(gates_ref[j:j + 1, part], (LANES, LANES)).T
    for k in range(1, groups):
        source = lax.rem(me - k + groups, groups)
        pltpu.make_async_remote_copy(
            src_ref=count, dst_ref=every.at[source], send_sem=csend.at[k], recv_sem=crecv.at[k],
            device_id={"expert": source}, device_id_type=MESH).wait_recv()
    group_tables(me, groups, rows, out_rows, group_experts, capacity, every, ids_ref, hot, same, rank_ref, pos_ref, lhs_v, ret_v, comb_v, load_ref)
    tables = [pltpu.make_async_copy(a, b, tsem.at[i + 1]) for i, (a, b) in enumerate(((lhs_v, lhs_idx), (ret_v, ret_idx), (comb_v, comb_idx)))]
    for t in tables:
        t.start()
    for t in tables:
        t.wait()

    for g in range(GROUPS):
        take_blocks(g, out_part, recv, rf, send, lambda peer: (peer * out_rows + g * rows) * sub, ssem, rsem)

        def gather_lhs(e, stage):
            for q in range(capacity):
                stage[pl.ds(q * sub, sub), :] = rf_rows[lhs_idx[e, q]]

        def ffn(e, stage):
            slot = lax.rem(e, BUFS)
            for c in fetch(e, slot):
                c.wait()
            lhs = jnp.concatenate([stage[pl.ds(k, capacity, stride=sub), :] for k in range(sub)], axis=1).astype(jnp.bfloat16)
            hidden = jax.nn.gelu(dot_f32(lhs, wi[slot])).astype(jnp.bfloat16)
            out = dot_f32(hidden, wo[slot]).astype(jnp.bfloat16).astype(jnp.float32)
            at = (e - g * group_experts) * capacity * sub
            for k in range(sub):
                of[pl.ds(at + k, capacity, stride=sub), :] = out[:, k * LANES:(k + 1) * LANES]

        def body(i, carry):
            for half in range(2):
                e = g * group_experts + i * 2 + half
                gather_lhs(e, stages[half])
                ffn(e, stages[half])

                @pl.when(e + BUFS < local_experts)
                def _():
                    for c in fetch(e + BUFS, lax.rem(e, BUFS)):
                        c.start()
            return carry

        lax.fori_loop(0, group_experts // 2, body, 0)
        send_blocks(g, back_part, lambda peer, dst: gather_rows(ret_idx, (g * groups + peer) * back_lines, 0, rows, of_rows, dst), rsend, rrecv, rssem, rrsem)

    for g in range(GROUPS):
        take_blocks(g, back_part, rrecv, retf, rsend, lambda peer: (g * groups + peer) * span, rssem, rrsem)

    half = tokens // LANES

    def combine(line, carry):
        for c in range(LANES // 16):
            got = []
            for r in range(16):
                col = c * 16 + r
                row = xr_rows[line * LANES + col]
                for j in range(2):
                    row = row + wide_gates[j, pl.ds(pl.multiple_of(line * LANES, LANES) + col, 1), :] * retf_rows[comb_idx[j * half + line, col]]
                got.append(row)
            xr[pl.ds(pl.multiple_of((line * LANES + c * 16) * sub, 16 * sub), 16 * sub), :] = jnp.concatenate(got, axis=0)
        part = pl.ds(pl.multiple_of(line * LANES, LANES), LANES)
        for k in range(sub):
            x_ref[part, k * LANES:(k + 1) * LANES] = xr[pl.ds(line * LANES * sub + k, LANES, stride=sub), :].astype(jnp.bfloat16)

        @pl.when(line >= 1)
        def _():
            put(line - 1).start()

        return carry

    def put(line):
        part = pl.ds(pl.multiple_of(line * LANES, LANES), LANES)
        return pltpu.make_async_copy(x_ref.at[part], out_hbm.at[part], osem.at[line])

    lax.fori_loop(0, half, combine, 0)
    put(half - 1).start()
    for line in range(half):
        put(line).wait()
    for g in range(GROUPS):
        for i in range(groups - 1):
            if g == 0:
                count_copy(i + 1).wait_send()
            copy_to(out_part, send, recv, g, i, ssem, rsem).wait_send()
            copy_to(back_part, rsend, rrecv, g, i, rssem, rrsem).wait_send()


def compact_step(groups, rows, out_rows, capacity, gates, ids, token_rows, w_in, w_out):
    tokens, model_dim = token_rows.shape
    local_experts, _, hidden_dim = w_in.shape
    experts = local_experts * groups
    group_experts = local_experts // GROUPS
    sub = model_dim // LANES
    span = rows * sub
    vmem = pl.BlockSpec(memory_space=pltpu.VMEM)
    hbm = pl.BlockSpec(memory_space=pl.ANY)
    wire = pltpu.VMEM((GROUPS, groups, span, LANES), jnp.bfloat16)
    sems = pltpu.SemaphoreType.DMA((GROUPS, groups))
    table_rows = (
        groups * -(-out_rows // LANES),
        local_experts,
        GROUPS * groups * -(-rows // LANES),
        2 * tokens // LANES,
    )
    return pl.pallas_call(
        functools.partial(exchange_kernel, groups, rows, out_rows, capacity),
        out_shape=(jax.ShapeDtypeStruct((tokens, model_dim), jnp.bfloat16), jax.ShapeDtypeStruct((1, 1), jnp.float32)),
        in_specs=[vmem, vmem, hbm, hbm, hbm],
        out_specs=(hbm, vmem),
        scratch_shapes=[
            pltpu.VMEM((2, LANES, tokens), jnp.bfloat16),
            pltpu.VMEM((experts, 2 * experts), jnp.bfloat16),
            pltpu.VMEM((8, experts), jnp.float32),
            pltpu.VMEM((groups, 8, experts), jnp.float32),
            pltpu.VMEM((8, tokens), jnp.float32),
            pltpu.VMEM((8, tokens), jnp.float32),
            *[pltpu.VMEM((r, LANES), jnp.int32) for r in table_rows],
            *[pltpu.SMEM((r, LANES), jnp.int32) for r in table_rows],
            pltpu.VMEM((2, tokens, LANES), jnp.float32),
            pltpu.VMEM((tokens, model_dim), jnp.bfloat16),
            pltpu.VMEM((tokens, sub, LANES), jnp.float32),
            pltpu.VMEM((groups, out_rows * sub, LANES), jnp.bfloat16),
            pltpu.VMEM((groups, out_rows * sub, LANES), jnp.bfloat16),
            pltpu.VMEM((groups * out_rows, sub, LANES), jnp.float32),
            pltpu.VMEM((capacity * sub, LANES), jnp.float32),
            pltpu.VMEM((capacity * sub, LANES), jnp.float32),
            pltpu.VMEM((group_experts * capacity, sub, LANES), jnp.float32),
            wire,
            wire,
            pltpu.VMEM((GROUPS * groups * rows + 8, sub, LANES), jnp.float32),
            pltpu.VMEM((BUFS, model_dim, hidden_dim), jnp.bfloat16),
            pltpu.VMEM((BUFS, hidden_dim, model_dim), jnp.bfloat16),
            pltpu.SemaphoreType.DMA((BUFS, 2)),
            sems, sems, sems, sems,
            pltpu.SemaphoreType.DMA((groups,)),
            pltpu.SemaphoreType.DMA((groups,)),
            pltpu.SemaphoreType.DMA((5,)),
            pltpu.SemaphoreType.DMA((tokens // LANES,)),
        ],
        compiler_params=pltpu.CompilerParams(collective_id=0, has_side_effects=True, vmem_limit_bytes=67043328),
        name="expert_exchange",
    )(gates, ids, token_rows, w_in, w_out)


def hand_over(rows):
    parts = 8
    size = rows.shape[0] // parts

    def kernel(a_ref, o_ref, buf, sem_in, sem_out):
        part = [pl.ds(i * size, size) for i in range(parts)]
        take = [pltpu.make_async_copy(a_ref.at[p], buf.at[p], sem_in.at[i]) for i, p in enumerate(part)]
        give = [pltpu.make_async_copy(buf.at[p], o_ref.at[p], sem_out.at[i]) for i, p in enumerate(part)]
        for t in take:
            t.start()
        for t, g in zip(take, give):
            t.wait()
            g.start()
        for g in give:
            g.wait()

    return pl.pallas_call(
        kernel,
        in_specs=[pl.BlockSpec(memory_space=pl.ANY)],
        out_specs=pl.BlockSpec(memory_space=pl.ANY),
        out_shape=jax.ShapeDtypeStruct(rows.shape, rows.dtype),
        scratch_shapes=[pltpu.VMEM(rows.shape, rows.dtype), pltpu.SemaphoreType.DMA((parts,)), pltpu.SemaphoreType.DMA((parts,))],
        name="hand_over",
    )(rows)


def solution(mesh):
    groups = mesh.shape["expert"]
    row_spec = P(("data", "expert"), None)
    weight_spec = P("expert", None, None)

    def device_step(token_rows, expert_ids, gate_weights, w_in, w_out):
        tokens, top_k = expert_ids.shape
        local_experts = w_in.shape[0]
        capacity = tokens * top_k // local_experts
        rows = block_rows(tokens, top_k, groups)
        fast, load = compact_step(groups, rows, total_rows(tokens, top_k, groups), capacity, gate_weights.T, expert_ids.T, token_rows, w_in, w_out)
        fast = hand_over(fast)
        overflow = load[0, 0] > 0.0
        general = lambda state: (jnp.array(False), padded_step(groups, token_rows, expert_ids, gate_weights, w_in, w_out))
        return lax.while_loop(lambda state: state[0], general, (overflow, fast))[1]

    return jax.shard_map(device_step, mesh=mesh, in_specs=(row_spec, row_spec, row_spec, weight_spec, weight_spec), out_specs=row_spec, check_vma=False)
```

```python
import functools

import jax
import jax.numpy as jnp
from jax import lax
from jax.experimental import pallas as pl
from jax.experimental.pallas import tpu as pltpu
from jax.sharding import PartitionSpec as P

GROUPS = 2
BUFS = 4
LANES = 128
MESH = pl.DeviceIdType.MESH


def route_local(expert_ids, experts):
    ids_t = expert_ids.T
    onehot = (ids_t[:, :, None] == jnp.arange(experts, dtype=jnp.int32)).astype(jnp.int32)
    running = jnp.cumsum(onehot, axis=1)
    counts = running[:, -1, :]
    rank_local = jnp.sum(onehot * running, axis=2) - 1
    return ids_t, counts, rank_local


def padded_step(groups, token_rows, expert_ids, gate_weights, w_in, w_out):
    tokens, top_k = expert_ids.shape
    local_experts, model_dim = w_in.shape[0], w_in.shape[1]
    experts = local_experts * groups
    mean_load = tokens * top_k // experts
    send_cap = -(-(7 * mean_load // 4) // 16) * 16
    capacity = groups * mean_load
    rows_total = experts * send_cap
    ids_t, counts, rank_local = route_local(expert_ids, experts)
    inclusive = counts
    shift = 1
    while shift < groups:
        pairs_list = [(source, source + shift) for source in range(groups - shift)]
        inclusive = inclusive + lax.ppermute(inclusive, "expert", pairs_list)
        shift = shift * 2
    before = inclusive - counts
    totals = lax.psum(counts, "expert")
    prior = jnp.cumsum(totals, axis=0) - totals
    within = jnp.cumsum(counts, axis=0) - counts
    slot = jnp.take_along_axis(prior + before, ids_t, axis=1) + rank_local
    keep = slot < capacity
    target = ids_t * send_cap + jnp.take_along_axis(within, ids_t, axis=1) + rank_local
    token_ids = jnp.broadcast_to(jnp.arange(tokens, dtype=jnp.int32), (top_k, tokens))
    source_row = jnp.full((rows_total,), tokens, jnp.int32).at[jnp.where(keep, target, rows_total).reshape(-1)].set(token_ids.reshape(-1), mode="drop")
    padded = jnp.concatenate([token_rows, jnp.zeros((1, model_dim), token_rows.dtype)], axis=0)
    outbound = jnp.take(padded, source_row, axis=0).reshape(experts, send_cap, model_dim)
    inbound = lax.all_to_all(outbound, "expert", 0, 0, tiled=True).reshape(groups, local_experts, send_cap, model_dim)

    def one_expert(e, total):
        rows = lax.dynamic_index_in_dim(inbound, e, 1, keepdims=False).reshape(groups * send_cap, model_dim)
        hidden = jax.nn.gelu(jnp.dot(rows, w_in[e], preferred_element_type=jnp.float32)).astype(jnp.bfloat16)
        out = jnp.dot(hidden, w_out[e], preferred_element_type=jnp.float32).astype(jnp.bfloat16)
        return lax.dynamic_update_index_in_dim(total, out.reshape(groups, send_cap, model_dim), e, 1)

    expert_out = lax.fori_loop(0, local_experts, one_expert, jnp.zeros_like(inbound))
    returned = lax.all_to_all(expert_out.reshape(experts, send_cap, model_dim), "expert", 0, 0, tiled=True).reshape(rows_total, model_dim)
    picked = jnp.take(returned, target, axis=0)
    weight = jnp.where(keep, gate_weights.T, 0.0)
    mixed = jnp.sum(weight[:, :, None] * picked.astype(jnp.float32), axis=0)
    return (token_rows.astype(jnp.float32) + mixed).astype(jnp.bfloat16)


def block_rows(tokens, top_k, groups):
    mean = tokens * top_k // (groups * GROUPS)
    return (mean * 19 // 16 + 15) // 16 * 16


def total_rows(tokens, top_k, groups):
    return (tokens * top_k // groups * 9 // 8 + 15) // 16 * 16


def stages_of(tokens, top_k, groups, local_experts):
    mean = tokens * top_k // groups
    cuts = [0, mean * 13 // 32 // 16 * 16, mean * 20 // 32 // 16 * 16, total_rows(tokens, top_k, groups)]
    return [(cuts[i], cuts[i + 1], local_experts * (2 + i) // 4) for i in range(3)]


def dot_f32(a, b):
    return jnp.dot(a, b, preferred_element_type=jnp.float32)


def dot_nt(a, b):
    return lax.dot_general(a, b, (((1,), (1,)), ((), ())), preferred_element_type=jnp.float32)


def iota(shape, axis):
    return lax.broadcasted_iota(jnp.int32, shape, axis)


def as_bf16(mask):
    return jnp.where(mask, 1.0, 0.0).astype(jnp.bfloat16)


def pad_rows(rows, total):
    have = sum(r.shape[0] for r in rows)
    if have < total:
        rows = rows + [jnp.zeros((total - have, rows[0].shape[1]), rows[0].dtype)]
    return jnp.concatenate(rows, axis=0)


def select_row(rows, high_row):
    total = jnp.zeros_like(rows[0])
    for i, row in enumerate(rows):
        total = total + jnp.where(high_row == i, row, 0.0)
    return total


def split_lanes(row):
    return [row[:, i * LANES:(i + 1) * LANES] for i in range(row.shape[1] // LANES)]


def local_counts(experts, ids_ref, hot, count_ref):
    tokens = ids_ref.shape[1]
    blocks = tokens // LANES
    highs = experts // LANES

    def fill(b, carry):
        at = pl.ds(pl.multiple_of(b * LANES, LANES), LANES)
        for j in range(2):
            hot[j, :, at] = as_bf16(iota((LANES, LANES), 0) == ids_ref[j:j + 1, at] % LANES)
        return carry

    lax.fori_loop(0, blocks, fill, 0)
    n = highs * blocks
    row, col = iota((n, n), 0), iota((n, n), 1)
    below = as_bf16((row // blocks == col // blocks) & (row > col))
    in_block = iota((n, tokens), 0) % blocks == iota((n, tokens), 1) // LANES
    base, count = [], []
    for j in range(2):
        part = as_bf16(in_block & (iota((n, tokens), 0) // blocks == ids_ref[j:j + 1, :] // LANES))
        per_block = dot_nt(part, hot[j])
        base.append(dot_f32(below, per_block.astype(jnp.bfloat16)))
        count.append(jnp.concatenate([jnp.sum(per_block[i * blocks:(i + 1) * blocks], axis=0, keepdims=True) for i in range(highs)], axis=1))
    count_ref[...] = pad_rows(count, 8)
    return base, count


def place_pairs(groups, rows, out_rows, group_experts, base, count, ids_ref, hot, same, rank_ref, pos_ref, pack_ref):
    tokens = ids_ref.shape[1]
    experts = same.shape[0]
    blocks = tokens // LANES
    highs = experts // LANES
    local_experts = experts // groups
    both = pad_rows([count[0] + count[1]], 8)
    start = dot_f32(both.astype(jnp.bfloat16), same[...])[0:1]
    lane = iota((1, experts), 1)
    stride = -(-out_rows // LANES) * LANES
    first = (lane // local_experts * stride).astype(jnp.float32) + start
    earlier = iota((LANES, LANES), 0) < iota((LANES, LANES), 1)
    found = None
    table_rows = pack_ref.shape[0]
    n = highs * blocks
    for j in range(2):
        at = first if j == 0 else first + count[0]
        coarse = jnp.floor(at * (1.0 / 64.0))
        lhs = [base[j]] + split_lanes(coarse) + split_lanes(at - 64.0 * coarse)
        look = dot_f32(pad_rows(lhs, -(-(n + 2 * highs) // 16) * 16).astype(jnp.bfloat16), hot[j])
        for b in range(blocks):
            cols = slice(b * LANES, (b + 1) * LANES)
            row = ids_ref[j:j + 1, cols]
            high_row = row // LANES
            wide = jnp.broadcast_to(row.astype(jnp.float32), (LANES, LANES))
            same_id = (wide.T == wide) & earlier
            rank = jnp.sum(jnp.where(same_id, 1.0, 0.0), axis=0, keepdims=True)
            rank = rank + select_row([look[i * blocks + b:i * blocks + b + 1, cols] for i in range(highs)], high_row)
            offset = select_row([64.0 * look[n + i:n + i + 1, cols] + look[n + highs + i:n + highs + i + 1, cols] for i in range(highs)], high_row)
            rank_ref[j:j + 1, cols] = rank
            pos_ref[j:j + 1, cols] = rank + offset
        pos = pos_ref[j:j + 1, :]
        pos_ref[j:j + 1, :] = pos - (stride - out_rows) * jnp.floor((pos + 0.5) * (1.0 / stride))
        pos = pos.astype(jnp.int32)
        token = iota((LANES, tokens), 1)
        high_t = as_bf16(iota((table_rows, tokens), 0) == pos // LANES)
        low = iota((LANES, tokens), 0) == pos % LANES
        low_hi = jnp.where(low, (token // 8).astype(jnp.float32), 0.0).astype(jnp.bfloat16)
        low_lo = jnp.where(low, (token % 8).astype(jnp.float32), 0.0).astype(jnp.bfloat16)
        hit = 8.0 * dot_nt(high_t, low_hi) + dot_nt(high_t, low_lo)
        found = hit if found is None else found + hit
    pack_ref[...] = jnp.clip(found.astype(jnp.int32), 0, tokens - 1)


def group_tables(me, groups, rows, out_rows, back, group_experts, capacity, every, ids_ref, hot, same, rank_ref, pos_ref, lhs_ref, ret_ref, comb_ref, load_ref):
    experts = same.shape[0]
    tokens = hot.shape[2]
    local_experts = experts // groups
    blocks = tokens // LANES
    c = [[every[s, j:j + 1, :] for s in range(groups)] for j in range(2)]
    both = pad_rows([c[0][s] + c[1][s] for s in range(groups)], 8)
    start = dot_f32(both.astype(jnp.bfloat16), same[...])
    local = iota((8, experts), 1) % local_experts
    over = jnp.maximum(start + both - out_rows, jnp.where(local == group_experts, start - rows, -1.0))
    for _, high, done in back[:-1]:
        over = jnp.maximum(over, jnp.where(local == done, high - start, -1.0))
    load_ref[...] = jnp.broadcast_to(jnp.max(over), load_ref.shape)
    kept = [[None] * groups, [None] * groups]
    used = jnp.zeros((1, experts), jnp.float32)
    for j in range(2):
        for s in range(groups):
            kept[j][s] = jnp.clip(capacity - used, 0.0, c[j][s])
            used = used + c[j][s]
    lane = iota((1, experts), 1)
    local = lane % local_experts
    slot = jnp.zeros((1, experts), jnp.float32)
    slots, steps, edges, jumps = [], [], [], []
    last = jnp.zeros((1, experts), jnp.float32)
    for s in range(groups):
        ret_v = []
        for j in range(2):
            edge = start[s:s + 1] if j == 0 else start[s:s + 1] + c[0][s]
            v = s * out_rows + edge - slot
            slots.append(slot)
            steps.append(v - last)
            last = v
            edges.append(edge)
            ret_v.append((local * capacity).astype(jnp.float32) + slot - edge)
            slot = slot + kept[j][s]
        before = jnp.concatenate([jnp.zeros((1, 1), jnp.float32), ret_v[1][:, :-1]], axis=1)
        jumps.append(ret_v[0] - jnp.where(local == 0, 0.0, before))
        jumps.append(ret_v[1] - ret_v[0])

    def mine(parts):
        a = jnp.concatenate(parts, axis=0)
        total = jnp.zeros((a.shape[0], local_experts), jnp.float32)
        for d in range(groups):
            total = total + jnp.where(me == d, a[:, d * local_experts:(d + 1) * local_experts], 0.0)
        return total

    slots, steps, edges, jumps = mine(slots), mine(steps), mine(edges), mine(jumps)
    tall = pad_rows([edges, jumps, slots, steps], LANES)
    tall = jnp.concatenate([tall, jnp.zeros((LANES, LANES - local_experts), jnp.float32)], axis=1).T if local_experts < LANES else tall.T
    q = iota((local_experts, LANES), 1).astype(jnp.float32)
    lhs = q
    for i in range(2 * groups):
        at = 4 * groups + i
        lhs = lhs + jnp.where(q >= tall[:local_experts, at:at + 1], tall[:local_experts, at + 2 * groups:at + 2 * groups + 1], 0.0)
    lhs_ref[...] = jnp.clip(lhs.astype(jnp.int32), 0, groups * out_rows - 1)

    width = -(-out_rows // LANES) * LANES
    p = iota((1, width), 1).astype(jnp.float32)
    part = tall[:local_experts]
    for s in range(groups):
        total = jnp.zeros((local_experts, width), jnp.float32)
        for j in range(2):
            i = 2 * s + j
            total = total + jnp.where(p >= part[:, i:i + 1], part[:, 2 * groups + i:2 * groups + i + 1], 0.0)
        row = p + jnp.sum(total, axis=0, keepdims=True)
        row = jnp.clip(row.astype(jnp.int32), 0, local_experts * capacity - 1)
        for i in range(width // LANES):
            at = s * (width // LANES) + i
            ret_ref[at:at + 1, :] = row[:, i * LANES:(i + 1) * LANES]

    for j in range(2):
        own = jnp.zeros((1, experts), jnp.float32)
        for s in range(groups):
            own = own + jnp.where(me == s, kept[j][s], 0.0)
        bound = dot_f32(pad_rows(split_lanes(own), 16).astype(jnp.bfloat16), hot[j])
        bound = select_row([bound[i:i + 1] for i in range(experts // LANES)], ids_ref[j:j + 1, :] // LANES)
        none = float(groups * out_rows)
        for b in range(blocks):
            cols = slice(b * LANES, (b + 1) * LANES)
            take = jnp.where(rank_ref[j:j + 1, cols] < bound[:, cols], pos_ref[j:j + 1, cols], none)
            comb_ref[j * blocks + b:j * blocks + b + 1, :] = jnp.clip(take.astype(jnp.int32), 0, groups * out_rows)


def exchange_kernel(
    groups, rows, out_rows, back, capacity,
    gates_ref, ids_ref, x_hbm, win_ref, wout_ref, out_hbm, load_ref,
    hot, same, count, every, rank_ref, pos_ref, pack_v, lhs_v, ret_v, comb_v, pack_idx, lhs_idx, ret_idx, comb_idx, wide_gates, x_ref,
    xr_rows, send, recv, rf_rows, stage0, stage1, of_rows, rsend, rrecv, retf_rows, wi, wo,
    wsem, ssem, rsem, rssem, rrsem, csend, crecv, tsem, osem,
):
    tokens, model_dim = x_hbm.shape
    sub = model_dim // LANES
    local_experts = win_ref.shape[0]
    group_experts = local_experts // GROUPS
    me = lax.axis_index("expert")
    span = rows * sub
    stages = (stage0, stage1)
    xr, rf, of, retf = (r.reshape(r.shape[0] * sub, LANES) for r in (xr_rows, rf_rows, of_rows, retf_rows))

    def fetch(e, slot):
        a = pltpu.make_async_copy(win_ref.at[e], wi.at[slot], wsem.at[slot, 0])
        b = pltpu.make_async_copy(wout_ref.at[e], wo.at[slot], wsem.at[slot, 1])
        return a, b

    x_copy = pltpu.make_async_copy(x_hbm, x_ref, tsem.at[4])
    x_copy.start()
    for e in range(BUFS):
        for c in fetch(e, e):
            c.start()
    barrier = pltpu.get_barrier_semaphore()
    for k in range(1, groups):
        pl.semaphore_signal(barrier, inc=1, device_id={"expert": lax.rem(me + k, groups)}, device_id_type=MESH)
    retf[pl.ds(groups * out_rows * sub, 8 * sub), :] = jnp.zeros((8 * sub, LANES), jnp.float32)
    experts = same.shape[0]
    i_e, i_f = iota((experts, experts), 0), iota((experts, experts), 1)
    same[...] = as_bf16((i_e // local_experts == i_f // local_experts) & (i_e < i_f))
    base, counts = local_counts(experts, ids_ref, hot, count)
    x_copy.wait()
    for k in range(sub):
        xr[pl.ds(k, tokens, stride=sub), :] = x_ref[:, k * LANES:(k + 1) * LANES].astype(jnp.float32)
    place_pairs(groups, rows, out_rows, group_experts, base, counts, ids_ref, hot, same, rank_ref, pos_ref, pack_v)
    pack_copy = pltpu.make_async_copy(pack_v, pack_idx, tsem.at[0])
    pack_copy.start()
    pl.semaphore_wait(barrier, groups - 1)

    def count_copy(k):
        return pltpu.make_async_remote_copy(
            src_ref=count, dst_ref=every.at[me], send_sem=csend.at[k], recv_sem=crecv.at[k],
            device_id={"expert": lax.rem(me + k, groups)}, device_id_type=MESH)

    for k in range(1, groups):
        count_copy(k).start()
    pack_copy.wait()

    def gather_rows(idx, line, low, high, table, dst):
        def some(at, col, first, size):
            for c in range(size // 16):
                got = [table[idx[at, col + c * 16 + r]] for r in range(16)]
                dst[pl.ds(pl.multiple_of((first + c * 16) * sub, 16 * sub), 16 * sub), :] = jnp.concatenate(got, axis=0).astype(jnp.bfloat16)

        head = min(-low % LANES, high - low)
        if head:
            some(line + low // LANES, low % LANES, 0, head)
        lines, rest = divmod(high - low - head, LANES)
        first = (low + head) // LANES

        def body(i, carry):
            some(line + first + i, 0, head + i * LANES, LANES)
            return carry

        lax.fori_loop(0, lines, body, 0)
        if rest:
            some(line + first + lines, 0, head + lines * LANES, rest)

    def widen(src, dst, first):
        def body(c, carry):
            part = pl.multiple_of(c * 16 * sub, 16 * sub)
            dst[pl.ds(pl.multiple_of(first + part, 16), 16 * sub), :] = src[pl.ds(part, 16 * sub), :].astype(jnp.float32)
            return carry
        lax.fori_loop(0, src.shape[0] // (16 * sub), body, 0)

    def out_part(ref, g, peer):
        low, high = ((0, rows), (rows, out_rows))[g]
        return ref.at[peer, pl.ds(low * sub, (high - low) * sub)]

    def back_part(ref, g, peer):
        low, high, _ = back[g]
        return ref.at[peer, pl.ds(low * sub, (high - low) * sub)]

    def copy_to(part, src, dst, g, k, s_sem, r_sem):
        peer = lax.rem(me + k, groups)
        return pltpu.make_async_remote_copy(
            src_ref=part(src, g, peer), dst_ref=part(dst, g, me), send_sem=s_sem.at[g, k], recv_sem=r_sem.at[g, k],
            device_id={"expert": peer}, device_id_type=MESH)

    def send_blocks(g, part, gather, src, dst, s_sem, r_sem):
        def body(i, carry):
            peer = lax.rem(me + i + 1, groups)
            gather(peer, part(src, g, peer))

            @pl.when(i >= 1)
            def _():
                copy_to(part, src, dst, g, i, s_sem, r_sem).start()

            return carry

        lax.fori_loop(0, groups, body, 0)

    def take_blocks(g, part, src, dst, own, first, s_sem, r_sem):
        widen(part(own, g, me), dst, first(me))

        def body(k, carry):
            peer = lax.rem(me - k + groups, groups)
            pltpu.make_async_remote_copy(
                src_ref=part(own, g, peer), dst_ref=part(src, g, peer), send_sem=s_sem.at[g, k], recv_sem=r_sem.at[g, k],
                device_id={"expert": peer}, device_id_type=MESH).wait_recv()
            widen(part(src, g, peer), dst, first(peer))
            return carry

        lax.fori_loop(1, groups, body, 0)

    out_lines = -(-out_rows // LANES)
    for g in range(GROUPS):
        low, high = ((0, rows), (rows, out_rows))[g]
        send_blocks(g, out_part, lambda peer, dst: gather_rows(pack_idx, peer * out_lines, low, high, xr_rows, dst), send, recv, ssem, rsem)

    every[me] = count[...]
    for j in range(2):
        for b in range(tokens // LANES):
            part = slice(b * LANES, (b + 1) * LANES)
            wide_gates[j, part, :] = jnp.broadcast_to(gates_ref[j:j + 1, part], (LANES, LANES)).T
    for k in range(1, groups):
        source = lax.rem(me - k + groups, groups)
        pltpu.make_async_remote_copy(
            src_ref=count, dst_ref=every.at[source], send_sem=csend.at[k], recv_sem=crecv.at[k],
            device_id={"expert": source}, device_id_type=MESH).wait_recv()
    group_tables(me, groups, rows, out_rows, back, group_experts, capacity, every, ids_ref, hot, same, rank_ref, pos_ref, lhs_v, ret_v, comb_v, load_ref)
    tables = [pltpu.make_async_copy(a, b, tsem.at[i + 1]) for i, (a, b) in enumerate(((lhs_v, lhs_idx), (ret_v, ret_idx), (comb_v, comb_idx)))]
    for t in tables:
        t.start()
    for t in tables:
        t.wait()

    def gather_lhs(e, stage):
        for q in range(capacity):
            stage[pl.ds(q * sub, sub), :] = rf_rows[lhs_idx[e, q]]

    def ffn(e, stage):
        slot = lax.rem(e, BUFS)
        for c in fetch(e, slot):
            c.wait()
        lhs = jnp.concatenate([stage[pl.ds(k, capacity, stride=sub), :] for k in range(sub)], axis=1).astype(jnp.bfloat16)
        hidden = jax.nn.gelu(dot_f32(lhs, wi[slot])).astype(jnp.bfloat16)
        out = dot_f32(hidden, wo[slot]).astype(jnp.bfloat16).astype(jnp.float32)
        at = e * capacity * sub
        for k in range(sub):
            of[pl.ds(at + k, capacity, stride=sub), :] = out[:, k * LANES:(k + 1) * LANES]

    first_expert = 0
    for b, (low, high, done) in enumerate(back):
        if b < GROUPS:
            take_blocks(b, out_part, recv, rf, send, lambda peer: (peer * out_rows + b * rows) * sub, ssem, rsem)

        def body(i, carry):
            for half in range(2):
                e = first_expert + i * 2 + half
                gather_lhs(e, stages[half])
                ffn(e, stages[half])

                @pl.when(e + BUFS < local_experts)
                def _():
                    for c in fetch(e + BUFS, lax.rem(e, BUFS)):
                        c.start()
            return carry

        lax.fori_loop(0, (done - first_expert) // 2, body, 0)
        first_expert = done
        send_blocks(b, back_part, lambda peer, dst: gather_rows(ret_idx, peer * out_lines, low, high, of_rows, dst), rsend, rrecv, rssem, rrsem)

    for b, (low, high, done) in enumerate(back):
        take_blocks(b, back_part, rrecv, retf, rsend, lambda peer: (peer * out_rows + low) * sub, rssem, rrsem)

    half = tokens // LANES

    def combine(line, carry):
        for c in range(LANES // 16):
            got = []
            for r in range(16):
                col = c * 16 + r
                row = xr_rows[line * LANES + col]
                for j in range(2):
                    row = row + wide_gates[j, pl.ds(pl.multiple_of(line * LANES, LANES) + col, 1), :] * retf_rows[comb_idx[j * half + line, col]]
                got.append(row)
            xr[pl.ds(pl.multiple_of((line * LANES + c * 16) * sub, 16 * sub), 16 * sub), :] = jnp.concatenate(got, axis=0)
        part = pl.ds(pl.multiple_of(line * LANES, LANES), LANES)
        for k in range(sub):
            x_ref[part, k * LANES:(k + 1) * LANES] = xr[pl.ds(line * LANES * sub + k, LANES, stride=sub), :].astype(jnp.bfloat16)

        @pl.when(line >= 1)
        def _():
            put(line - 1).start()

        return carry

    def put(line):
        part = pl.ds(pl.multiple_of(line * LANES, LANES), LANES)
        return pltpu.make_async_copy(x_ref.at[part], out_hbm.at[part], osem.at[line])

    lax.fori_loop(0, half, combine, 0)
    put(half - 1).start()
    for line in range(half):
        put(line).wait()
    for g in range(GROUPS):
        for k in range(1, groups):
            if g == 0:
                count_copy(k).wait_send()
            copy_to(out_part, send, recv, g, k, ssem, rsem).wait_send()
    for b in range(len(back)):
        for k in range(1, groups):
            copy_to(back_part, rsend, rrecv, b, k, rssem, rrsem).wait_send()


def compact_step(groups, rows, out_rows, capacity, gates, ids, token_rows, w_in, w_out):
    tokens, model_dim = token_rows.shape
    local_experts, _, hidden_dim = w_in.shape
    experts = local_experts * groups
    group_experts = local_experts // GROUPS
    sub = model_dim // LANES
    span = rows * sub
    vmem = pl.BlockSpec(memory_space=pltpu.VMEM)
    hbm = pl.BlockSpec(memory_space=pl.ANY)
    wire = pltpu.VMEM((groups, out_rows * sub, LANES), jnp.bfloat16)
    back = stages_of(tokens, 2, groups, local_experts)
    back_sems = pltpu.SemaphoreType.DMA((len(back), groups))
    sems = pltpu.SemaphoreType.DMA((GROUPS, groups))
    table_rows = (
        groups * -(-out_rows // LANES),
        local_experts,
        groups * -(-out_rows // LANES),
        2 * tokens // LANES,
    )
    return pl.pallas_call(
        functools.partial(exchange_kernel, groups, rows, out_rows, back, capacity),
        out_shape=(jax.ShapeDtypeStruct((tokens, model_dim), jnp.bfloat16), jax.ShapeDtypeStruct((1, 1), jnp.float32)),
        in_specs=[vmem, vmem, hbm, hbm, hbm],
        out_specs=(hbm, vmem),
        scratch_shapes=[
            pltpu.VMEM((2, LANES, tokens), jnp.bfloat16),
            pltpu.VMEM((experts, experts), jnp.bfloat16),
            pltpu.VMEM((8, experts), jnp.float32),
            pltpu.VMEM((groups, 8, experts), jnp.float32),
            pltpu.VMEM((8, tokens), jnp.float32),
            pltpu.VMEM((8, tokens), jnp.float32),
            *[pltpu.VMEM((r, LANES), jnp.int32) for r in table_rows],
            *[pltpu.SMEM((r, LANES), jnp.int32) for r in table_rows],
            pltpu.VMEM((2, tokens, LANES), jnp.float32),
            pltpu.VMEM((tokens, model_dim), jnp.bfloat16),
            pltpu.VMEM((tokens, sub, LANES), jnp.float32),
            wire,
            wire,
            pltpu.VMEM((groups * out_rows, sub, LANES), jnp.float32),
            pltpu.VMEM((capacity * sub, LANES), jnp.float32),
            pltpu.VMEM((capacity * sub, LANES), jnp.float32),
            pltpu.VMEM((local_experts * capacity, sub, LANES), jnp.float32),
            wire,
            wire,
            pltpu.VMEM((groups * out_rows + 8, sub, LANES), jnp.float32),
            pltpu.VMEM((BUFS, model_dim, hidden_dim), jnp.bfloat16),
            pltpu.VMEM((BUFS, hidden_dim, model_dim), jnp.bfloat16),
            pltpu.SemaphoreType.DMA((BUFS, 2)),
            sems, sems, back_sems, back_sems,
            pltpu.SemaphoreType.DMA((groups,)),
            pltpu.SemaphoreType.DMA((groups,)),
            pltpu.SemaphoreType.DMA((5,)),
            pltpu.SemaphoreType.DMA((tokens // LANES,)),
        ],
        compiler_params=pltpu.CompilerParams(collective_id=0, has_side_effects=True, vmem_limit_bytes=67043328),
        name="expert_exchange",
    )(gates, ids, token_rows, w_in, w_out)


def hand_over(rows):
    parts = 8
    size = rows.shape[0] // parts

    def kernel(a_ref, o_ref, buf, sem_in, sem_out):
        part = [pl.ds(i * size, size) for i in range(parts)]
        take = [pltpu.make_async_copy(a_ref.at[p], buf.at[p], sem_in.at[i]) for i, p in enumerate(part)]
        give = [pltpu.make_async_copy(buf.at[p], o_ref.at[p], sem_out.at[i]) for i, p in enumerate(part)]
        for t in take:
            t.start()
        for t, g in zip(take, give):
            t.wait()
            g.start()
        for g in give:
            g.wait()

    return pl.pallas_call(
        kernel,
        in_specs=[pl.BlockSpec(memory_space=pl.ANY)],
        out_specs=pl.BlockSpec(memory_space=pl.ANY),
        out_shape=jax.ShapeDtypeStruct(rows.shape, rows.dtype),
        scratch_shapes=[pltpu.VMEM(rows.shape, rows.dtype), pltpu.SemaphoreType.DMA((parts,)), pltpu.SemaphoreType.DMA((parts,))],
        name="hand_over",
    )(rows)


def solution(mesh):
    groups = mesh.shape["expert"]
    row_spec = P(("data", "expert"), None)
    weight_spec = P("expert", None, None)

    def device_step(token_rows, expert_ids, gate_weights, w_in, w_out):
        tokens, top_k = expert_ids.shape
        local_experts = w_in.shape[0]
        capacity = tokens * top_k // local_experts
        rows = block_rows(tokens, top_k, groups)
        fast, load = compact_step(groups, rows, total_rows(tokens, top_k, groups), capacity, gate_weights.T, expert_ids.T, token_rows, w_in, w_out)
        fast = hand_over(fast)
        overflow = load[0, 0] > 0.0
        general = lambda state: (jnp.array(False), padded_step(groups, token_rows, expert_ids, gate_weights, w_in, w_out))
        return lax.while_loop(lambda state: state[0], general, (overflow, fast))[1]

    return jax.shard_map(device_step, mesh=mesh, in_specs=(row_spec, row_spec, row_spec, weight_spec, weight_spec), out_specs=row_spec, check_vma=False)
```

```python
import functools

import jax
import jax.numpy as jnp
from jax import lax
from jax.experimental import pallas as pl
from jax.experimental.pallas import tpu as pltpu
from jax.sharding import PartitionSpec as P

GROUPS = 2
BUFS = 4
LANES = 128
MESH = pl.DeviceIdType.MESH


def route_local(expert_ids, experts):
    ids_t = expert_ids.T
    onehot = (ids_t[:, :, None] == jnp.arange(experts, dtype=jnp.int32)).astype(jnp.int32)
    running = jnp.cumsum(onehot, axis=1)
    counts = running[:, -1, :]
    rank_local = jnp.sum(onehot * running, axis=2) - 1
    return ids_t, counts, rank_local


def padded_step(groups, token_rows, expert_ids, gate_weights, w_in, w_out):
    tokens, top_k = expert_ids.shape
    local_experts, model_dim = w_in.shape[0], w_in.shape[1]
    experts = local_experts * groups
    mean_load = tokens * top_k // experts
    send_cap = -(-(7 * mean_load // 4) // 16) * 16
    capacity = groups * mean_load
    rows_total = experts * send_cap
    ids_t, counts, rank_local = route_local(expert_ids, experts)
    inclusive = counts
    shift = 1
    while shift < groups:
        pairs_list = [(source, source + shift) for source in range(groups - shift)]
        inclusive = inclusive + lax.ppermute(inclusive, "expert", pairs_list)
        shift = shift * 2
    before = inclusive - counts
    totals = lax.psum(counts, "expert")
    prior = jnp.cumsum(totals, axis=0) - totals
    within = jnp.cumsum(counts, axis=0) - counts
    slot = jnp.take_along_axis(prior + before, ids_t, axis=1) + rank_local
    keep = slot < capacity
    target = ids_t * send_cap + jnp.take_along_axis(within, ids_t, axis=1) + rank_local
    token_ids = jnp.broadcast_to(jnp.arange(tokens, dtype=jnp.int32), (top_k, tokens))
    source_row = jnp.full((rows_total,), tokens, jnp.int32).at[jnp.where(keep, target, rows_total).reshape(-1)].set(token_ids.reshape(-1), mode="drop")
    padded = jnp.concatenate([token_rows, jnp.zeros((1, model_dim), token_rows.dtype)], axis=0)
    outbound = jnp.take(padded, source_row, axis=0).reshape(experts, send_cap, model_dim)
    inbound = lax.all_to_all(outbound, "expert", 0, 0, tiled=True).reshape(groups, local_experts, send_cap, model_dim)

    def one_expert(e, total):
        rows = lax.dynamic_index_in_dim(inbound, e, 1, keepdims=False).reshape(groups * send_cap, model_dim)
        hidden = jax.nn.gelu(jnp.dot(rows, w_in[e], preferred_element_type=jnp.float32)).astype(jnp.bfloat16)
        out = jnp.dot(hidden, w_out[e], preferred_element_type=jnp.float32).astype(jnp.bfloat16)
        return lax.dynamic_update_index_in_dim(total, out.reshape(groups, send_cap, model_dim), e, 1)

    expert_out = lax.fori_loop(0, local_experts, one_expert, jnp.zeros_like(inbound))
    returned = lax.all_to_all(expert_out.reshape(experts, send_cap, model_dim), "expert", 0, 0, tiled=True).reshape(rows_total, model_dim)
    picked = jnp.take(returned, target, axis=0)
    weight = jnp.where(keep, gate_weights.T, 0.0)
    mixed = jnp.sum(weight[:, :, None] * picked.astype(jnp.float32), axis=0)
    return (token_rows.astype(jnp.float32) + mixed).astype(jnp.bfloat16)


def block_rows(tokens, top_k, groups):
    mean = tokens * top_k // (groups * GROUPS)
    return (mean * 19 // 16 + 15) // 16 * 16


def total_rows(tokens, top_k, groups):
    return (tokens * top_k // groups * 9 // 8 + 15) // 16 * 16


def stages_of(tokens, top_k, groups, local_experts):
    mean = tokens * top_k // groups
    cuts = [0, mean * 13 // 32 // 16 * 16, mean * 20 // 32 // 16 * 16, total_rows(tokens, top_k, groups)]
    return [(cuts[i], cuts[i + 1], local_experts * (2 + i) // 4) for i in range(3)]


def dot_f32(a, b):
    return jnp.dot(a, b, preferred_element_type=jnp.float32)


def dot_nt(a, b):
    return lax.dot_general(a, b, (((1,), (1,)), ((), ())), preferred_element_type=jnp.float32)


def iota(shape, axis):
    return lax.broadcasted_iota(jnp.int32, shape, axis)


def as_bf16(mask):
    return jnp.where(mask, 1.0, 0.0).astype(jnp.bfloat16)


def pad_rows(rows, total):
    have = sum(r.shape[0] for r in rows)
    if have < total:
        rows = rows + [jnp.zeros((total - have, rows[0].shape[1]), rows[0].dtype)]
    return jnp.concatenate(rows, axis=0)


def select_row(rows, high_row):
    total = jnp.zeros_like(rows[0])
    for i, row in enumerate(rows):
        total = total + jnp.where(high_row == i, row, 0.0)
    return total


def split_lanes(row):
    return [row[:, i * LANES:(i + 1) * LANES] for i in range(row.shape[1] // LANES)]


def local_counts(experts, ids_ref, hot, count_ref):
    tokens = ids_ref.shape[1]
    blocks = tokens // LANES
    highs = experts // LANES

    def fill(b, carry):
        at = pl.ds(pl.multiple_of(b * LANES, LANES), LANES)
        for j in range(2):
            hot[j, :, at] = as_bf16(iota((LANES, LANES), 0) == ids_ref[j:j + 1, at] % LANES)
        return carry

    lax.fori_loop(0, blocks, fill, 0)
    n = highs * blocks
    row, col = iota((n, n), 0), iota((n, n), 1)
    below = as_bf16((row // blocks == col // blocks) & (row > col))
    in_block = iota((n, tokens), 0) % blocks == iota((n, tokens), 1) // LANES
    base, count = [], []
    for j in range(2):
        part = as_bf16(in_block & (iota((n, tokens), 0) // blocks == ids_ref[j:j + 1, :] // LANES))
        per_block = dot_nt(part, hot[j])
        base.append(dot_f32(below, per_block.astype(jnp.bfloat16)))
        count.append(jnp.concatenate([jnp.sum(per_block[i * blocks:(i + 1) * blocks], axis=0, keepdims=True) for i in range(highs)], axis=1))
    count_ref[...] = pad_rows(count, 8)
    return base, count


def place_pairs(groups, rows, out_rows, group_experts, base, count, ids_ref, hot, same, rank_ref, pos_ref, pack_ref):
    tokens = ids_ref.shape[1]
    experts = same.shape[0]
    blocks = tokens // LANES
    highs = experts // LANES
    local_experts = experts // groups
    both = pad_rows([count[0] + count[1]], 8)
    start = dot_f32(both.astype(jnp.bfloat16), same[...])[0:1]
    lane = iota((1, experts), 1)
    stride = -(-out_rows // LANES) * LANES
    first = (lane // local_experts * stride).astype(jnp.float32) + start
    earlier = iota((LANES, LANES), 0) < iota((LANES, LANES), 1)
    found = None
    table_rows = pack_ref.shape[0]
    n = highs * blocks
    for j in range(2):
        at = first if j == 0 else first + count[0]
        coarse = jnp.floor(at * (1.0 / 64.0))
        lhs = [base[j]] + split_lanes(coarse) + split_lanes(at - 64.0 * coarse)
        look = dot_f32(pad_rows(lhs, -(-(n + 2 * highs) // 16) * 16).astype(jnp.bfloat16), hot[j])
        for b in range(blocks):
            cols = slice(b * LANES, (b + 1) * LANES)
            row = ids_ref[j:j + 1, cols]
            high_row = row // LANES
            wide = jnp.broadcast_to(row.astype(jnp.float32), (LANES, LANES))
            same_id = (wide.T == wide) & earlier
            rank = jnp.sum(jnp.where(same_id, 1.0, 0.0), axis=0, keepdims=True)
            rank = rank + select_row([look[i * blocks + b:i * blocks + b + 1, cols] for i in range(highs)], high_row)
            offset = select_row([64.0 * look[n + i:n + i + 1, cols] + look[n + highs + i:n + highs + i + 1, cols] for i in range(highs)], high_row)
            rank_ref[j:j + 1, cols] = rank
            pos_ref[j:j + 1, cols] = rank + offset
        pos = pos_ref[j:j + 1, :]
        pos_ref[j:j + 1, :] = pos - (stride - out_rows) * jnp.floor((pos + 0.5) * (1.0 / stride))
        pos = pos.astype(jnp.int32)
        token = iota((LANES, tokens), 1)
        high_t = as_bf16(iota((table_rows, tokens), 0) == pos // LANES)
        low = iota((LANES, tokens), 0) == pos % LANES
        low_hi = jnp.where(low, (token // 8).astype(jnp.float32), 0.0).astype(jnp.bfloat16)
        low_lo = jnp.where(low, (token % 8).astype(jnp.float32), 0.0).astype(jnp.bfloat16)
        hit = 8.0 * dot_nt(high_t, low_hi) + dot_nt(high_t, low_lo)
        found = hit if found is None else found + hit
    pack_ref[...] = jnp.clip(found.astype(jnp.int32), 0, tokens - 1)


def group_tables(me, groups, rows, out_rows, back, group_experts, capacity, every, ids_ref, hot, same, rank_ref, pos_ref, lhs_ref, ret_ref, comb_ref, load_ref):
    experts = same.shape[0]
    tokens = hot.shape[2]
    local_experts = experts // groups
    blocks = tokens // LANES
    c = [[every[s, j:j + 1, :] for s in range(groups)] for j in range(2)]
    both = pad_rows([c[0][s] + c[1][s] for s in range(groups)], 8)
    start = dot_f32(both.astype(jnp.bfloat16), same[...])
    local = iota((8, experts), 1) % local_experts
    over = jnp.maximum(start + both - out_rows, jnp.where(local == group_experts, start - rows, -1.0))
    for _, high, done in back[:-1]:
        over = jnp.maximum(over, jnp.where(local == done, high - start, -1.0))
    load_ref[...] = jnp.broadcast_to(jnp.max(over), load_ref.shape)
    kept = [[None] * groups, [None] * groups]
    used = jnp.zeros((1, experts), jnp.float32)
    for j in range(2):
        for s in range(groups):
            kept[j][s] = jnp.clip(capacity - used, 0.0, c[j][s])
            used = used + c[j][s]
    lane = iota((1, experts), 1)
    local = lane % local_experts
    slot = jnp.zeros((1, experts), jnp.float32)
    slots, steps, edges, jumps = [], [], [], []
    last = jnp.zeros((1, experts), jnp.float32)
    for s in range(groups):
        ret_v = []
        for j in range(2):
            edge = start[s:s + 1] if j == 0 else start[s:s + 1] + c[0][s]
            v = s * out_rows + edge - slot
            slots.append(slot)
            steps.append(v - last)
            last = v
            edges.append(edge)
            ret_v.append((local * capacity).astype(jnp.float32) + slot - edge)
            slot = slot + kept[j][s]
        before = jnp.concatenate([jnp.zeros((1, 1), jnp.float32), ret_v[1][:, :-1]], axis=1)
        jumps.append(ret_v[0] - jnp.where(local == 0, 0.0, before))
        jumps.append(ret_v[1] - ret_v[0])

    def mine(parts):
        a = jnp.concatenate(parts, axis=0)
        total = jnp.zeros((a.shape[0], local_experts), jnp.float32)
        for d in range(groups):
            total = total + jnp.where(me == d, a[:, d * local_experts:(d + 1) * local_experts], 0.0)
        return total

    slots, steps, edges, jumps = mine(slots), mine(steps), mine(edges), mine(jumps)
    tall = pad_rows([edges, jumps, slots, steps], LANES)
    tall = jnp.concatenate([tall, jnp.zeros((LANES, LANES - local_experts), jnp.float32)], axis=1).T if local_experts < LANES else tall.T
    q = iota((local_experts, LANES), 1).astype(jnp.float32)
    lhs = q
    for i in range(2 * groups):
        at = 4 * groups + i
        lhs = lhs + jnp.where(q >= tall[:local_experts, at:at + 1], tall[:local_experts, at + 2 * groups:at + 2 * groups + 1], 0.0)
    lhs_ref[...] = jnp.clip(lhs.astype(jnp.int32), 0, groups * out_rows - 1)

    width = -(-out_rows // LANES) * LANES
    p = iota((1, width), 1).astype(jnp.float32)
    part = tall[:local_experts]
    for s in range(groups):
        total = jnp.zeros((local_experts, width), jnp.float32)
        for j in range(2):
            i = 2 * s + j
            total = total + jnp.where(p >= part[:, i:i + 1], part[:, 2 * groups + i:2 * groups + i + 1], 0.0)
        row = p + jnp.sum(total, axis=0, keepdims=True)
        row = jnp.clip(row.astype(jnp.int32), 0, local_experts * capacity - 1)
        for i in range(width // LANES):
            at = s * (width // LANES) + i
            ret_ref[at:at + 1, :] = row[:, i * LANES:(i + 1) * LANES]

    for j in range(2):
        own = jnp.zeros((1, experts), jnp.float32)
        for s in range(groups):
            own = own + jnp.where(me == s, kept[j][s], 0.0)
        bound = dot_f32(pad_rows(split_lanes(own), 16).astype(jnp.bfloat16), hot[j])
        bound = select_row([bound[i:i + 1] for i in range(experts // LANES)], ids_ref[j:j + 1, :] // LANES)
        none = float(groups * out_rows)
        for b in range(blocks):
            cols = slice(b * LANES, (b + 1) * LANES)
            take = jnp.where(rank_ref[j:j + 1, cols] < bound[:, cols], pos_ref[j:j + 1, cols], none)
            comb_ref[j * blocks + b:j * blocks + b + 1, :] = jnp.clip(take.astype(jnp.int32), 0, groups * out_rows)


def exchange_kernel(
    groups, rows, out_rows, back, capacity,
    gates_ref, ids_ref, x_hbm, win_ref, wout_ref, out_hbm, load_ref,
    hot, same, count, every, rank_ref, pos_ref, pack_v, lhs_v, ret_v, comb_v, pack_idx, lhs_idx, ret_idx, comb_idx, wide_gates, x_ref,
    xr_rows, send, recv, rf_rows, stage0, stage1, of_rows, rsend, rrecv, retf_rows, wi, wo,
    wsem, ssem, rsem, rssem, rrsem, csend, crecv, tsem, osem,
):
    tokens, model_dim = x_hbm.shape
    sub = model_dim // LANES
    local_experts = win_ref.shape[0]
    group_experts = local_experts // GROUPS
    me = lax.axis_index("expert")
    span = rows * sub
    stages = (stage0, stage1)
    xr, rf, of, retf = (r.reshape(r.shape[0] * sub, LANES) for r in (xr_rows, rf_rows, of_rows, retf_rows))

    def fetch(e, slot):
        a = pltpu.make_async_copy(win_ref.at[e], wi.at[slot], wsem.at[slot, 0])
        b = pltpu.make_async_copy(wout_ref.at[e], wo.at[slot], wsem.at[slot, 1])
        return a, b

    x_copy = pltpu.make_async_copy(x_hbm, x_ref, tsem.at[4])
    x_copy.start()
    for e in range(BUFS):
        for c in fetch(e, e):
            c.start()
    barrier = pltpu.get_barrier_semaphore()
    for k in range(1, groups):
        pl.semaphore_signal(barrier, inc=1, device_id={"expert": lax.rem(me + k, groups)}, device_id_type=MESH)
    retf[pl.ds(groups * out_rows * sub, 8 * sub), :] = jnp.zeros((8 * sub, LANES), jnp.float32)
    experts = same.shape[0]
    i_e, i_f = iota((experts, experts), 0), iota((experts, experts), 1)
    same[...] = as_bf16((i_e // local_experts == i_f // local_experts) & (i_e < i_f))
    base, counts = local_counts(experts, ids_ref, hot, count)
    x_copy.wait()
    for k in range(sub):
        xr[pl.ds(k, tokens, stride=sub), :] = x_ref[:, k * LANES:(k + 1) * LANES].astype(jnp.float32)
    place_pairs(groups, rows, out_rows, group_experts, base, counts, ids_ref, hot, same, rank_ref, pos_ref, pack_v)
    pack_copy = pltpu.make_async_copy(pack_v, pack_idx, tsem.at[0])
    pack_copy.start()
    pl.semaphore_wait(barrier, groups - 1)

    def count_copy(k):
        return pltpu.make_async_remote_copy(
            src_ref=count, dst_ref=every.at[me], send_sem=csend.at[k], recv_sem=crecv.at[k],
            device_id={"expert": lax.rem(me + k, groups)}, device_id_type=MESH)

    for k in range(1, groups):
        count_copy(k).start()
    pack_copy.wait()

    def gather_rows(idx, line, low, high, table, dst):
        def some(at, col, first, size):
            for c in range(size // 16):
                got = [table[idx[at, col + c * 16 + r]] for r in range(16)]
                dst[pl.ds(pl.multiple_of((first + c * 16) * sub, 16 * sub), 16 * sub), :] = jnp.concatenate(got, axis=0).astype(jnp.bfloat16)

        head = min(-low % LANES, high - low)
        if head:
            some(line + low // LANES, low % LANES, 0, head)
        lines, rest = divmod(high - low - head, LANES)
        first = (low + head) // LANES

        def body(i, carry):
            some(line + first + i, 0, head + i * LANES, LANES)
            return carry

        lax.fori_loop(0, lines, body, 0)
        if rest:
            some(line + first + lines, 0, head + lines * LANES, rest)

    def widen(src, dst, first):
        def body(c, carry):
            part = pl.multiple_of(c * 16 * sub, 16 * sub)
            dst[pl.ds(pl.multiple_of(first + part, 16), 16 * sub), :] = src[pl.ds(part, 16 * sub), :].astype(jnp.float32)
            return carry
        lax.fori_loop(0, src.shape[0] // (16 * sub), body, 0)

    def out_part(ref, g, peer):
        low, high = ((0, rows), (rows, out_rows))[g]
        return ref.at[peer, pl.ds(low * sub, (high - low) * sub)]

    def back_part(ref, g, peer):
        low, high, _ = back[g]
        return ref.at[peer, pl.ds(low * sub, (high - low) * sub)]

    def copy_to(part, src, dst, g, k, s_sem, r_sem):
        peer = lax.rem(me + k, groups)
        return pltpu.make_async_remote_copy(
            src_ref=part(src, g, peer), dst_ref=part(dst, g, me), send_sem=s_sem.at[g, k], recv_sem=r_sem.at[g, k],
            device_id={"expert": peer}, device_id_type=MESH)

    def send_blocks(g, part, gather, src, dst, s_sem, r_sem):
        def body(i, carry):
            peer = lax.rem(me + i + 1, groups)
            gather(peer, part(src, g, peer))

            @pl.when(i >= 1)
            def _():
                copy_to(part, src, dst, g, i, s_sem, r_sem).start()

            return carry

        lax.fori_loop(0, groups, body, 0)

    def take_blocks(g, part, src, dst, own, first, s_sem, r_sem):
        widen(part(own, g, me), dst, first(me))

        def body(k, carry):
            peer = lax.rem(me - k + groups, groups)
            pltpu.make_async_remote_copy(
                src_ref=part(own, g, peer), dst_ref=part(src, g, peer), send_sem=s_sem.at[g, k], recv_sem=r_sem.at[g, k],
                device_id={"expert": peer}, device_id_type=MESH).wait_recv()
            widen(part(src, g, peer), dst, first(peer))
            return carry

        lax.fori_loop(1, groups, body, 0)

    out_lines = -(-out_rows // LANES)
    for g in range(GROUPS):
        low, high = ((0, rows), (rows, out_rows))[g]
        send_blocks(g, out_part, lambda peer, dst: gather_rows(pack_idx, peer * out_lines, low, high, xr_rows, dst), send, recv, ssem, rsem)

    every[me] = count[...]
    for j in range(2):
        for b in range(tokens // LANES):
            part = slice(b * LANES, (b + 1) * LANES)
            wide_gates[j, part, :] = jnp.broadcast_to(gates_ref[j:j + 1, part], (LANES, LANES)).T
    for k in range(1, groups):
        source = lax.rem(me - k + groups, groups)
        pltpu.make_async_remote_copy(
            src_ref=count, dst_ref=every.at[source], send_sem=csend.at[k], recv_sem=crecv.at[k],
            device_id={"expert": source}, device_id_type=MESH).wait_recv()
    group_tables(me, groups, rows, out_rows, back, group_experts, capacity, every, ids_ref, hot, same, rank_ref, pos_ref, lhs_v, ret_v, comb_v, load_ref)
    tables = [pltpu.make_async_copy(a, b, tsem.at[i + 1]) for i, (a, b) in enumerate(((lhs_v, lhs_idx), (ret_v, ret_idx), (comb_v, comb_idx)))]
    for t in tables:
        t.start()
    for t in tables:
        t.wait()

    def gather_lhs(e, stage):
        for q in range(capacity):
            stage[pl.ds(q * sub, sub), :] = rf_rows[lhs_idx[e, q]]

    def ffn(e, stage):
        slot = lax.rem(e, BUFS)
        for c in fetch(e, slot):
            c.wait()
        lhs = jnp.concatenate([stage[pl.ds(k, capacity, stride=sub), :] for k in range(sub)], axis=1).astype(jnp.bfloat16)
        hidden = jax.nn.gelu(dot_f32(lhs, wi[slot])).astype(jnp.bfloat16)
        out = dot_f32(hidden, wo[slot]).astype(jnp.bfloat16).astype(jnp.float32)
        at = e * capacity * sub
        for k in range(sub):
            of[pl.ds(at + k, capacity, stride=sub), :] = out[:, k * LANES:(k + 1) * LANES]

    first_expert = 0
    for b, (low, high, done) in enumerate(back):
        if b < GROUPS:
            take_blocks(b, out_part, recv, rf, send, lambda peer: (peer * out_rows + b * rows) * sub, ssem, rsem)

        def body(i, carry):
            for half in range(2):
                e = first_expert + i * 2 + half
                gather_lhs(e, stages[half])
                ffn(e, stages[half])

                @pl.when(e + BUFS < local_experts)
                def _():
                    for c in fetch(e + BUFS, lax.rem(e, BUFS)):
                        c.start()
            return carry

        lax.fori_loop(0, (done - first_expert) // 2, body, 0)
        first_expert = done
        send_blocks(b, back_part, lambda peer, dst: gather_rows(ret_idx, peer * out_lines, low, high, of_rows, dst), rsend, rrecv, rssem, rrsem)

    for b, (low, high, done) in enumerate(back):
        take_blocks(b, back_part, rrecv, retf, rsend, lambda peer: (peer * out_rows + low) * sub, rssem, rrsem)

    half = tokens // LANES

    def combine(line, carry):
        for c in range(LANES // 16):
            got = []
            for r in range(16):
                col = c * 16 + r
                row = xr_rows[line * LANES + col]
                for j in range(2):
                    row = row + wide_gates[j, pl.ds(pl.multiple_of(line * LANES, LANES) + col, 1), :] * retf_rows[comb_idx[j * half + line, col]]
                got.append(row)
            xr[pl.ds(pl.multiple_of((line * LANES + c * 16) * sub, 16 * sub), 16 * sub), :] = jnp.concatenate(got, axis=0)
        part = pl.ds(pl.multiple_of(line * LANES, LANES), LANES)
        for k in range(sub):
            x_ref[part, k * LANES:(k + 1) * LANES] = xr[pl.ds(line * LANES * sub + k, LANES, stride=sub), :].astype(jnp.bfloat16)

        @pl.when(line >= 1)
        def _():
            put(line - 1).start()

        return carry

    def put(line):
        part = pl.ds(pl.multiple_of(line * LANES, LANES), LANES)
        return pltpu.make_async_copy(x_ref.at[part], out_hbm.at[part], osem.at[line])

    lax.fori_loop(0, half, combine, 0)
    put(half - 1).start()
    for line in range(half):
        put(line).wait()
    for g in range(GROUPS):
        for k in range(1, groups):
            if g == 0:
                count_copy(k).wait_send()
            copy_to(out_part, send, recv, g, k, ssem, rsem).wait_send()
    for b in range(len(back)):
        for k in range(1, groups):
            copy_to(back_part, rsend, rrecv, b, k, rssem, rrsem).wait_send()


def compact_step(groups, rows, out_rows, capacity, gates, ids, token_rows, w_in, w_out):
    tokens, model_dim = token_rows.shape
    local_experts, _, hidden_dim = w_in.shape
    experts = local_experts * groups
    group_experts = local_experts // GROUPS
    sub = model_dim // LANES
    span = rows * sub
    vmem = pl.BlockSpec(memory_space=pltpu.VMEM)
    hbm = pl.BlockSpec(memory_space=pl.ANY)
    wire = pltpu.VMEM((groups, out_rows * sub, LANES), jnp.bfloat16)
    back = stages_of(tokens, 2, groups, local_experts)
    back_sems = pltpu.SemaphoreType.DMA((len(back), groups))
    sems = pltpu.SemaphoreType.DMA((GROUPS, groups))
    table_rows = (
        groups * -(-out_rows // LANES),
        local_experts,
        groups * -(-out_rows // LANES),
        2 * tokens // LANES,
    )
    return pl.pallas_call(
        functools.partial(exchange_kernel, groups, rows, out_rows, back, capacity),
        out_shape=(jax.ShapeDtypeStruct((tokens, model_dim), jnp.bfloat16), jax.ShapeDtypeStruct((1, 1), jnp.float32)),
        in_specs=[vmem, vmem, hbm, hbm, hbm],
        out_specs=(hbm, vmem),
        scratch_shapes=[
            pltpu.VMEM((2, LANES, tokens), jnp.bfloat16),
            pltpu.VMEM((experts, experts), jnp.bfloat16),
            pltpu.VMEM((8, experts), jnp.float32),
            pltpu.VMEM((groups, 8, experts), jnp.float32),
            pltpu.VMEM((8, tokens), jnp.float32),
            pltpu.VMEM((8, tokens), jnp.float32),
            *[pltpu.VMEM((r, LANES), jnp.int32) for r in table_rows],
            *[pltpu.SMEM((r, LANES), jnp.int32) for r in table_rows],
            pltpu.VMEM((2, tokens, LANES), jnp.float32),
            pltpu.VMEM((tokens, model_dim), jnp.bfloat16),
            pltpu.VMEM((tokens, sub, LANES), jnp.float32),
            wire,
            wire,
            pltpu.VMEM((groups * out_rows, sub, LANES), jnp.float32),
            pltpu.VMEM((capacity * sub, LANES), jnp.float32),
            pltpu.VMEM((capacity * sub, LANES), jnp.float32),
            pltpu.VMEM((local_experts * capacity, sub, LANES), jnp.float32),
            wire,
            wire,
            pltpu.VMEM((groups * out_rows + 8, sub, LANES), jnp.float32),
            pltpu.VMEM((BUFS, model_dim, hidden_dim), jnp.bfloat16),
            pltpu.VMEM((BUFS, hidden_dim, model_dim), jnp.bfloat16),
            pltpu.SemaphoreType.DMA((BUFS, 2)),
            sems, sems, back_sems, back_sems,
            pltpu.SemaphoreType.DMA((groups,)),
            pltpu.SemaphoreType.DMA((groups,)),
            pltpu.SemaphoreType.DMA((5,)),
            pltpu.SemaphoreType.DMA((tokens // LANES,)),
        ],
        compiler_params=pltpu.CompilerParams(collective_id=0, has_side_effects=True, vmem_limit_bytes=67043328),
        name="expert_exchange",
    )(gates, ids, token_rows, w_in, w_out)


def hand_over(rows):
    parts = 16
    size = rows.shape[0] // parts

    def kernel(a_ref, o_ref, buf, sem_in, sem_out):
        part = [pl.ds(i * size, size) for i in range(parts)]
        take = [pltpu.make_async_copy(a_ref.at[p], buf.at[p], sem_in.at[i]) for i, p in enumerate(part)]
        give = [pltpu.make_async_copy(buf.at[p], o_ref.at[p], sem_out.at[i]) for i, p in enumerate(part)]
        for t in take:
            t.start()
        for t, g in zip(take, give):
            t.wait()
            g.start()
        for g in give:
            g.wait()

    return pl.pallas_call(
        kernel,
        in_specs=[pl.BlockSpec(memory_space=pl.ANY)],
        out_specs=pl.BlockSpec(memory_space=pl.ANY),
        out_shape=jax.ShapeDtypeStruct(rows.shape, rows.dtype),
        scratch_shapes=[pltpu.VMEM(rows.shape, rows.dtype), pltpu.SemaphoreType.DMA((parts,)), pltpu.SemaphoreType.DMA((parts,))],
        name="hand_over",
    )(rows)


def solution(mesh):
    groups = mesh.shape["expert"]
    row_spec = P(("data", "expert"), None)
    weight_spec = P("expert", None, None)

    def device_step(token_rows, expert_ids, gate_weights, w_in, w_out):
        tokens, top_k = expert_ids.shape
        local_experts = w_in.shape[0]
        capacity = tokens * top_k // local_experts
        rows = block_rows(tokens, top_k, groups)
        fast, load = compact_step(groups, rows, total_rows(tokens, top_k, groups), capacity, gate_weights.T, expert_ids.T, token_rows, w_in, w_out)
        fast = hand_over(fast)
        overflow = load[0, 0] > 0.0
        general = lambda state: (jnp.array(False), padded_step(groups, token_rows, expert_ids, gate_weights, w_in, w_out))
        return lax.while_loop(lambda state: state[0], general, (overflow, fast))[1]

    return jax.shard_map(device_step, mesh=mesh, in_specs=(row_spec, row_spec, row_spec, weight_spec, weight_spec), out_specs=row_spec, check_vma=False)
```
